512 devices in a mesh: dist: 4 (over y_lo, core), pix: 128 (over z, x, y_hi).
Axes of the slice: x: 4, y: 8 (y_hi: 4, y_lo: 2; y = y_hi * 2 + y_lo), z: 8, core: 2. Of those that a mesh axis runs over, the one named last changes fastest.
Arguments:
- contrast: float32 [4, 2, 2048, 2048], P('dist', None, 'pix'), may hold values from -6 to 6
- defocus: float32 [4], P('dist'), may hold values from 40 to 400
- blurring: float32 [4], P('dist'), may hold values from 0.5 to 4
Outputs:
- phase: float32 [2, 2048, 2048], P(None, 'pix')
The draws below stay inside these ranges and needn't reach their ends.
All inputs are finite; a program needn't handle non-finite values.
Results may differ from the reference program's by a relative error of at most 0.0003.
Values sent between devices are 32-bit elements; how exact they have to be, the bound alone decides.
No kernel may reach another device: no remote copies, remote signals or barrier semaphores. Data moves between devices by JAX's collectives and lax.ppermute only.
A program may use at most 64 MiB of HBM per device.

```python
import math
import jax
import jax.numpy as jnp
from jax import lax

NC = 2048
NR = 2048
PROJ = 2
NDIST = 4


def shard_levels(key, dims, cuts, least, high):
    def one(position, shards_of):
        steps = jax.random.uniform(jax.random.fold_in(jax.random.fold_in(key, 6), position), (shards_of,), jnp.float32, least / len(cuts), high / len(cuts))
        return jnp.repeat(jnp.exp(steps), dims[position] // shards_of).reshape((-1,) + (1,) * (len(dims) - position - 1))

    loudness = one(*cuts[0])
    for cut in cuts[1:]:
        loudness = loudness * one(*cut)
    return loudness


def bell_draw(stream_key, shape, deviation, most, shards=(), kind=jnp.bfloat16):
    result = deviation * jax.random.normal(stream_key, shape, jnp.float32)
    if shards:
        result = result * shard_levels(stream_key, shape, shards, -0.22, 0.18)
    return jnp.clip(result, -most, most).astype(kind)


def setup_inputs(seed: int = 0) -> dict:
    streams_of = jax.random.split(jax.random.key(seed), 4)
    return {
        "contrast": bell_draw(streams_of[0], (NDIST, PROJ, NR, NC), 1.0, 6.0, ((0, 4), (2, 128)), jnp.float32),
        "defocus": jnp.clip(jnp.exp(math.log(400.0) - 2.3025851 * jax.random.uniform(streams_of[1], (NDIST,), jnp.float32) ** shard_levels(streams_of[1], (NDIST,), ((0, 4),), -0.2, 0.2)), 40.0, 400.0),
        "blurring": jnp.clip(0.5 + 3.5 * jax.random.uniform(streams_of[2], (NDIST,), jnp.float32) ** shard_levels(streams_of[2], (NDIST,), ((0, 4),), -0.2, 0.2), 0.5, 4.0),
    }


ABSORB_RATIO = 0.1
REGULARIZER = 0.05


def signed_square(freq_index, period):
    shifted = freq_index - period * (2 * freq_index >= period).astype(jnp.int32)
    fraction = shifted.astype(jnp.float32) / period
    return fraction * fraction


def transfer(defocus_value, blur_rate, squared):
    return jnp.exp(-blur_rate * squared) * (jnp.sin(defocus_value * squared) + ABSORB_RATIO * jnp.cos(defocus_value * squared))


def reference(contrast, defocus, blurring):
    row_square = signed_square(jnp.arange(NR, dtype=jnp.int32), NR)
    col_square = signed_square(jnp.arange(NC, dtype=jnp.int32), NC)
    squared = row_square[:, None] + col_square[None, :]
    gain_table = transfer(defocus[:, None, None], blurring[:, None, None], squared[None])
    denominator = jnp.sum(gain_table * gain_table, axis=0) + REGULARIZER

    def one_window(window_index):
        images = lax.dynamic_index_in_dim(contrast, window_index, 1, keepdims=False)
        spectra = jnp.fft.fft2(images)
        numerator = jnp.sum(gain_table * spectra, axis=0)
        return jnp.real(jnp.fft.ifft2(numerator / (2.0 * denominator)))

    return lax.map(one_window, jnp.arange(PROJ, dtype=jnp.int32))
```

```python
import math

import jax
import jax.numpy as jnp
import numpy as np
from jax import lax
from jax.experimental import pallas as pl
from jax.experimental.pallas import tpu as pltpu
from jax.sharding import PartitionSpec as P

ABSORB_RATIO = 0.1
REGULARIZER = 0.05
SIZE = 2048
LONG = 128
SHORT = 16
NDIST = 4
WIDE = 4


def angle_tables(left, right, period):
    turns = np.outer(np.arange(left), np.arange(right)) % period
    angles = 2.0 * np.pi * turns / period
    return np.cos(angles), np.sin(angles)


def right_table():
    cosine, sine = angle_tables(SHORT, SHORT, SHORT)
    same = np.eye(WIDE)
    c, s = np.kron(same, cosine), np.kron(same, sine)
    return np.block([[c, -s], [s, c]])


def turn_lanes(table):
    half = table.shape[0] // 2
    return np.concatenate([-table[half:], table[:half]], axis=0)


def turn_after(table):
    half = table.shape[1] // 2
    return np.concatenate([table[:, half:], -table[:, :half]], axis=1)


COS, SIN = angle_tables(LONG, LONG, LONG)
RIGHT = right_table()
BACK = np.array(RIGHT.T)
ROW_TWIST = angle_tables(SHORT, LONG, SIZE)
COL_TWIST = tuple(np.tile(t, (1, 2 * WIDE)) for t in angle_tables(LONG, SHORT, SIZE))


def f32(x):
    return np.asarray(x, np.float32)


ROW_FORWARD = f32(np.concatenate([COS, SIN], axis=1))
COL_FORWARD = f32(np.concatenate([COS, SIN], axis=0))
COL_RIGHT = f32(np.concatenate([RIGHT, turn_lanes(RIGHT)], axis=0))
COL_LEFT = f32(np.concatenate([BACK, turn_after(BACK)], axis=1))
COL_BACK = f32(np.concatenate([COS, -SIN], axis=1))
ROW_BACK = f32(np.concatenate([COS, -SIN], axis=0))
ROW_TW = f32(np.stack(ROW_TWIST))
COL_TW = f32(np.stack(COL_TWIST))


def product(a, b, a_dim=1, b_dim=0):
    return lax.dot_general(
        a,
        b,
        (((a_dim,), (b_dim,)), ((), ())),
        precision=lax.Precision.HIGHEST,
        preferred_element_type=jnp.float32,
    )


def four_point(z, sign):
    (r0, i0), (r1, i1), (r2, i2), (r3, i3) = z
    ar, ai, br, bi = r0 + r2, i0 + i2, r0 - r2, i0 - i2
    cr, ci, dr, di = r1 + r3, i1 + i3, r1 - r3, i1 - i3
    if sign > 0:
        plus, minus = (br + di, bi - dr), (br - di, bi + dr)
    else:
        plus, minus = (br - di, bi + dr), (br + di, bi - dr)
    return [(ar + cr, ai + ci), plus, (ar - cr, ai - ci), minus]


def times(z, turns, sign):
    r, i = z
    if turns == 0:
        return z
    c = float(np.float32(math.cos(2 * math.pi * turns / 16)))
    s = float(np.float32(sign * math.sin(2 * math.pi * turns / 16)))
    return r * c + i * s, i * c - r * s


def sixteen_point(z, sign):
    inner = [four_point([z[4 * a + b] for a in range(4)], sign) for b in range(4)]
    out = [None] * 16
    for c in range(4):
        mixed = four_point([times(inner[b][c], b * c, sign) for b in range(4)], sign)
        for e in range(4):
            out[c + 4 * e] = mixed[e]
    return out


def row_forward(images, table, twist):
    z = [(images[0][:, LONG * j : LONG * (j + 1)], images[1][:, LONG * j : LONG * (j + 1)]) for j in range(SHORT)]
    spread = sixteen_point(z, 1)
    turned = []
    for j, (r, i) in enumerate(spread):
        c, s = twist[0][j : j + 1, :], twist[1][j : j + 1, :]
        turned.append((r * c + i * s, i * c - r * s))
    out = []
    for d in range(NDIST):
        part = turned[WIDE * d : WIDE * (d + 1)]
        re, im = [r for r, _ in part], [i for _, i in part]
        left = jnp.concatenate(re + im, axis=0)
        right = jnp.concatenate(im + [-r for r in re], axis=0)
        both = jnp.concatenate([left, right], axis=1)
        out.append(product(table, both, 1, 1))
    return jnp.concatenate(out, axis=0)


def wave(turns):
    r = turns - jnp.floor(turns + 0.5)
    r = jnp.where(r > 0.25, 0.5 - r, jnp.where(r < -0.25, -0.5 - r, r))
    x = r * (2.0 * math.pi)
    y = x * x
    p = -1.0 / 39916800.0
    for term in (1.0 / 362880.0, -1.0 / 5040.0, 1.0 / 120.0, -1.0 / 6.0, 1.0):
        p = p * y + term
    return x * p


def signed_square(index):
    shifted = jnp.where(2 * index >= SIZE, index - SIZE, index)
    fraction = shifted.astype(jnp.float32) * (1.0 / SIZE)
    return fraction * fraction


def gains(defocus, blurring, first_col):
    shape = (LONG, LONG)
    lane = lax.broadcasted_iota(jnp.int32, shape, 1)
    row = lax.broadcasted_iota(jnp.int32, shape, 0)
    squared = signed_square(row + LONG * (lane & 15)) + signed_square(first_col + ((lane >> 4) & 3))
    low = lane < LONG // 2
    amplitude = math.sqrt(1.0 + ABSORB_RATIO * ABSORB_RATIO)
    shift = math.atan(ABSORB_RATIO) / (2.0 * math.pi)
    out = []
    for d in range(0, NDIST, 2):
        focus = jnp.where(low, defocus[d], defocus[d + 1]) * (1.0 / (2.0 * math.pi))
        blur = jnp.where(low, blurring[d], blurring[d + 1])
        g = (amplitude * jnp.exp(-blur * squared)) * wave(focus * squared + shift)
        other = jnp.concatenate([g[:, LONG // 2 :], g[:, : LONG // 2]], axis=1)
        out += [jnp.where(low, g, other), jnp.where(low, other, g)]
    return out


def column_middle(x, gain, forward, right, left, back, twist):
    c, s = twist[0], twist[1]
    parts = []
    for d in range(NDIST):
        both = product(forward, x[LONG * d : LONG * (d + 1)])
        u, v = both[:LONG], both[LONG:]
        parts.append(jnp.concatenate([u * c - v * s, v * c + u * s], axis=1))
    spectra = product(jnp.concatenate(parts, axis=0), right)
    numerator = gain[0] * spectra[:LONG]
    weight = gain[0] * gain[0]
    for d in range(1, NDIST):
        numerator = numerator + gain[d] * spectra[LONG * d : LONG * (d + 1)]
        weight = weight + gain[d] * gain[d]
    quotient = numerator / (2.0 * (weight + REGULARIZER))
    both = product(quotient, left)
    a, b = both[:, :LONG], both[:, LONG:]
    upright = jnp.concatenate([a * c - b * s, b * c + a * s], axis=0)
    return product(back, upright)


def row_back(x, table, twist):
    z = []
    scale = 1.0 / (SIZE * SIZE)
    for d in range(NDIST):
        t = x[LONG * d : LONG * (d + 1)].T
        half = LONG // 2
        turned = jnp.concatenate([t[half:], -t[:half]], axis=0)
        o = product(jnp.concatenate([t, turned], axis=1), table)
        for j in range(WIDE):
            r = o[SHORT * j : SHORT * (j + 1)]
            i = o[half + SHORT * j : half + SHORT * (j + 1)]
            v = WIDE * d + j
            c, s = twist[0][v : v + 1, :] * scale, twist[1][v : v + 1, :] * scale
            z.append((r * c - i * s, i * c + r * s))
    return sixteen_point(z, -1)


def first_kernel(images, table, twist, out):
    out[...] = row_forward(images[...], table[...], twist[...])


def middle_kernel(par, x, forward, right, left, back, twist, out):
    first_col = SHORT * lax.axis_index("pix") + WIDE * lax.axis_index("dist")
    table = gains([par[d, 0] for d in range(NDIST)], [par[d, 1] for d in range(NDIST)], first_col)
    out[...] = column_middle(x[...], table, forward[...], right[...], left[...], back[...], twist[...])


def last_kernel(x, table, twist, out):
    for j, (r, i) in enumerate(row_back(x[...], table[...], twist[...])):
        out[0, :, LONG * j : LONG * (j + 1)] = r
        out[1, :, LONG * j : LONG * (j + 1)] = i


def call(kernel, shape, name, smem_first=False):
    def run(*args):
        specs = [pl.BlockSpec(memory_space=pltpu.VMEM) for _ in args]
        if smem_first:
            specs[0] = pl.BlockSpec(memory_space=pltpu.SMEM)
        return pl.pallas_call(
            kernel,
            out_shape=jax.ShapeDtypeStruct(shape, jnp.float32),
            in_specs=specs,
            out_specs=pl.BlockSpec(memory_space=pltpu.VMEM),
            name=name,
        )(*args)

    return run


def body(contrast, defocus, blurring):
    par = lax.all_gather(jnp.stack([defocus, blurring], axis=1), "dist", axis=0, tiled=True)
    sent = call(first_kernel, (NDIST * LONG, LONG), "rows_forward")(contrast[0], ROW_FORWARD, ROW_TW)
    got = lax.all_to_all(sent.reshape(NDIST * LONG, 1, LONG), ("dist", "pix"), 0, 0, tiled=True)
    middle = call(middle_kernel, (LONG, LONG), "columns", True)(
        par, got.reshape(NDIST * LONG, LONG), COL_FORWARD, COL_RIGHT, COL_LEFT, COL_BACK, COL_TW
    )
    mine = lax.all_to_all(middle.reshape(LONG, 1, LONG), "pix", 0, 0, tiled=True).reshape(LONG, LONG)
    whole = lax.all_gather(mine, "dist", axis=0, tiled=True)
    return call(last_kernel, (2, SHORT, SIZE), "rows_back")(whole, ROW_BACK, ROW_TW)


def solution(mesh):
    return jax.shard_map(
        body,
        mesh=mesh,
        in_specs=(P("dist", None, "pix", None), P("dist"), P("dist")),
        out_specs=P(None, "pix", None),
        check_vma=False,
    )
```

```python
import math

import jax
import jax.numpy as jnp
import numpy as np
from jax import lax
from jax.experimental import pallas as pl
from jax.experimental.pallas import tpu as pltpu
from jax.sharding import PartitionSpec as P

ABSORB_RATIO = 0.1
REGULARIZER = 0.05
SIZE = 2048
LONG = 128
SHORT = 16
NDIST = 4
WIDE = 4
VMEM_LIMIT = 8 << 20


def angle_tables(left, right, period):
    turns = np.outer(np.arange(left), np.arange(right)) % period
    angles = 2.0 * np.pi * turns / period
    return np.cos(angles), np.sin(angles)


def right_table():
    cosine, sine = angle_tables(SHORT, SHORT, SHORT)
    same = np.eye(WIDE)
    c, s = np.kron(same, cosine), np.kron(same, sine)
    return np.block([[c, -s], [s, c]])


def turn_lanes(table):
    half = table.shape[0] // 2
    return np.concatenate([-table[half:], table[:half]], axis=0)


def turn_after(table):
    half = table.shape[1] // 2
    return np.concatenate([table[:, half:], -table[:, :half]], axis=1)


COS, SIN = angle_tables(LONG, LONG, LONG)
RIGHT = right_table()
BACK = np.array(RIGHT.T)
ROW_TWIST = angle_tables(SHORT, LONG, SIZE)
COL_TWIST = tuple(np.tile(t, (1, 2 * WIDE)) for t in angle_tables(LONG, SHORT, SIZE))


def f32(x):
    return np.asarray(x, np.float32)


ROW_FORWARD = f32(np.concatenate([COS, SIN], axis=1))
COL_FORWARD = f32(np.concatenate([COS, SIN], axis=0))
COL_RIGHT = f32(np.concatenate([RIGHT, turn_lanes(RIGHT)], axis=0))
COL_LEFT = f32(np.concatenate([BACK, turn_after(BACK)], axis=1))
COL_BACK = f32(np.concatenate([COS, -SIN], axis=1))
ROW_BACK = f32(np.concatenate([COS, -SIN], axis=0))
ROW_TW = f32(np.stack(ROW_TWIST))
COL_TW = f32(np.stack(COL_TWIST))


def product(a, b, a_dim=1, b_dim=0):
    return lax.dot_general(
        a,
        b,
        (((a_dim,), (b_dim,)), ((), ())),
        precision=lax.Precision.HIGHEST,
        preferred_element_type=jnp.float32,
    )


def four_point(z, sign):
    (r0, i0), (r1, i1), (r2, i2), (r3, i3) = z
    ar, ai, br, bi = r0 + r2, i0 + i2, r0 - r2, i0 - i2
    cr, ci, dr, di = r1 + r3, i1 + i3, r1 - r3, i1 - i3
    if sign > 0:
        plus, minus = (br + di, bi - dr), (br - di, bi + dr)
    else:
        plus, minus = (br - di, bi + dr), (br + di, bi - dr)
    return [(ar + cr, ai + ci), plus, (ar - cr, ai - ci), minus]


def times(z, turns, sign):
    r, i = z
    if turns == 0:
        return z
    c = float(np.float32(math.cos(2 * math.pi * turns / 16)))
    s = float(np.float32(sign * math.sin(2 * math.pi * turns / 16)))
    return r * c + i * s, i * c - r * s


def sixteen_point(z, sign):
    inner = [four_point([z[4 * a + b] for a in range(4)], sign) for b in range(4)]
    out = [None] * 16
    for c in range(4):
        mixed = four_point([times(inner[b][c], b * c, sign) for b in range(4)], sign)
        for e in range(4):
            out[c + 4 * e] = mixed[e]
    return out


def row_forward(images, table, twist):
    z = [(images[0][:, LONG * j : LONG * (j + 1)], images[1][:, LONG * j : LONG * (j + 1)]) for j in range(SHORT)]
    spread = sixteen_point(z, 1)
    turned = []
    for j, (r, i) in enumerate(spread):
        c, s = twist[0][j : j + 1, :], twist[1][j : j + 1, :]
        turned.append((r * c + i * s, i * c - r * s))
    out = []
    for d in range(NDIST):
        part = turned[WIDE * d : WIDE * (d + 1)]
        re, im = [r for r, _ in part], [i for _, i in part]
        left = jnp.concatenate(re + im, axis=0)
        right = jnp.concatenate(im + [-r for r in re], axis=0)
        both = jnp.concatenate([left, right], axis=1)
        out.append(product(table, both, 1, 1))
    return jnp.concatenate(out, axis=0)


def wave(turns):
    r = turns - jnp.floor(turns + 0.5)
    r = jnp.where(r > 0.25, 0.5 - r, jnp.where(r < -0.25, -0.5 - r, r))
    x = r * (2.0 * math.pi)
    y = x * x
    p = -1.0 / 39916800.0
    for term in (1.0 / 362880.0, -1.0 / 5040.0, 1.0 / 120.0, -1.0 / 6.0, 1.0):
        p = p * y + term
    return x * p


def signed_square(index):
    shifted = jnp.where(2 * index >= SIZE, index - SIZE, index)
    fraction = shifted.astype(jnp.float32) * (1.0 / SIZE)
    return fraction * fraction


def gains(defocus, blurring, first_col):
    shape = (LONG, LONG)
    lane = lax.broadcasted_iota(jnp.int32, shape, 1)
    row = lax.broadcasted_iota(jnp.int32, shape, 0)
    squared = signed_square(row + LONG * (lane & 15)) + signed_square(first_col + ((lane >> 4) & 3))
    low = lane < LONG // 2
    amplitude = math.sqrt(1.0 + ABSORB_RATIO * ABSORB_RATIO)
    shift = math.atan(ABSORB_RATIO) / (2.0 * math.pi)
    out = []
    for d in range(0, NDIST, 2):
        focus = jnp.where(low, defocus[d], defocus[d + 1]) * (1.0 / (2.0 * math.pi))
        blur = jnp.where(low, blurring[d], blurring[d + 1])
        g = (amplitude * jnp.exp(-blur * squared)) * wave(focus * squared + shift)
        other = jnp.concatenate([g[:, LONG // 2 :], g[:, : LONG // 2]], axis=1)
        out += [jnp.where(low, g, other), jnp.where(low, other, g)]
    return out


def column_middle(blocks, gain, forward, right, left, back, twist):
    c, s = twist[0], twist[1]
    parts = []
    for x in blocks:
        both = product(forward, x)
        u, v = both[:LONG], both[LONG:]
        parts.append(jnp.concatenate([u * c - v * s, v * c + u * s], axis=1))
    spectra = product(jnp.concatenate(parts, axis=0), right)
    numerator = gain[0] * spectra[:LONG]
    weight = gain[0] * gain[0]
    for d in range(1, NDIST):
        numerator = numerator + gain[d] * spectra[LONG * d : LONG * (d + 1)]
        weight = weight + gain[d] * gain[d]
    quotient = numerator / (2.0 * (weight + REGULARIZER))
    both = product(quotient, left)
    a, b = both[:, :LONG], both[:, LONG:]
    upright = jnp.concatenate([a * c - b * s, b * c + a * s], axis=0)
    return product(back, upright)


def row_back(x, table, twist):
    z = []
    scale = 1.0 / (SIZE * SIZE)
    for d in range(NDIST):
        t = x[LONG * d : LONG * (d + 1)].T
        half = LONG // 2
        turned = jnp.concatenate([t[half:], -t[:half]], axis=0)
        o = product(jnp.concatenate([t, turned], axis=1), table)
        for j in range(WIDE):
            r = o[SHORT * j : SHORT * (j + 1)]
            i = o[half + SHORT * j : half + SHORT * (j + 1)]
            v = WIDE * d + j
            c, s = twist[0][v : v + 1, :] * scale, twist[1][v : v + 1, :] * scale
            z.append((r * c - i * s, i * c + r * s))
    return sixteen_point(z, -1)


def first_kernel(images, defocus, blurring, table, twist, out, own):
    out[...] = row_forward(images[...], table[...], twist[...])
    lane = lax.broadcasted_iota(jnp.int32, own.shape, 1)
    own[...] = jnp.where(lane < LONG // 2, defocus[0], blurring[0])


def middle_kernel(par0, par1, par2, par3, x, forward, right, left, back, twist, out):
    distance = lax.axis_index("dist")
    first_col = SHORT * lax.axis_index("pix") + WIDE * distance
    half = LONG // 2
    pars = [p[...] for p in (par0, par1, par2, par3)]
    table = gains([p[:1, :1] for p in pars], [p[:1, half : half + 1] for p in pars], first_col)
    blocks = []
    for j in range(NDIST):
        start = pl.multiple_of(LONG * (distance ^ j), LONG)
        blocks.append(x[pl.ds(start, LONG), :])
    y = column_middle(blocks, table, forward[...], right[...], left[...], back[...], twist[...])
    for j in range(NDIST):
        out[LONG * j : LONG * (j + 1), :] = y


def last_kernel(x, table, twist, out):
    for j, (r, i) in enumerate(row_back(x[...], table[...], twist[...])):
        out[0, :, LONG * j : LONG * (j + 1)] = r
        out[1, :, LONG * j : LONG * (j + 1)] = i


def call(kernel, shapes, name, smem=()):
    def run(*args):
        specs = [pl.BlockSpec(memory_space=pltpu.SMEM if i in smem else pltpu.VMEM) for i in range(len(args))]
        return pl.pallas_call(
            kernel,
            out_shape=[jax.ShapeDtypeStruct(shape, jnp.float32) for shape in shapes],
            in_specs=specs,
            out_specs=[pl.BlockSpec(memory_space=pltpu.VMEM) for _ in shapes],
            compiler_params=pltpu.CompilerParams(vmem_limit_bytes=VMEM_LIMIT),
            name=name,
        )(*args)

    return run


def exchange(x):
    return lax.all_to_all(x.reshape(x.shape[0], 1, LONG), ("dist", "pix"), 0, 0, tiled=True).reshape(x.shape)


def body(contrast, defocus, blurring):
    rows = NDIST * LONG
    sent, own = call(first_kernel, ((rows, LONG), (8, LONG)), "rows_forward", (1, 2))(
        contrast[0], defocus, blurring, ROW_FORWARD, ROW_TW
    )
    pars = [own]
    for j in range(1, NDIST):
        pars.append(lax.ppermute(own, "dist", [(i, i ^ j) for i in range(NDIST)]))
    got = exchange(sent)
    (middle,) = call(middle_kernel, ((rows, LONG),), "columns")(
        *pars, got, COL_FORWARD, COL_RIGHT, COL_LEFT, COL_BACK, COL_TW
    )
    whole = exchange(middle)
    return call(last_kernel, ((2, SHORT, SIZE),), "rows_back")(whole, ROW_BACK, ROW_TW)[0]


def solution(mesh):
    return jax.shard_map(
        body,
        mesh=mesh,
        in_specs=(P("dist", None, "pix", None), P("dist"), P("dist")),
        out_specs=P(None, "pix", None),
        check_vma=False,
    )
```

```python
import math

import jax
import jax.numpy as jnp
import numpy as np
from jax import lax
from jax.experimental import pallas as pl
from jax.experimental.pallas import tpu as pltpu
from jax.sharding import Mesh
from jax.sharding import PartitionSpec as P

ABSORB_RATIO = 0.1
REGULARIZER = 0.05
SIZE = 2048
LONG = 128
SHORT = 16
NDIST = 4
WIDE = 4
VMEM_LIMIT = 8 << 20
DIST = ("l", "c")
PIX = ("z", "x", "h")
PIX_SIZES = (8, 4, 4)
BACK_ORDER = np.arange(LONG).reshape(PIX_SIZES).transpose(2, 1, 0).reshape(-1)


def angle_tables(left, right, period):
    turns = np.outer(np.arange(left), np.arange(right)) % period
    angles = 2.0 * np.pi * turns / period
    return np.cos(angles), np.sin(angles)


def right_table():
    cosine, sine = angle_tables(SHORT, SHORT, SHORT)
    same = np.eye(WIDE)
    c, s = np.kron(same, cosine), np.kron(same, sine)
    return np.block([[c, -s], [s, c]])


def turn_lanes(table):
    half = table.shape[0] // 2
    return np.concatenate([-table[half:], table[:half]], axis=0)


def turn_after(table):
    half = table.shape[1] // 2
    return np.concatenate([table[:, half:], -table[:, :half]], axis=1)


COS, SIN = angle_tables(LONG, LONG, LONG)
RIGHT = right_table()
BACK = np.array(RIGHT.T)
ROW_TWIST = angle_tables(SHORT, LONG, SIZE)
COL_TWIST = tuple(np.tile(t, (1, 2 * WIDE)) for t in angle_tables(LONG, SHORT, SIZE))


def f32(x):
    return np.asarray(x, np.float32)


ROW_FORWARD = f32(np.concatenate([COS, SIN], axis=1))
COL_FORWARD = f32(np.concatenate([COS, SIN], axis=0))
COL_RIGHT = f32(np.concatenate([RIGHT, turn_lanes(RIGHT)], axis=0))
COL_LEFT = f32(np.concatenate([BACK, turn_after(BACK)], axis=1))
COL_BACK = f32(np.concatenate([COS, -SIN], axis=1)[BACK_ORDER])
ROW_BACK = f32(np.concatenate([COS[BACK_ORDER], -SIN[BACK_ORDER]], axis=0))
ROW_TW = f32(np.stack(ROW_TWIST))
COL_TW = f32(np.stack(COL_TWIST))


def product(a, b, a_dim=1, b_dim=0):
    return lax.dot_general(
        a,
        b,
        (((a_dim,), (b_dim,)), ((), ())),
        precision=lax.Precision.HIGHEST,
        preferred_element_type=jnp.float32,
    )


def four_point(z, sign):
    (r0, i0), (r1, i1), (r2, i2), (r3, i3) = z
    ar, ai, br, bi = r0 + r2, i0 + i2, r0 - r2, i0 - i2
    cr, ci, dr, di = r1 + r3, i1 + i3, r1 - r3, i1 - i3
    if sign > 0:
        plus, minus = (br + di, bi - dr), (br - di, bi + dr)
    else:
        plus, minus = (br - di, bi + dr), (br + di, bi - dr)
    return [(ar + cr, ai + ci), plus, (ar - cr, ai - ci), minus]


def times(z, turns, sign):
    r, i = z
    if turns == 0:
        return z
    c = float(np.float32(math.cos(2 * math.pi * turns / 16)))
    s = float(np.float32(sign * math.sin(2 * math.pi * turns / 16)))
    return r * c + i * s, i * c - r * s


def sixteen_point(z, sign):
    inner = [four_point([z[4 * a + b] for a in range(4)], sign) for b in range(4)]
    out = [None] * 16
    for c in range(4):
        mixed = four_point([times(inner[b][c], b * c, sign) for b in range(4)], sign)
        for e in range(4):
            out[c + 4 * e] = mixed[e]
    return out


def row_forward(images, table, twist):
    z = [(images[0][:, LONG * j : LONG * (j + 1)], images[1][:, LONG * j : LONG * (j + 1)]) for j in range(SHORT)]
    spread = sixteen_point(z, 1)
    turned = []
    for j, (r, i) in enumerate(spread):
        c, s = twist[0][j : j + 1, :], twist[1][j : j + 1, :]
        turned.append((r * c + i * s, i * c - r * s))
    out = []
    for d in range(NDIST):
        part = turned[WIDE * d : WIDE * (d + 1)]
        re, im = [r for r, _ in part], [i for _, i in part]
        left = jnp.concatenate(re + im, axis=0)
        right = jnp.concatenate(im + [-r for r in re], axis=0)
        both = jnp.concatenate([left, right], axis=1)
        out.append(product(table, both, 1, 1))
    return jnp.concatenate(out, axis=0)


def wave(turns):
    r = turns - jnp.floor(turns + 0.5)
    r = jnp.where(r > 0.25, 0.5 - r, jnp.where(r < -0.25, -0.5 - r, r))
    x = r * (2.0 * math.pi)
    y = x * x
    p = -1.0 / 39916800.0
    for term in (1.0 / 362880.0, -1.0 / 5040.0, 1.0 / 120.0, -1.0 / 6.0, 1.0):
        p = p * y + term
    return x * p


def signed_square(index):
    shifted = jnp.where(2 * index >= SIZE, index - SIZE, index)
    fraction = shifted.astype(jnp.float32) * (1.0 / SIZE)
    return fraction * fraction


def gains(defocus, blurring, first_col):
    shape = (LONG, LONG)
    lane = lax.broadcasted_iota(jnp.int32, shape, 1)
    row = lax.broadcasted_iota(jnp.int32, shape, 0)
    squared = signed_square(row + LONG * (lane & 15)) + signed_square(first_col + ((lane >> 4) & 3))
    low = lane < LONG // 2
    amplitude = math.sqrt(1.0 + ABSORB_RATIO * ABSORB_RATIO)
    shift = math.atan(ABSORB_RATIO) / (2.0 * math.pi)
    out = []
    for d in range(0, NDIST, 2):
        focus = jnp.where(low, defocus[d], defocus[d + 1]) * (1.0 / (2.0 * math.pi))
        blur = jnp.where(low, blurring[d], blurring[d + 1])
        g = (amplitude * jnp.exp(-blur * squared)) * wave(focus * squared + shift)
        other = jnp.concatenate([g[:, LONG // 2 :], g[:, : LONG // 2]], axis=1)
        out += [jnp.where(low, g, other), jnp.where(low, other, g)]
    return out


def column_middle(blocks, gain, forward, right, left, back, twist):
    c, s = twist[0], twist[1]
    parts = []
    for x in blocks:
        both = product(forward, x)
        u, v = both[:LONG], both[LONG:]
        parts.append(jnp.concatenate([u * c - v * s, v * c + u * s], axis=1))
    spectra = product(jnp.concatenate(parts, axis=0), right)
    numerator = gain[0] * spectra[:LONG]
    weight = gain[0] * gain[0]
    for d in range(1, NDIST):
        numerator = numerator + gain[d] * spectra[LONG * d : LONG * (d + 1)]
        weight = weight + gain[d] * gain[d]
    quotient = numerator / (2.0 * (weight + REGULARIZER))
    both = product(quotient, left)
    a, b = both[:, :LONG], both[:, LONG:]
    upright = jnp.concatenate([a * c - b * s, b * c + a * s], axis=0)
    return product(back, upright)


def row_back(x, table, twist):
    z = []
    scale = 1.0 / (SIZE * SIZE)
    for d in range(NDIST):
        start = LONG * (2 * (d % 2) + d // 2)
        t = x[start : start + LONG].T
        half = LONG // 2
        turned = jnp.concatenate([t[half:], -t[:half]], axis=0)
        o = product(jnp.concatenate([t, turned], axis=1), table)
        for j in range(WIDE):
            r = o[SHORT * j : SHORT * (j + 1)]
            i = o[half + SHORT * j : half + SHORT * (j + 1)]
            v = WIDE * d + j
            c, s = twist[0][v : v + 1, :] * scale, twist[1][v : v + 1, :] * scale
            z.append((r * c - i * s, i * c + r * s))
    return sixteen_point(z, -1)


def pair_kernel(defocus, blurring, out):
    lane = lax.broadcasted_iota(jnp.int32, out.shape, 1)
    out[...] = jnp.where(lane < LONG // 2, defocus[...], blurring[...])


def first_kernel(images, par, table, twist, out, par_out):
    out[...] = row_forward(images[...], table[...], twist[...])
    par_out[...] = par[...]


def middle_kernel(par, x, forward, right, left, back, twist, out):
    first_col = SHORT * lax.axis_index(PIX) + WIDE * lax.axis_index(DIST)
    half = LONG // 2
    defocus = [par[8 * d : 8 * d + 1, :1] for d in range(NDIST)]
    blurring = [par[8 * d : 8 * d + 1, half : half + 1] for d in range(NDIST)]
    table = gains(defocus, blurring, first_col)
    blocks = [x[LONG * d : LONG * (d + 1), :] for d in range(NDIST)]
    y = column_middle(blocks, table, forward[...], right[...], left[...], back[...], twist[...])
    out[:LONG, :] = y
    out[LONG:, :] = y


def last_kernel(x, table, twist, out):
    for j, (r, i) in enumerate(row_back(x[...], table[...], twist[...])):
        out[0, :, LONG * j : LONG * (j + 1)] = r
        out[1, :, LONG * j : LONG * (j + 1)] = i


def call(kernel, shapes, name, limit=VMEM_LIMIT):
    def run(*args):
        return pl.pallas_call(
            kernel,
            out_shape=[jax.ShapeDtypeStruct(shape, jnp.float32) for shape in shapes],
            in_specs=[pl.BlockSpec(memory_space=pltpu.VMEM) for _ in args],
            out_specs=[pl.BlockSpec(memory_space=pltpu.VMEM) for _ in shapes],
            compiler_params=pltpu.CompilerParams(vmem_limit_bytes=limit),
            name=name,
        )(*args)

    return run


def exchange(x, axes):
    return lax.all_to_all(x.reshape(x.shape[0], 1, LONG), axes, 0, 0, tiled=True).reshape(x.shape)


def body(contrast, defocus, blurring):
    rows = NDIST * LONG
    (pair,) = call(pair_kernel, ((8, LONG),), "pair")(defocus.reshape(1, 1), blurring.reshape(1, 1))
    par = lax.all_gather(pair, DIST, axis=0, tiled=True)
    sent, par = call(first_kernel, ((rows, LONG), par.shape), "rows_forward")(contrast[0], par, ROW_FORWARD, ROW_TW)
    got = exchange(sent, DIST + PIX)
    (middle,) = call(middle_kernel, ((2 * LONG, LONG),), "columns")(
        par, got, COL_FORWARD, COL_RIGHT, COL_LEFT, COL_BACK, COL_TW
    )
    bands = exchange(middle, ("l", "h", "x", "z"))
    whole = lax.all_gather(bands, "c", axis=0, tiled=True)
    return call(last_kernel, ((2, SHORT, SIZE),), "rows_back")(whole, ROW_BACK, ROW_TW)[0]


def solution(mesh):
    parts = Mesh(mesh.devices.reshape((2, 2) + PIX_SIZES), DIST + PIX)
    return jax.shard_map(
        body,
        mesh=parts,
        in_specs=(P(DIST, None, PIX, None), P(DIST), P(DIST)),
        out_specs=P(None, PIX, None),
        check_vma=False,
    )
```

```python
import math

import jax
import jax.numpy as jnp
import numpy as np
from jax import lax
from jax.experimental import pallas as pl
from jax.experimental.pallas import tpu as pltpu
from jax.sharding import Mesh
from jax.sharding import PartitionSpec as P

ABSORB_RATIO = 0.1
REGULARIZER = 0.05
SIZE = 2048
LONG = 128
SHORT = 16
NDIST = 4
WIDE = 4
VMEM_LIMIT = 8 << 20
DIST = ("l", "c")
PIX = ("z", "x", "h")
PIX_SIZES = (8, 4, 4)
BACK_ORDER = np.arange(LONG).reshape(PIX_SIZES).transpose(2, 1, 0).reshape(-1)


def angle_tables(left, right, period):
    turns = np.outer(np.arange(left), np.arange(right)) % period
    angles = 2.0 * np.pi * turns / period
    return np.cos(angles), np.sin(angles)


def right_table():
    cosine, sine = angle_tables(SHORT, SHORT, SHORT)
    same = np.eye(WIDE)
    c, s = np.kron(same, cosine), np.kron(same, sine)
    return np.block([[c, -s], [s, c]])


def turn_lanes(table):
    half = table.shape[0] // 2
    return np.concatenate([-table[half:], table[:half]], axis=0)


def turn_after(table):
    half = table.shape[1] // 2
    return np.concatenate([table[:, half:], -table[:, :half]], axis=1)


COS, SIN = angle_tables(LONG, LONG, LONG)
RIGHT = right_table()
BACK = np.array(RIGHT.T)
ROW_TWIST = angle_tables(SHORT, LONG, SIZE)
COL_TWIST = tuple(np.tile(t, (1, 2 * WIDE)) for t in angle_tables(LONG, SHORT, SIZE))


def f32(x):
    return np.asarray(x, np.float32)


ROW_FORWARD = f32(np.concatenate([COS, SIN], axis=1))
COL_FORWARD = f32(np.concatenate([COS, SIN], axis=0))
COL_RIGHT = f32(np.concatenate([RIGHT, turn_lanes(RIGHT)], axis=0))
COL_LEFT = f32(np.concatenate([BACK, turn_after(BACK)], axis=1))
COL_BACK = f32(np.concatenate([COS, -SIN], axis=1)[BACK_ORDER])
ROW_BACK = f32(np.concatenate([COS[BACK_ORDER], -SIN[BACK_ORDER]], axis=0))
ROW_TW = f32(np.stack(ROW_TWIST))
COL_TW = f32(np.stack(COL_TWIST))


def product(a, b, a_dim=1, b_dim=0):
    return lax.dot_general(
        a,
        b,
        (((a_dim,), (b_dim,)), ((), ())),
        precision=lax.Precision.HIGHEST,
        preferred_element_type=jnp.float32,
    )


def four_point(z, sign):
    (r0, i0), (r1, i1), (r2, i2), (r3, i3) = z
    ar, ai, br, bi = r0 + r2, i0 + i2, r0 - r2, i0 - i2
    cr, ci, dr, di = r1 + r3, i1 + i3, r1 - r3, i1 - i3
    if sign > 0:
        plus, minus = (br + di, bi - dr), (br - di, bi + dr)
    else:
        plus, minus = (br - di, bi + dr), (br + di, bi - dr)
    return [(ar + cr, ai + ci), plus, (ar - cr, ai - ci), minus]


def times(z, turns, sign):
    r, i = z
    if turns == 0:
        return z
    c = float(np.float32(math.cos(2 * math.pi * turns / 16)))
    s = float(np.float32(sign * math.sin(2 * math.pi * turns / 16)))
    return r * c + i * s, i * c - r * s


def sixteen_point(z, sign):
    inner = [four_point([z[4 * a + b] for a in range(4)], sign) for b in range(4)]
    out = [None] * 16
    for c in range(4):
        mixed = four_point([times(inner[b][c], b * c, sign) for b in range(4)], sign)
        for e in range(4):
            out[c + 4 * e] = mixed[e]
    return out


def row_forward(images, table, twist):
    z = [(images[0][:, LONG * j : LONG * (j + 1)], images[1][:, LONG * j : LONG * (j + 1)]) for j in range(SHORT)]
    spread = sixteen_point(z, 1)
    turned = []
    for j, (r, i) in enumerate(spread):
        c, s = twist[0][j : j + 1, :], twist[1][j : j + 1, :]
        turned.append((r * c + i * s, i * c - r * s))
    out = []
    for d in range(NDIST):
        part = turned[WIDE * d : WIDE * (d + 1)]
        re, im = [r for r, _ in part], [i for _, i in part]
        left = jnp.concatenate(re + im, axis=0)
        right = jnp.concatenate(im + [-r for r in re], axis=0)
        both = jnp.concatenate([left, right], axis=1)
        out.append(product(table, both, 1, 1))
    return jnp.concatenate(out, axis=0)


def wave(turns):
    r = turns - jnp.floor(turns + 0.5)
    r = jnp.where(r > 0.25, 0.5 - r, jnp.where(r < -0.25, -0.5 - r, r))
    x = r * (2.0 * math.pi)
    y = x * x
    p = -1.0 / 39916800.0
    for term in (1.0 / 362880.0, -1.0 / 5040.0, 1.0 / 120.0, -1.0 / 6.0, 1.0):
        p = p * y + term
    return x * p


def signed_square(index):
    shifted = jnp.where(2 * index >= SIZE, index - SIZE, index)
    fraction = shifted.astype(jnp.float32) * (1.0 / SIZE)
    return fraction * fraction


def gains(defocus, blurring, first_col):
    shape = (LONG, LONG)
    lane = lax.broadcasted_iota(jnp.int32, shape, 1)
    row = lax.broadcasted_iota(jnp.int32, shape, 0)
    squared = signed_square(row + LONG * (lane & 15)) + signed_square(first_col + ((lane >> 4) & 3))
    low = lane < LONG // 2
    amplitude = math.sqrt(1.0 + ABSORB_RATIO * ABSORB_RATIO)
    shift = math.atan(ABSORB_RATIO) / (2.0 * math.pi)
    out = []
    for d in range(0, NDIST, 2):
        focus = jnp.where(low, defocus[d], defocus[d + 1]) * (1.0 / (2.0 * math.pi))
        blur = jnp.where(low, blurring[d], blurring[d + 1])
        g = (amplitude * jnp.exp(-blur * squared)) * wave(focus * squared + shift)
        other = jnp.concatenate([g[:, LONG // 2 :], g[:, : LONG // 2]], axis=1)
        out += [jnp.where(low, g, other), jnp.where(low, other, g)]
    return out


def column_middle(blocks, gain, forward, right, left, back, twist):
    c, s = twist[0], twist[1]
    parts = []
    for x in blocks:
        both = product(forward, x)
        u, v = both[:LONG], both[LONG:]
        parts.append(jnp.concatenate([u * c - v * s, v * c + u * s], axis=1))
    spectra = product(jnp.concatenate(parts, axis=0), right)
    numerator = gain[0] * spectra[:LONG]
    weight = gain[0] * gain[0]
    for d in range(1, NDIST):
        numerator = numerator + gain[d] * spectra[LONG * d : LONG * (d + 1)]
        weight = weight + gain[d] * gain[d]
    quotient = numerator / (2.0 * (weight + REGULARIZER))
    both = product(quotient, left)
    a, b = both[:, :LONG], both[:, LONG:]
    upright = jnp.concatenate([a * c - b * s, b * c + a * s], axis=0)
    return product(back, upright)


def row_back(x, table, twist):
    z = []
    scale = 1.0 / (SIZE * SIZE)
    for d in range(NDIST):
        start = LONG * (2 * (d % 2) + d // 2)
        t = x[start : start + LONG].T
        half = LONG // 2
        turned = jnp.concatenate([t[half:], -t[:half]], axis=0)
        o = product(jnp.concatenate([t, turned], axis=1), table)
        for j in range(WIDE):
            r = o[SHORT * j : SHORT * (j + 1)]
            i = o[half + SHORT * j : half + SHORT * (j + 1)]
            v = WIDE * d + j
            c, s = twist[0][v : v + 1, :] * scale, twist[1][v : v + 1, :] * scale
            z.append((r * c - i * s, i * c + r * s))
    return sixteen_point(z, -1)


def first_kernel(images, table, twist, out):
    out[...] = row_forward(images[...], table[...], twist[...])


def middle_kernel(par, x, forward, right, left, back, twist, out):
    first_col = SHORT * lax.axis_index(PIX) + WIDE * lax.axis_index(DIST)
    defocus = [par[d : d + 1, :1] for d in range(NDIST)]
    blurring = [par[d : d + 1, 1:] for d in range(NDIST)]
    table = gains(defocus, blurring, first_col)
    blocks = [x[LONG * d : LONG * (d + 1), :] for d in range(NDIST)]
    y = column_middle(blocks, table, forward[...], right[...], left[...], back[...], twist[...])
    out[:LONG, :] = y
    out[LONG:, :] = y


def last_kernel(x, table, twist, out):
    for j, (r, i) in enumerate(row_back(x[...], table[...], twist[...])):
        out[0, :, LONG * j : LONG * (j + 1)] = r
        out[1, :, LONG * j : LONG * (j + 1)] = i


def call(kernel, shapes, name, limit=VMEM_LIMIT):
    def run(*args):
        return pl.pallas_call(
            kernel,
            out_shape=[jax.ShapeDtypeStruct(shape, jnp.float32) for shape in shapes],
            in_specs=[pl.BlockSpec(memory_space=pltpu.VMEM) for _ in args],
            out_specs=[pl.BlockSpec(memory_space=pltpu.VMEM) for _ in shapes],
            compiler_params=pltpu.CompilerParams(vmem_limit_bytes=limit),
            name=name,
        )(*args)

    return run


def exchange(x, axes):
    return lax.all_to_all(x.reshape(x.shape[0], 1, LONG), axes, 0, 0, tiled=True).reshape(x.shape)


def body(contrast, defocus, blurring):
    rows = NDIST * LONG
    (sent,) = call(first_kernel, ((rows, LONG),), "rows_forward", None)(contrast[0], ROW_FORWARD, ROW_TW)
    par = lax.all_gather(jnp.stack([defocus, blurring], axis=1), DIST, axis=0, tiled=True)
    got = exchange(sent, DIST + PIX)
    (middle,) = call(middle_kernel, ((2 * LONG, LONG),), "columns")(
        par, got, COL_FORWARD, COL_RIGHT, COL_LEFT, COL_BACK, COL_TW
    )
    bands = exchange(middle, ("l", "h", "x", "z"))
    whole = lax.all_gather(bands, "c", axis=0, tiled=True)
    return call(last_kernel, ((2, SHORT, SIZE),), "rows_back")(whole, ROW_BACK, ROW_TW)[0]


def solution(mesh):
    parts = Mesh(mesh.devices.reshape((2, 2) + PIX_SIZES), DIST + PIX)
    return jax.shard_map(
        body,
        mesh=parts,
        in_specs=(P(DIST, None, PIX, None), P(DIST), P(DIST)),
        out_specs=P(None, PIX, None),
        check_vma=False,
    )
```

```python
import math

import jax
import jax.numpy as jnp
import numpy as np
from jax import lax
from jax.experimental import pallas as pl
from jax.experimental.pallas import tpu as pltpu
from jax.sharding import Mesh
from jax.sharding import PartitionSpec as P

ABSORB_RATIO = 0.1
REGULARIZER = 0.05
SIZE = 2048
LONG = 128
SHORT = 16
NDIST = 4
WIDE = 4
VMEM_LIMIT = 8 << 20
DIST = ("l", "c")
PIX = ("z", "x", "h")
PIX_SIZES = (8, 4, 4)
BACK_ORDER = np.arange(LONG).reshape(PIX_SIZES).transpose(2, 1, 0).reshape(-1)


def angle_tables(left, right, period):
    turns = np.outer(np.arange(left), np.arange(right)) % period
    angles = 2.0 * np.pi * turns / period
    return np.cos(angles), np.sin(angles)


def right_table():
    cosine, sine = angle_tables(SHORT, SHORT, SHORT)
    same = np.eye(WIDE)
    c, s = np.kron(same, cosine), np.kron(same, sine)
    return np.block([[c, -s], [s, c]])


def turn_lanes(table):
    half = table.shape[0] // 2
    return np.concatenate([-table[half:], table[:half]], axis=0)


def turn_after(table):
    half = table.shape[1] // 2
    return np.concatenate([table[:, half:], -table[:, :half]], axis=1)


COS, SIN = angle_tables(LONG, LONG, LONG)
RIGHT = right_table()
BACK = np.array(RIGHT.T)
ROW_TWIST = angle_tables(SHORT, LONG, SIZE)
COL_TWIST = tuple(np.tile(t, (1, 2 * WIDE)) for t in angle_tables(LONG, SHORT, SIZE))


def f32(x):
    return np.asarray(x, np.float32)


def split_table(x):
    high = np.asarray(x, jnp.bfloat16)
    return np.stack([high, np.asarray(x - high.astype(np.float64), jnp.bfloat16)])


ROW_FORWARD = split_table(np.concatenate([COS, SIN], axis=1))
COL_FORWARD = split_table(np.concatenate([COS, SIN], axis=0))
COL_RIGHT = split_table(np.concatenate([RIGHT, turn_lanes(RIGHT)], axis=0))
COL_LEFT = split_table(np.concatenate([BACK, turn_after(BACK)], axis=1))
COL_BACK = split_table(np.concatenate([COS, -SIN], axis=1)[BACK_ORDER])
ROW_BACK = split_table(np.concatenate([COS[BACK_ORDER], -SIN[BACK_ORDER]], axis=0))
ROW_TW = f32(np.stack(ROW_TWIST))
COL_TW = f32(np.stack(COL_TWIST))


def halves(x):
    high = x.astype(jnp.bfloat16)
    return high, (x - high.astype(jnp.float32)).astype(jnp.bfloat16)


def joined(parts, axis):
    return tuple(jnp.concatenate([p[i] for p in parts], axis=axis) for i in range(2))


def product(a, b, a_dim=1, b_dim=0):
    def one(x, y):
        return lax.dot_general(
            x, y, (((a_dim,), (b_dim,)), ((), ())), preferred_element_type=jnp.float32
        )

    return one(a[0], b[0]) + (one(a[0], b[1]) + one(a[1], b[0]))


def four_point(z, sign):
    (r0, i0), (r1, i1), (r2, i2), (r3, i3) = z
    ar, ai, br, bi = r0 + r2, i0 + i2, r0 - r2, i0 - i2
    cr, ci, dr, di = r1 + r3, i1 + i3, r1 - r3, i1 - i3
    if sign > 0:
        plus, minus = (br + di, bi - dr), (br - di, bi + dr)
    else:
        plus, minus = (br - di, bi + dr), (br + di, bi - dr)
    return [(ar + cr, ai + ci), plus, (ar - cr, ai - ci), minus]


def times(z, turns, sign):
    r, i = z
    if turns == 0:
        return z
    c = float(np.float32(math.cos(2 * math.pi * turns / 16)))
    s = float(np.float32(sign * math.sin(2 * math.pi * turns / 16)))
    return r * c + i * s, i * c - r * s


def sixteen_point(z, sign):
    inner = [four_point([z[4 * a + b] for a in range(4)], sign) for b in range(4)]
    out = [None] * 16
    for c in range(4):
        mixed = four_point([times(inner[b][c], b * c, sign) for b in range(4)], sign)
        for e in range(4):
            out[c + 4 * e] = mixed[e]
    return out


def row_forward(images, table, twist):
    z = [(images[0][:, LONG * j : LONG * (j + 1)], images[1][:, LONG * j : LONG * (j + 1)]) for j in range(SHORT)]
    spread = sixteen_point(z, 1)
    turned = []
    for j, (r, i) in enumerate(spread):
        c, s = twist[0][j : j + 1, :], twist[1][j : j + 1, :]
        turned.append((r * c + i * s, i * c - r * s))
    out = []
    for d in range(NDIST):
        part = turned[WIDE * d : WIDE * (d + 1)]
        re, im = [r for r, _ in part], [i for _, i in part]
        re, im = halves(jnp.concatenate(re, axis=0)), halves(jnp.concatenate(im, axis=0))
        minus = tuple(-r for r in re)
        both = joined([joined([re, im], 0), joined([im, minus], 0)], 1)
        out.append(product(table, both, 1, 1))
    return jnp.concatenate(out, axis=0)


def wave(turns):
    r = turns - jnp.floor(turns + 0.5)
    r = jnp.where(r > 0.25, 0.5 - r, jnp.where(r < -0.25, -0.5 - r, r))
    x = r * (2.0 * math.pi)
    y = x * x
    p = -1.0 / 39916800.0
    for term in (1.0 / 362880.0, -1.0 / 5040.0, 1.0 / 120.0, -1.0 / 6.0, 1.0):
        p = p * y + term
    return x * p


def signed_square(index):
    shifted = jnp.where(2 * index >= SIZE, index - SIZE, index)
    fraction = shifted.astype(jnp.float32) * (1.0 / SIZE)
    return fraction * fraction


def gains(defocus, blurring, first_col):
    shape = (LONG, LONG)
    lane = lax.broadcasted_iota(jnp.int32, shape, 1)
    row = lax.broadcasted_iota(jnp.int32, shape, 0)
    squared = signed_square(row + LONG * (lane & 15)) + signed_square(first_col + ((lane >> 4) & 3))
    low = lane < LONG // 2
    amplitude = math.sqrt(1.0 + ABSORB_RATIO * ABSORB_RATIO)
    shift = math.atan(ABSORB_RATIO) / (2.0 * math.pi)
    out = []
    for d in range(0, NDIST, 2):
        focus = jnp.where(low, defocus[d], defocus[d + 1]) * (1.0 / (2.0 * math.pi))
        blur = jnp.where(low, blurring[d], blurring[d + 1])
        g = (amplitude * jnp.exp(-blur * squared)) * wave(focus * squared + shift)
        other = jnp.concatenate([g[:, LONG // 2 :], g[:, : LONG // 2]], axis=1)
        out += [jnp.where(low, g, other), jnp.where(low, other, g)]
    return out


def column_middle(blocks, gain, forward, right, left, back, twist):
    c, s = twist[0], twist[1]
    parts = []
    for x in blocks:
        both = product(forward, halves(x))
        u, v = both[:LONG], both[LONG:]
        parts.append(joined([halves(u * c - v * s), halves(v * c + u * s)], 1))
    spectra = product(joined(parts, 0), right)
    numerator = gain[0] * spectra[:LONG]
    weight = gain[0] * gain[0]
    for d in range(1, NDIST):
        numerator = numerator + gain[d] * spectra[LONG * d : LONG * (d + 1)]
        weight = weight + gain[d] * gain[d]
    quotient = numerator / (2.0 * (weight + REGULARIZER))
    both = product(halves(quotient), left)
    a, b = both[:, :LONG], both[:, LONG:]
    upright = joined([halves(a * c - b * s), halves(b * c + a * s)], 0)
    return product(back, upright)


def row_back(x, table, twist):
    z = []
    scale = 1.0 / (SIZE * SIZE)
    for d in range(NDIST):
        start = LONG * (2 * (d % 2) + d // 2)
        half = LONG // 2
        t = halves(x[start : start + LONG].T)
        turned = joined([tuple(p[half:] for p in t), tuple(-p[:half] for p in t)], 0)
        o = product(joined([t, turned], 1), table)
        for j in range(WIDE):
            r = o[SHORT * j : SHORT * (j + 1)]
            i = o[half + SHORT * j : half + SHORT * (j + 1)]
            v = WIDE * d + j
            c, s = twist[0][v : v + 1, :] * scale, twist[1][v : v + 1, :] * scale
            z.append((r * c - i * s, i * c + r * s))
    return sixteen_point(z, -1)


def first_kernel(images, table, twist, out):
    out[...] = row_forward(images[...], table[...], twist[...])


def middle_kernel(par, x, forward, right, left, back, twist, out):
    first_col = SHORT * lax.axis_index(PIX) + WIDE * lax.axis_index(DIST)
    defocus = [par[d : d + 1, :1] for d in range(NDIST)]
    blurring = [par[d : d + 1, 1:] for d in range(NDIST)]
    table = gains(defocus, blurring, first_col)
    blocks = [x[LONG * d : LONG * (d + 1), :] for d in range(NDIST)]
    y = column_middle(blocks, table, forward[...], right[...], left[...], back[...], twist[...])
    out[:LONG, :] = y
    out[LONG:, :] = y


def last_kernel(x, table, twist, out):
    for j, (r, i) in enumerate(row_back(x[...], table[...], twist[...])):
        out[0, :, LONG * j : LONG * (j + 1)] = r
        out[1, :, LONG * j : LONG * (j + 1)] = i


def call(kernel, shapes, name, limit=VMEM_LIMIT):
    def run(*args):
        return pl.pallas_call(
            kernel,
            out_shape=[jax.ShapeDtypeStruct(shape, jnp.float32) for shape in shapes],
            in_specs=[pl.BlockSpec(memory_space=pltpu.VMEM) for _ in args],
            out_specs=[pl.BlockSpec(memory_space=pltpu.VMEM) for _ in shapes],
            compiler_params=pltpu.CompilerParams(vmem_limit_bytes=limit),
            name=name,
        )(*args)

    return run


def exchange(x, axes):
    return lax.all_to_all(x.reshape(x.shape[0], 1, LONG), axes, 0, 0, tiled=True).reshape(x.shape)


def body(contrast, defocus, blurring):
    rows = NDIST * LONG
    (sent,) = call(first_kernel, ((rows, LONG),), "rows_forward", None)(contrast[0], ROW_FORWARD, ROW_TW)
    par = lax.all_gather(jnp.stack([defocus, blurring], axis=1), DIST, axis=0, tiled=True)
    got = exchange(sent, DIST + PIX)
    (middle,) = call(middle_kernel, ((2 * LONG, LONG),), "columns")(
        par, got, COL_FORWARD, COL_RIGHT, COL_LEFT, COL_BACK, COL_TW
    )
    bands = exchange(middle, ("l", "h", "x", "z"))
    whole = lax.all_gather(bands, "c", axis=0, tiled=True)
    return call(last_kernel, ((2, SHORT, SIZE),), "rows_back")(whole, ROW_BACK, ROW_TW)[0]


def solution(mesh):
    parts = Mesh(mesh.devices.reshape((2, 2) + PIX_SIZES), DIST + PIX)
    return jax.shard_map(
        body,
        mesh=parts,
        in_specs=(P(DIST, None, PIX, None), P(DIST), P(DIST)),
        out_specs=P(None, PIX, None),
        check_vma=False,
    )
```

```python
import math

import jax
import jax.numpy as jnp
import numpy as np
from jax import lax
from jax.experimental import pallas as pl
from jax.experimental.pallas import tpu as pltpu
from jax.sharding import Mesh
from jax.sharding import PartitionSpec as P

ABSORB_RATIO = 0.1
REGULARIZER = 0.05
SIZE = 2048
LONG = 128
SHORT = 16
NDIST = 4
WIDE = 4
VMEM_LIMIT = 8 << 20
DIST = ("l", "c")
PIX = ("z", "x", "h")
PIX_SIZES = (8, 4, 4)


def angle_tables(left, right, period):
    turns = np.outer(np.arange(left), np.arange(right)) % period
    angles = 2.0 * np.pi * turns / period
    return np.cos(angles), np.sin(angles)


def right_table():
    cosine, sine = angle_tables(SHORT, SHORT, SHORT)
    same = np.eye(WIDE)
    c, s = np.kron(same, cosine), np.kron(same, sine)
    return np.block([[c, -s], [s, c]])


def turn_lanes(table):
    half = table.shape[0] // 2
    return np.concatenate([-table[half:], table[:half]], axis=0)


def turn_after(table):
    half = table.shape[1] // 2
    return np.concatenate([table[:, half:], -table[:, :half]], axis=1)


COS, SIN = angle_tables(LONG, LONG, LONG)
RIGHT = right_table()
BACK = np.array(RIGHT.T)
ROW_TWIST = angle_tables(SHORT, LONG, SIZE)
COL_TWIST = tuple(np.tile(t, (1, 2 * WIDE)) for t in angle_tables(LONG, SHORT, SIZE))


def f32(x):
    return np.asarray(x, np.float32)


def split_table(x):
    high = np.asarray(x, jnp.bfloat16)
    return np.stack([high, np.asarray(x - high.astype(np.float64), jnp.bfloat16)])


ROW_FORWARD = split_table(np.concatenate([COS, SIN], axis=1))
COL_FORWARD = split_table(np.concatenate([COS, SIN], axis=0))
COL_RIGHT = split_table(np.concatenate([RIGHT, turn_lanes(RIGHT)], axis=0))
COL_LEFT = split_table(np.concatenate([BACK, turn_after(BACK)], axis=1))
COL_BACK = split_table(np.concatenate([COS, -SIN], axis=1))
ROW_BACK = split_table(np.concatenate([COS, -SIN], axis=0))
ROW_TW = f32(np.stack(ROW_TWIST))
COL_TW = f32(np.stack(COL_TWIST))


def halves(x):
    high = x.astype(jnp.bfloat16)
    return high, (x - high.astype(jnp.float32)).astype(jnp.bfloat16)


def joined(parts, axis):
    return tuple(jnp.concatenate([p[i] for p in parts], axis=axis) for i in range(2))


def product(a, b, a_dim=1, b_dim=0):
    def one(x, y):
        return lax.dot_general(
            x, y, (((a_dim,), (b_dim,)), ((), ())), preferred_element_type=jnp.float32
        )

    return one(a[0], b[0]) + (one(a[0], b[1]) + one(a[1], b[0]))


def four_point(z, sign):
    (r0, i0), (r1, i1), (r2, i2), (r3, i3) = z
    ar, ai, br, bi = r0 + r2, i0 + i2, r0 - r2, i0 - i2
    cr, ci, dr, di = r1 + r3, i1 + i3, r1 - r3, i1 - i3
    if sign > 0:
        plus, minus = (br + di, bi - dr), (br - di, bi + dr)
    else:
        plus, minus = (br - di, bi + dr), (br + di, bi - dr)
    return [(ar + cr, ai + ci), plus, (ar - cr, ai - ci), minus]


def times(z, turns, sign):
    r, i = z
    if turns == 0:
        return z
    c = float(np.float32(math.cos(2 * math.pi * turns / 16)))
    s = float(np.float32(sign * math.sin(2 * math.pi * turns / 16)))
    return r * c + i * s, i * c - r * s


def sixteen_point(z, sign):
    inner = [four_point([z[4 * a + b] for a in range(4)], sign) for b in range(4)]
    out = [None] * 16
    for c in range(4):
        mixed = four_point([times(inner[b][c], b * c, sign) for b in range(4)], sign)
        for e in range(4):
            out[c + 4 * e] = mixed[e]
    return out


def row_forward(images, table, twist):
    z = [(images[0][:, LONG * j : LONG * (j + 1)], images[1][:, LONG * j : LONG * (j + 1)]) for j in range(SHORT)]
    spread = sixteen_point(z, 1)
    turned = []
    for j, (r, i) in enumerate(spread):
        c, s = twist[0][j : j + 1, :], twist[1][j : j + 1, :]
        turned.append((r * c + i * s, i * c - r * s))
    out = []
    for d in range(NDIST):
        part = turned[WIDE * d : WIDE * (d + 1)]
        re, im = [r for r, _ in part], [i for _, i in part]
        re, im = halves(jnp.concatenate(re, axis=0)), halves(jnp.concatenate(im, axis=0))
        minus = tuple(-r for r in re)
        both = joined([joined([re, im], 0), joined([im, minus], 0)], 1)
        out.append(product(table, both, 1, 1))
    return jnp.concatenate(out, axis=0)


def wave(turns):
    r = turns - jnp.floor(turns + 0.5)
    r = jnp.where(r > 0.25, 0.5 - r, jnp.where(r < -0.25, -0.5 - r, r))
    x = r * (2.0 * math.pi)
    y = x * x
    p = -1.0 / 39916800.0
    for term in (1.0 / 362880.0, -1.0 / 5040.0, 1.0 / 120.0, -1.0 / 6.0, 1.0):
        p = p * y + term
    return x * p


def signed_square(index):
    shifted = jnp.where(2 * index >= SIZE, index - SIZE, index)
    fraction = shifted.astype(jnp.float32) * (1.0 / SIZE)
    return fraction * fraction


def gains(defocus, blurring, first_col):
    shape = (LONG, LONG)
    lane = lax.broadcasted_iota(jnp.int32, shape, 1)
    row = lax.broadcasted_iota(jnp.int32, shape, 0)
    squared = signed_square(row + LONG * (lane & 15)) + signed_square(first_col + ((lane >> 4) & 3))
    low = lane < LONG // 2
    amplitude = math.sqrt(1.0 + ABSORB_RATIO * ABSORB_RATIO)
    shift = math.atan(ABSORB_RATIO) / (2.0 * math.pi)
    out = []
    for d in range(0, NDIST, 2):
        focus = jnp.where(low, defocus[d], defocus[d + 1]) * (1.0 / (2.0 * math.pi))
        blur = jnp.where(low, blurring[d], blurring[d + 1])
        g = (amplitude * jnp.exp(-blur * squared)) * wave(focus * squared + shift)
        other = jnp.concatenate([g[:, LONG // 2 :], g[:, : LONG // 2]], axis=1)
        out += [jnp.where(low, g, other), jnp.where(low, other, g)]
    return out


def column_middle(blocks, gain, forward, right, left, back, twist):
    c, s = twist[0], twist[1]
    parts = []
    for x in blocks:
        both = product(forward, halves(x))
        u, v = both[:LONG], both[LONG:]
        parts.append(joined([halves(u * c - v * s), halves(v * c + u * s)], 1))
    spectra = product(joined(parts, 0), right)
    numerator = gain[0] * spectra[:LONG]
    weight = gain[0] * gain[0]
    for d in range(1, NDIST):
        numerator = numerator + gain[d] * spectra[LONG * d : LONG * (d + 1)]
        weight = weight + gain[d] * gain[d]
    quotient = numerator / (2.0 * (weight + REGULARIZER))
    both = product(halves(quotient), left)
    a, b = both[:, :LONG], both[:, LONG:]
    upright = joined([halves(a * c - b * s), halves(b * c + a * s)], 0)
    return product(back, upright)


def row_back(x, table, twist):
    z = []
    scale = 1.0 / (SIZE * SIZE)
    for d in range(NDIST):
        start = LONG * (2 * (d % 2) + d // 2)
        half = LONG // 2
        t = halves(x[start : start + LONG].T)
        turned = joined([tuple(p[half:] for p in t), tuple(-p[:half] for p in t)], 0)
        o = product(joined([t, turned], 1), table)
        for j in range(WIDE):
            r = o[SHORT * j : SHORT * (j + 1)]
            i = o[half + SHORT * j : half + SHORT * (j + 1)]
            v = WIDE * d + j
            c, s = twist[0][v : v + 1, :] * scale, twist[1][v : v + 1, :] * scale
            z.append((r * c - i * s, i * c + r * s))
    return sixteen_point(z, -1)


def first_kernel(images, table, twist, out):
    out[...] = row_forward(images[...], table[...], twist[...])


def middle_kernel(par, x, forward, right, left, back, twist, out):
    first_col = SHORT * lax.axis_index(PIX) + WIDE * lax.axis_index(DIST)
    defocus = [par[d : d + 1, :1] for d in range(NDIST)]
    blurring = [par[d : d + 1, 1:] for d in range(NDIST)]
    table = gains(defocus, blurring, first_col)
    blocks = [x[LONG * d : LONG * (d + 1), :] for d in range(NDIST)]
    y = column_middle(blocks, table, forward[...], right[...], left[...], back[...], twist[...])
    out[:LONG, :] = y
    out[LONG:, :] = y


def last_kernel(x, table, twist, out):
    for j, (r, i) in enumerate(row_back(x[...], table[...], twist[...])):
        out[0, :, LONG * j : LONG * (j + 1)] = r
        out[1, :, LONG * j : LONG * (j + 1)] = i


def call(kernel, shapes, name, limit=VMEM_LIMIT):
    def run(*args):
        return pl.pallas_call(
            kernel,
            out_shape=[jax.ShapeDtypeStruct(shape, jnp.float32) for shape in shapes],
            in_specs=[pl.BlockSpec(memory_space=pltpu.VMEM) for _ in args],
            out_specs=[pl.BlockSpec(memory_space=pltpu.VMEM) for _ in shapes],
            compiler_params=pltpu.CompilerParams(vmem_limit_bytes=limit),
            name=name,
        )(*args)

    return run


def exchange(x, axes):
    return lax.all_to_all(x.reshape(x.shape[0], 1, LONG), axes, 0, 0, tiled=True).reshape(x.shape)


def body(contrast, defocus, blurring):
    rows = NDIST * LONG
    (sent,) = call(first_kernel, ((rows, LONG),), "rows_forward", None)(contrast[0], ROW_FORWARD, ROW_TW)
    par = lax.all_gather(jnp.stack([defocus, blurring], axis=1), DIST, axis=0, tiled=True)
    got = exchange(sent, DIST + PIX)
    (middle,) = call(middle_kernel, ((2 * LONG, LONG),), "columns")(
        par, got, COL_FORWARD, COL_RIGHT, COL_LEFT, COL_BACK, COL_TW
    )
    bands = exchange(middle, ("l",) + PIX)
    whole = lax.all_gather(bands, "c", axis=0, tiled=True)
    return call(last_kernel, ((2, SHORT, SIZE),), "rows_back")(whole, ROW_BACK, ROW_TW)[0]


def solution(mesh):
    parts = Mesh(mesh.devices.reshape((2, 2) + PIX_SIZES), DIST + PIX)
    return jax.shard_map(
        body,
        mesh=parts,
        in_specs=(P(DIST, None, PIX, None), P(DIST), P(DIST)),
        out_specs=P(None, PIX, None),
        check_vma=False,
    )
```

```python
import math

import jax
import jax.numpy as jnp
import numpy as np
from jax import lax
from jax.experimental import pallas as pl
from jax.experimental.pallas import tpu as pltpu
from jax.sharding import Mesh
from jax.sharding import PartitionSpec as P

ABSORB_RATIO = 0.1
REGULARIZER = 0.05
SIZE = 2048
LONG = 128
SHORT = 16
NDIST = 4
WIDE = 4
VMEM_LIMIT = 8 << 20
DIST = ("l", "c")
PIX = ("z", "x", "h")
PIX_SIZES = (8, 4, 4)
FLAT = DIST + PIX


def far_first():
    z, x, h = np.unravel_index(np.arange(LONG), PIX_SIZES)
    hops = np.minimum(z, 8 - z) + np.minimum(x, 4 - x) + 2 * np.minimum(h, 4 - h)
    hops[0] = 99
    return np.argsort(-hops, kind="stable")


BACK_ORDER = far_first()


def back_groups():
    return [[(2 * low + core) * LONG + int(k) for k in BACK_ORDER for low in range(2)] for core in range(2)]


def angle_tables(left, right, period):
    turns = np.outer(np.arange(left), np.arange(right)) % period
    angles = 2.0 * np.pi * turns / period
    return np.cos(angles), np.sin(angles)


def right_table():
    cosine, sine = angle_tables(SHORT, SHORT, SHORT)
    same = np.eye(WIDE)
    c, s = np.kron(same, cosine), np.kron(same, sine)
    return np.block([[c, -s], [s, c]])


def turn_lanes(table):
    half = table.shape[0] // 2
    return np.concatenate([-table[half:], table[:half]], axis=0)


def turn_after(table):
    half = table.shape[1] // 2
    return np.concatenate([table[:, half:], -table[:, :half]], axis=1)


COS, SIN = angle_tables(LONG, LONG, LONG)
RIGHT = right_table()
BACK = np.array(RIGHT.T)
ROW_TWIST = angle_tables(SHORT, LONG, SIZE)
COL_TWIST = tuple(np.tile(t, (1, 2 * WIDE)) for t in angle_tables(LONG, SHORT, SIZE))


def f32(x):
    return np.asarray(x, np.float32)


def split_table(x):
    high = np.asarray(x, jnp.bfloat16)
    return np.stack([high, np.asarray(x - high.astype(np.float64), jnp.bfloat16)])


ROW_FORWARD = split_table(np.concatenate([COS, SIN], axis=1))
COL_FORWARD = split_table(np.concatenate([COS, SIN], axis=0))
COL_RIGHT = split_table(np.concatenate([RIGHT, turn_lanes(RIGHT)], axis=0))
COL_LEFT = split_table(np.concatenate([BACK, turn_after(BACK)], axis=1))
COL_BACK = split_table(np.concatenate([COS, -SIN], axis=1)[BACK_ORDER])
ROW_BACK = split_table(np.concatenate([COS[BACK_ORDER], -SIN[BACK_ORDER]], axis=0))
ROW_TW = f32(np.stack(ROW_TWIST))
COL_TW = f32(np.stack(COL_TWIST))


def halves(x):
    high = x.astype(jnp.bfloat16)
    return high, (x - high.astype(jnp.float32)).astype(jnp.bfloat16)


def joined(parts, axis):
    return tuple(jnp.concatenate([p[i] for p in parts], axis=axis) for i in range(2))


def product(a, b, a_dim=1, b_dim=0):
    def one(x, y):
        return lax.dot_general(
            x, y, (((a_dim,), (b_dim,)), ((), ())), preferred_element_type=jnp.float32
        )

    return one(a[0], b[0]) + (one(a[0], b[1]) + one(a[1], b[0]))


def four_point(z, sign):
    (r0, i0), (r1, i1), (r2, i2), (r3, i3) = z
    ar, ai, br, bi = r0 + r2, i0 + i2, r0 - r2, i0 - i2
    cr, ci, dr, di = r1 + r3, i1 + i3, r1 - r3, i1 - i3
    if sign > 0:
        plus, minus = (br + di, bi - dr), (br - di, bi + dr)
    else:
        plus, minus = (br - di, bi + dr), (br + di, bi - dr)
    return [(ar + cr, ai + ci), plus, (ar - cr, ai - ci), minus]


def times(z, turns, sign):
    r, i = z
    if turns == 0:
        return z
    c = float(np.float32(math.cos(2 * math.pi * turns / 16)))
    s = float(np.float32(sign * math.sin(2 * math.pi * turns / 16)))
    return r * c + i * s, i * c - r * s


def sixteen_point(z, sign):
    inner = [four_point([z[4 * a + b] for a in range(4)], sign) for b in range(4)]
    out = [None] * 16
    for c in range(4):
        mixed = four_point([times(inner[b][c], b * c, sign) for b in range(4)], sign)
        for e in range(4):
            out[c + 4 * e] = mixed[e]
    return out


def row_forward(images, table, twist):
    z = [(images[0][:, LONG * j : LONG * (j + 1)], images[1][:, LONG * j : LONG * (j + 1)]) for j in range(SHORT)]
    spread = sixteen_point(z, 1)
    turned = []
    for j, (r, i) in enumerate(spread):
        c, s = twist[0][j : j + 1, :], twist[1][j : j + 1, :]
        turned.append((r * c + i * s, i * c - r * s))
    out = []
    for d in range(NDIST):
        part = turned[WIDE * d : WIDE * (d + 1)]
        re, im = [r for r, _ in part], [i for _, i in part]
        re, im = halves(jnp.concatenate(re, axis=0)), halves(jnp.concatenate(im, axis=0))
        minus = tuple(-r for r in re)
        both = joined([joined([re, im], 0), joined([im, minus], 0)], 1)
        out.append(product(table, both, 1, 1))
    return jnp.concatenate(out, axis=0)


def wave(turns):
    r = turns - jnp.floor(turns + 0.5)
    r = jnp.where(r > 0.25, 0.5 - r, jnp.where(r < -0.25, -0.5 - r, r))
    x = r * (2.0 * math.pi)
    y = x * x
    p = -1.0 / 39916800.0
    for term in (1.0 / 362880.0, -1.0 / 5040.0, 1.0 / 120.0, -1.0 / 6.0, 1.0):
        p = p * y + term
    return x * p


def signed_square(index):
    shifted = jnp.where(2 * index >= SIZE, index - SIZE, index)
    fraction = shifted.astype(jnp.float32) * (1.0 / SIZE)
    return fraction * fraction


def gains(defocus, blurring, first_col):
    shape = (LONG, LONG)
    lane = lax.broadcasted_iota(jnp.int32, shape, 1)
    row = lax.broadcasted_iota(jnp.int32, shape, 0)
    squared = signed_square(row + LONG * (lane & 15)) + signed_square(first_col + ((lane >> 4) & 3))
    low = lane < LONG // 2
    amplitude = math.sqrt(1.0 + ABSORB_RATIO * ABSORB_RATIO)
    shift = math.atan(ABSORB_RATIO) / (2.0 * math.pi)
    out = []
    for d in range(0, NDIST, 2):
        focus = jnp.where(low, defocus[d], defocus[d + 1]) * (1.0 / (2.0 * math.pi))
        blur = jnp.where(low, blurring[d], blurring[d + 1])
        g = (amplitude * jnp.exp(-blur * squared)) * wave(focus * squared + shift)
        other = jnp.concatenate([g[:, LONG // 2 :], g[:, : LONG // 2]], axis=1)
        out += [jnp.where(low, g, other), jnp.where(low, other, g)]
    return out


def column_middle(blocks, gain, forward, right, left, back, twist):
    c, s = twist[0], twist[1]
    parts = []
    for x in blocks:
        both = product(forward, halves(x))
        u, v = both[:LONG], both[LONG:]
        parts.append(joined([halves(u * c - v * s), halves(v * c + u * s)], 1))
    spectra = product(joined(parts, 0), right)
    numerator = gain[0] * spectra[:LONG]
    weight = gain[0] * gain[0]
    for d in range(1, NDIST):
        numerator = numerator + gain[d] * spectra[LONG * d : LONG * (d + 1)]
        weight = weight + gain[d] * gain[d]
    quotient = numerator / (2.0 * (weight + REGULARIZER))
    both = product(halves(quotient), left)
    a, b = both[:, :LONG], both[:, LONG:]
    upright = joined([halves(a * c - b * s), halves(b * c + a * s)], 0)
    return product(back, upright)


def row_back(blocks, table, twist):
    z = []
    scale = 1.0 / (SIZE * SIZE)
    for d in range(NDIST):
        half = LONG // 2
        t = halves(blocks[d].T)
        turned = joined([tuple(p[half:] for p in t), tuple(-p[:half] for p in t)], 0)
        o = product(joined([t, turned], 1), table)
        for j in range(WIDE):
            r = o[SHORT * j : SHORT * (j + 1)]
            i = o[half + SHORT * j : half + SHORT * (j + 1)]
            v = WIDE * d + j
            c, s = twist[0][v : v + 1, :] * scale, twist[1][v : v + 1, :] * scale
            z.append((r * c - i * s, i * c + r * s))
    return sixteen_point(z, -1)


def first_kernel(images, table, twist, out):
    out[...] = row_forward(images[...], table[...], twist[...])


def middle_kernel(par, x, forward, right, left, back, twist, out):
    first_col = SHORT * lax.axis_index(PIX) + WIDE * lax.axis_index(DIST)
    defocus = [par[d : d + 1, :1] for d in range(NDIST)]
    blurring = [par[d : d + 1, 1:] for d in range(NDIST)]
    table = gains(defocus, blurring, first_col)
    blocks = [x[LONG * d : LONG * (d + 1), :] for d in range(NDIST)]
    y = column_middle(blocks, table, forward[...], right[...], left[...], back[...], twist[...])
    for low in range(2):
        out[pl.ds(low, LONG, stride=2), :] = y


def last_kernel(x, table, twist, out):
    blocks = [x[pl.ds(2 * LONG * (d % 2) + d // 2, LONG, stride=2), :] for d in range(NDIST)]
    for j, (r, i) in enumerate(row_back(blocks, table[...], twist[...])):
        out[0, :, LONG * j : LONG * (j + 1)] = r
        out[1, :, LONG * j : LONG * (j + 1)] = i


def call(kernel, shapes, name, limit=VMEM_LIMIT):
    def run(*args):
        return pl.pallas_call(
            kernel,
            out_shape=[jax.ShapeDtypeStruct(shape, jnp.float32) for shape in shapes],
            in_specs=[pl.BlockSpec(memory_space=pltpu.VMEM) for _ in args],
            out_specs=[pl.BlockSpec(memory_space=pltpu.VMEM) for _ in shapes],
            compiler_params=pltpu.CompilerParams(vmem_limit_bytes=limit),
            name=name,
        )(*args)

    return run


def exchange(x, groups=None):
    sent = x.reshape(x.shape[0], 1, LONG)
    return lax.all_to_all(sent, FLAT, 0, 0, axis_index_groups=groups, tiled=True).reshape(x.shape)


def body(contrast, defocus, blurring):
    rows = NDIST * LONG
    (sent,) = call(first_kernel, ((rows, LONG),), "rows_forward", None)(contrast[0], ROW_FORWARD, ROW_TW)
    par = lax.all_gather(jnp.stack([defocus, blurring], axis=1), DIST, axis=0, tiled=True)
    got = exchange(sent)
    (middle,) = call(middle_kernel, ((2 * LONG, LONG),), "columns")(
        par, got, COL_FORWARD, COL_RIGHT, COL_LEFT, COL_BACK, COL_TW
    )
    bands = exchange(middle, back_groups())
    whole = lax.all_gather(bands, "c", axis=0, tiled=True)
    return call(last_kernel, ((2, SHORT, SIZE),), "rows_back")(whole, ROW_BACK, ROW_TW)[0]


def solution(mesh):
    parts = Mesh(mesh.devices.reshape((2, 2) + PIX_SIZES), FLAT)
    return jax.shard_map(
        body,
        mesh=parts,
        in_specs=(P(DIST, None, PIX, None), P(DIST), P(DIST)),
        out_specs=P(None, PIX, None),
        check_vma=False,
    )
```

```python
import math

import jax
import jax.numpy as jnp
import numpy as np
from jax import lax
from jax.experimental import pallas as pl
from jax.experimental.pallas import tpu as pltpu
from jax.sharding import Mesh
from jax.sharding import PartitionSpec as P

ABSORB_RATIO = 0.1
REGULARIZER = 0.05
SIZE = 2048
LONG = 128
SHORT = 16
NDIST = 4
WIDE = 4
VMEM_LIMIT = 8 << 20
DIST = ("l", "c")
PIX = ("z", "x", "h")
PIX_SIZES = (8, 4, 4)
FLAT = DIST + PIX


FIRST = (7, 2, 2)


def far_first():
    place = np.unravel_index(np.arange(LONG), PIX_SIZES)
    z, x, h = [np.abs(p - f) for p, f in zip(place, FIRST)]
    hops = np.minimum(z, 8 - z) + np.minimum(x, 4 - x) + 2 * np.minimum(h, 4 - h)
    hops[np.ravel_multi_index(FIRST, PIX_SIZES)] = 99
    return np.argsort(-hops, kind="stable")


ORDER = far_first()


def all_groups():
    return [[LONG * d + int(k) for d in range(NDIST) for k in ORDER]]


def back_groups():
    return [[(2 * low + core) * LONG + int(k) for k in ORDER for low in range(2)] for core in range(2)]


def angle_tables(left, right, period):
    turns = np.outer(np.arange(left), np.arange(right)) % period
    angles = 2.0 * np.pi * turns / period
    return np.cos(angles), np.sin(angles)


def right_table():
    cosine, sine = angle_tables(SHORT, SHORT, SHORT)
    same = np.eye(WIDE)
    c, s = np.kron(same, cosine), np.kron(same, sine)
    return np.block([[c, -s], [s, c]])


def turn_lanes(table):
    half = table.shape[0] // 2
    return np.concatenate([-table[half:], table[:half]], axis=0)


def turn_after(table):
    half = table.shape[1] // 2
    return np.concatenate([table[:, half:], -table[:, :half]], axis=1)


COS, SIN = angle_tables(LONG, LONG, LONG)
RIGHT = right_table()
BACK = np.array(RIGHT.T)
ROW_TWIST = angle_tables(SHORT, LONG, SIZE)
COL_TWIST = tuple(np.tile(t, (1, 2 * WIDE)) for t in angle_tables(LONG, SHORT, SIZE))


def f32(x):
    return np.asarray(x, np.float32)


def split_table(x):
    high = np.asarray(x, jnp.bfloat16)
    return np.stack([high, np.asarray(x - high.astype(np.float64), jnp.bfloat16)])


ROW_FORWARD = split_table(np.concatenate([COS, SIN], axis=1)[ORDER])
COL_FORWARD = split_table(np.concatenate([COS[:, ORDER], SIN[:, ORDER]], axis=0))
COL_RIGHT = split_table(np.concatenate([RIGHT, turn_lanes(RIGHT)], axis=0))
COL_LEFT = split_table(np.concatenate([BACK, turn_after(BACK)], axis=1))
COL_BACK = split_table(np.concatenate([COS, -SIN], axis=1)[ORDER])
ROW_BACK = split_table(np.concatenate([COS[ORDER], -SIN[ORDER]], axis=0))
ROW_TW = f32(np.stack(ROW_TWIST))
COL_TW = f32(np.stack(COL_TWIST))


def halves(x):
    high = x.astype(jnp.bfloat16)
    return high, (x - high.astype(jnp.float32)).astype(jnp.bfloat16)


def joined(parts, axis):
    return tuple(jnp.concatenate([p[i] for p in parts], axis=axis) for i in range(2))


def product(a, b, a_dim=1, b_dim=0):
    def one(x, y):
        return lax.dot_general(
            x, y, (((a_dim,), (b_dim,)), ((), ())), preferred_element_type=jnp.float32
        )

    return one(a[0], b[0]) + (one(a[0], b[1]) + one(a[1], b[0]))


def four_point(z, sign):
    (r0, i0), (r1, i1), (r2, i2), (r3, i3) = z
    ar, ai, br, bi = r0 + r2, i0 + i2, r0 - r2, i0 - i2
    cr, ci, dr, di = r1 + r3, i1 + i3, r1 - r3, i1 - i3
    if sign > 0:
        plus, minus = (br + di, bi - dr), (br - di, bi + dr)
    else:
        plus, minus = (br - di, bi + dr), (br + di, bi - dr)
    return [(ar + cr, ai + ci), plus, (ar - cr, ai - ci), minus]


def times(z, turns, sign):
    r, i = z
    if turns == 0:
        return z
    c = float(np.float32(math.cos(2 * math.pi * turns / 16)))
    s = float(np.float32(sign * math.sin(2 * math.pi * turns / 16)))
    return r * c + i * s, i * c - r * s


def sixteen_point(z, sign):
    inner = [four_point([z[4 * a + b] for a in range(4)], sign) for b in range(4)]
    out = [None] * 16
    for c in range(4):
        mixed = four_point([times(inner[b][c], b * c, sign) for b in range(4)], sign)
        for e in range(4):
            out[c + 4 * e] = mixed[e]
    return out


def row_forward(images, table, twist):
    z = [(images[0][:, LONG * j : LONG * (j + 1)], images[1][:, LONG * j : LONG * (j + 1)]) for j in range(SHORT)]
    spread = sixteen_point(z, 1)
    turned = []
    for j, (r, i) in enumerate(spread):
        c, s = twist[0][j : j + 1, :], twist[1][j : j + 1, :]
        turned.append((r * c + i * s, i * c - r * s))
    out = []
    for d in range(NDIST):
        part = turned[WIDE * d : WIDE * (d + 1)]
        re, im = [r for r, _ in part], [i for _, i in part]
        re, im = halves(jnp.concatenate(re, axis=0)), halves(jnp.concatenate(im, axis=0))
        minus = tuple(-r for r in re)
        both = joined([joined([re, im], 0), joined([im, minus], 0)], 1)
        out.append(product(table, both, 1, 1))
    return jnp.concatenate(out, axis=0)


def wave(turns):
    r = turns - jnp.floor(turns + 0.5)
    r = jnp.where(r > 0.25, 0.5 - r, jnp.where(r < -0.25, -0.5 - r, r))
    x = r * (2.0 * math.pi)
    y = x * x
    p = -1.0 / 39916800.0
    for term in (1.0 / 362880.0, -1.0 / 5040.0, 1.0 / 120.0, -1.0 / 6.0, 1.0):
        p = p * y + term
    return x * p


def signed_square(index):
    shifted = jnp.where(2 * index >= SIZE, index - SIZE, index)
    fraction = shifted.astype(jnp.float32) * (1.0 / SIZE)
    return fraction * fraction


def gains(defocus, blurring, first_col):
    shape = (LONG, LONG)
    lane = lax.broadcasted_iota(jnp.int32, shape, 1)
    row = lax.broadcasted_iota(jnp.int32, shape, 0)
    squared = signed_square(row + LONG * (lane & 15)) + signed_square(first_col + ((lane >> 4) & 3))
    low = lane < LONG // 2
    amplitude = math.sqrt(1.0 + ABSORB_RATIO * ABSORB_RATIO)
    shift = math.atan(ABSORB_RATIO) / (2.0 * math.pi)
    out = []
    for d in range(0, NDIST, 2):
        focus = jnp.where(low, defocus[d], defocus[d + 1]) * (1.0 / (2.0 * math.pi))
        blur = jnp.where(low, blurring[d], blurring[d + 1])
        g = (amplitude * jnp.exp(-blur * squared)) * wave(focus * squared + shift)
        other = jnp.concatenate([g[:, LONG // 2 :], g[:, : LONG // 2]], axis=1)
        out += [jnp.where(low, g, other), jnp.where(low, other, g)]
    return out


def column_middle(blocks, gain, forward, right, left, back, twist):
    c, s = twist[0], twist[1]
    parts = []
    for x in blocks:
        both = product(forward, halves(x))
        u, v = both[:LONG], both[LONG:]
        parts.append(joined([halves(u * c - v * s), halves(v * c + u * s)], 1))
    spectra = product(joined(parts, 0), right)
    numerator = gain[0] * spectra[:LONG]
    weight = gain[0] * gain[0]
    for d in range(1, NDIST):
        numerator = numerator + gain[d] * spectra[LONG * d : LONG * (d + 1)]
        weight = weight + gain[d] * gain[d]
    quotient = numerator / (2.0 * (weight + REGULARIZER))
    both = product(halves(quotient), left)
    a, b = both[:, :LONG], both[:, LONG:]
    upright = joined([halves(a * c - b * s), halves(b * c + a * s)], 0)
    return product(back, upright)


def row_back(blocks, table, twist):
    z = []
    scale = 1.0 / (SIZE * SIZE)
    for d in range(NDIST):
        half = LONG // 2
        t = halves(blocks[d].T)
        turned = joined([tuple(p[half:] for p in t), tuple(-p[:half] for p in t)], 0)
        o = product(joined([t, turned], 1), table)
        for j in range(WIDE):
            r = o[SHORT * j : SHORT * (j + 1)]
            i = o[half + SHORT * j : half + SHORT * (j + 1)]
            v = WIDE * d + j
            c, s = twist[0][v : v + 1, :] * scale, twist[1][v : v + 1, :] * scale
            z.append((r * c - i * s, i * c + r * s))
    return sixteen_point(z, -1)


def first_kernel(images, table, twist, out):
    out[...] = row_forward(images[...], table[...], twist[...])


def middle_kernel(par, x, forward, right, left, back, twist, out):
    first_col = SHORT * lax.axis_index(PIX) + WIDE * lax.axis_index(DIST)
    defocus = [par[d : d + 1, :1] for d in range(NDIST)]
    blurring = [par[d : d + 1, 1:] for d in range(NDIST)]
    table = gains(defocus, blurring, first_col)
    blocks = [x[LONG * d : LONG * (d + 1), :] for d in range(NDIST)]
    y = column_middle(blocks, table, forward[...], right[...], left[...], back[...], twist[...])
    for low in range(2):
        out[pl.ds(low, LONG, stride=2), :] = y


def last_kernel(x, table, twist, out):
    blocks = [x[pl.ds(2 * LONG * (d % 2) + d // 2, LONG, stride=2), :] for d in range(NDIST)]
    for j, (r, i) in enumerate(row_back(blocks, table[...], twist[...])):
        out[0, :, LONG * j : LONG * (j + 1)] = r
        out[1, :, LONG * j : LONG * (j + 1)] = i


def call(kernel, shapes, name, limit=VMEM_LIMIT):
    def run(*args):
        return pl.pallas_call(
            kernel,
            out_shape=[jax.ShapeDtypeStruct(shape, jnp.float32) for shape in shapes],
            in_specs=[pl.BlockSpec(memory_space=pltpu.VMEM) for _ in args],
            out_specs=[pl.BlockSpec(memory_space=pltpu.VMEM) for _ in shapes],
            compiler_params=pltpu.CompilerParams(vmem_limit_bytes=limit),
            name=name,
        )(*args)

    return run


def exchange(x, groups):
    sent = x.reshape(x.shape[0], 1, LONG)
    return lax.all_to_all(sent, FLAT, 0, 0, axis_index_groups=groups, tiled=True).reshape(x.shape)


def body(contrast, defocus, blurring):
    rows = NDIST * LONG
    (sent,) = call(first_kernel, ((rows, LONG),), "rows_forward", None)(contrast[0], ROW_FORWARD, ROW_TW)
    par = lax.all_gather(jnp.stack([defocus, blurring], axis=1), DIST, axis=0, tiled=True)
    got = exchange(sent, all_groups())
    (middle,) = call(middle_kernel, ((2 * LONG, LONG),), "columns")(
        par, got, COL_FORWARD, COL_RIGHT, COL_LEFT, COL_BACK, COL_TW
    )
    bands = exchange(middle, back_groups())
    whole = lax.all_gather(bands, "c", axis=0, tiled=True)
    return call(last_kernel, ((2, SHORT, SIZE),), "rows_back")(whole, ROW_BACK, ROW_TW)[0]


def solution(mesh):
    parts = Mesh(mesh.devices.reshape((2, 2) + PIX_SIZES), FLAT)
    return jax.shard_map(
        body,
        mesh=parts,
        in_specs=(P(DIST, None, PIX, None), P(DIST), P(DIST)),
        out_specs=P(None, PIX, None),
        check_vma=False,
    )
```

```python
import math

import jax
import jax.numpy as jnp
import numpy as np
from jax import lax
from jax.experimental import pallas as pl
from jax.experimental.pallas import tpu as pltpu
from jax.sharding import Mesh
from jax.sharding import PartitionSpec as P

ABSORB_RATIO = 0.1
REGULARIZER = 0.05
SIZE = 2048
LONG = 128
SHORT = 16
NDIST = 4
WIDE = 4
VMEM_LIMIT = 8 << 20
DIST = ("l", "c")
PIX = ("z", "x", "h")
PIX_SIZES = (8, 4, 4)
FLAT = DIST + PIX


FIRST = (7, 2, 2)


def far_first():
    place = np.unravel_index(np.arange(LONG), PIX_SIZES)
    z, x, h = [np.abs(p - f) for p, f in zip(place, FIRST)]
    hops = np.minimum(z, 8 - z) + np.minimum(x, 4 - x) + 2 * np.minimum(h, 4 - h)
    hops[np.ravel_multi_index(FIRST, PIX_SIZES)] = 99
    return np.argsort(-hops, kind="stable")


ORDER = far_first()


def chip_groups():
    return [[(2 * low + core) * LONG + int(k) for k in ORDER for low in range(2)] for core in range(2)]


def angle_tables(left, right, period):
    turns = np.outer(np.arange(left), np.arange(right)) % period
    angles = 2.0 * np.pi * turns / period
    return np.cos(angles), np.sin(angles)


def right_table():
    cosine, sine = angle_tables(SHORT, SHORT, SHORT)
    same = np.eye(WIDE)
    c, s = np.kron(same, cosine), np.kron(same, sine)
    return np.block([[c, -s], [s, c]])


def turn_lanes(table):
    half = table.shape[0] // 2
    return np.concatenate([-table[half:], table[:half]], axis=0)


def turn_after(table):
    half = table.shape[1] // 2
    return np.concatenate([table[:, half:], -table[:, :half]], axis=1)


COS, SIN = angle_tables(LONG, LONG, LONG)
RIGHT = right_table()
BACK = np.array(RIGHT.T)
ROW_TWIST = angle_tables(SHORT, LONG, SIZE)
COL_TWIST = tuple(np.tile(t, (1, 2 * WIDE)) for t in angle_tables(LONG, SHORT, SIZE))


def f32(x):
    return np.asarray(x, np.float32)


def split_table(x):
    high = np.asarray(x, jnp.bfloat16)
    return np.stack([high, np.asarray(x - high.astype(np.float64), jnp.bfloat16)])


ROW_FORWARD = split_table(np.concatenate([COS, SIN], axis=1)[ORDER])
COL_FORWARD = split_table(np.concatenate([COS[:, ORDER], SIN[:, ORDER]], axis=0))
COL_RIGHT = split_table(np.concatenate([RIGHT, turn_lanes(RIGHT)], axis=0))
COL_LEFT = split_table(np.concatenate([BACK, turn_after(BACK)], axis=1))
COL_BACK = split_table(np.concatenate([COS, -SIN], axis=1)[ORDER])
ROW_BACK = split_table(np.concatenate([COS[ORDER], -SIN[ORDER]], axis=0))
ROW_TW = f32(np.stack(ROW_TWIST))
COL_TW = f32(np.stack(COL_TWIST))


def halves(x):
    high = x.astype(jnp.bfloat16)
    return high, (x - high.astype(jnp.float32)).astype(jnp.bfloat16)


def joined(parts, axis):
    return tuple(jnp.concatenate([p[i] for p in parts], axis=axis) for i in range(2))


def product(a, b, a_dim=1, b_dim=0):
    def one(x, y):
        return lax.dot_general(
            x, y, (((a_dim,), (b_dim,)), ((), ())), preferred_element_type=jnp.float32
        )

    return one(a[0], b[0]) + (one(a[0], b[1]) + one(a[1], b[0]))


def four_point(z, sign):
    (r0, i0), (r1, i1), (r2, i2), (r3, i3) = z
    ar, ai, br, bi = r0 + r2, i0 + i2, r0 - r2, i0 - i2
    cr, ci, dr, di = r1 + r3, i1 + i3, r1 - r3, i1 - i3
    if sign > 0:
        plus, minus = (br + di, bi - dr), (br - di, bi + dr)
    else:
        plus, minus = (br - di, bi + dr), (br + di, bi - dr)
    return [(ar + cr, ai + ci), plus, (ar - cr, ai - ci), minus]


def times(z, turns, sign):
    r, i = z
    if turns == 0:
        return z
    c = float(np.float32(math.cos(2 * math.pi * turns / 16)))
    s = float(np.float32(sign * math.sin(2 * math.pi * turns / 16)))
    return r * c + i * s, i * c - r * s


def sixteen_point(z, sign):
    inner = [four_point([z[4 * a + b] for a in range(4)], sign) for b in range(4)]
    out = [None] * 16
    for c in range(4):
        mixed = four_point([times(inner[b][c], b * c, sign) for b in range(4)], sign)
        for e in range(4):
            out[c + 4 * e] = mixed[e]
    return out


def row_forward(images, table, twist):
    z = [(images[0][:, LONG * j : LONG * (j + 1)], images[1][:, LONG * j : LONG * (j + 1)]) for j in range(SHORT)]
    spread = sixteen_point(z, 1)
    turned = []
    for j, (r, i) in enumerate(spread):
        c, s = twist[0][j : j + 1, :], twist[1][j : j + 1, :]
        turned.append((r * c + i * s, i * c - r * s))
    out = []
    for d in range(NDIST):
        part = turned[WIDE * d : WIDE * (d + 1)]
        re, im = [r for r, _ in part], [i for _, i in part]
        re, im = halves(jnp.concatenate(re, axis=0)), halves(jnp.concatenate(im, axis=0))
        minus = tuple(-r for r in re)
        both = joined([joined([re, im], 0), joined([im, minus], 0)], 1)
        out.append(product(table, both, 1, 1))
    return out


def wave(turns):
    r = turns - jnp.floor(turns + 0.5)
    r = jnp.where(r > 0.25, 0.5 - r, jnp.where(r < -0.25, -0.5 - r, r))
    x = r * (2.0 * math.pi)
    y = x * x
    p = -1.0 / 39916800.0
    for term in (1.0 / 362880.0, -1.0 / 5040.0, 1.0 / 120.0, -1.0 / 6.0, 1.0):
        p = p * y + term
    return x * p


def signed_square(index):
    shifted = jnp.where(2 * index >= SIZE, index - SIZE, index)
    fraction = shifted.astype(jnp.float32) * (1.0 / SIZE)
    return fraction * fraction


def gains(defocus, blurring, first_col):
    shape = (LONG, LONG)
    lane = lax.broadcasted_iota(jnp.int32, shape, 1)
    row = lax.broadcasted_iota(jnp.int32, shape, 0)
    squared = signed_square(row + LONG * (lane & 15)) + signed_square(first_col + ((lane >> 4) & 3))
    low = lane < LONG // 2
    amplitude = math.sqrt(1.0 + ABSORB_RATIO * ABSORB_RATIO)
    shift = math.atan(ABSORB_RATIO) / (2.0 * math.pi)
    out = []
    for d in range(0, NDIST, 2):
        focus = jnp.where(low, defocus[d], defocus[d + 1]) * (1.0 / (2.0 * math.pi))
        blur = jnp.where(low, blurring[d], blurring[d + 1])
        g = (amplitude * jnp.exp(-blur * squared)) * wave(focus * squared + shift)
        other = jnp.concatenate([g[:, LONG // 2 :], g[:, : LONG // 2]], axis=1)
        out += [jnp.where(low, g, other), jnp.where(low, other, g)]
    return out


def column_middle(blocks, gain, forward, right, left, back, twist):
    c, s = twist[0], twist[1]
    parts = []
    for x in blocks:
        both = product(forward, halves(x))
        u, v = both[:LONG], both[LONG:]
        parts.append(joined([halves(u * c - v * s), halves(v * c + u * s)], 1))
    spectra = product(joined(parts, 0), right)
    numerator = gain[0] * spectra[:LONG]
    weight = gain[0] * gain[0]
    for d in range(1, NDIST):
        numerator = numerator + gain[d] * spectra[LONG * d : LONG * (d + 1)]
        weight = weight + gain[d] * gain[d]
    quotient = numerator / (2.0 * (weight + REGULARIZER))
    both = product(halves(quotient), left)
    a, b = both[:, :LONG], both[:, LONG:]
    upright = joined([halves(a * c - b * s), halves(b * c + a * s)], 0)
    return product(back, upright)


def row_back(blocks, table, twist):
    z = []
    scale = 1.0 / (SIZE * SIZE)
    for d in range(NDIST):
        half = LONG // 2
        t = halves(blocks[d].T)
        turned = joined([tuple(p[half:] for p in t), tuple(-p[:half] for p in t)], 0)
        o = product(joined([t, turned], 1), table)
        for j in range(WIDE):
            r = o[SHORT * j : SHORT * (j + 1)]
            i = o[half + SHORT * j : half + SHORT * (j + 1)]
            v = WIDE * d + j
            c, s = twist[0][v : v + 1, :] * scale, twist[1][v : v + 1, :] * scale
            z.append((r * c - i * s, i * c + r * s))
    return sixteen_point(z, -1)


def first_kernel(images, table, twist, out):
    for d, band in enumerate(row_forward(images[...], table[...], twist[...])):
        out[pl.ds(d, LONG, stride=NDIST), :] = band


def middle_kernel(par, x, forward, right, left, back, twist, out):
    first_col = SHORT * lax.axis_index(PIX) + WIDE * lax.axis_index(DIST)
    defocus = [par[d : d + 1, :1] for d in range(NDIST)]
    blurring = [par[d : d + 1, 1:] for d in range(NDIST)]
    table = gains(defocus, blurring, first_col)
    core = lax.axis_index("c")
    blocks = []
    for d in range(NDIST):
        start = NDIST * LONG * (d % 2) + 2 * (d // 2) + core
        blocks.append(x[pl.ds(start, LONG, stride=NDIST), :])
    y = column_middle(blocks, table, forward[...], right[...], left[...], back[...], twist[...])
    for low in range(2):
        out[pl.ds(low, LONG, stride=2), :] = y


def last_kernel(x, table, twist, out):
    blocks = [x[pl.ds(2 * LONG * (d % 2) + d // 2, LONG, stride=2), :] for d in range(NDIST)]
    for j, (r, i) in enumerate(row_back(blocks, table[...], twist[...])):
        out[0, :, LONG * j : LONG * (j + 1)] = r
        out[1, :, LONG * j : LONG * (j + 1)] = i


def call(kernel, shapes, name, limit=VMEM_LIMIT):
    def run(*args):
        return pl.pallas_call(
            kernel,
            out_shape=[jax.ShapeDtypeStruct(shape, jnp.float32) for shape in shapes],
            in_specs=[pl.BlockSpec(memory_space=pltpu.VMEM) for _ in args],
            out_specs=[pl.BlockSpec(memory_space=pltpu.VMEM) for _ in shapes],
            compiler_params=pltpu.CompilerParams(vmem_limit_bytes=limit),
            name=name,
        )(*args)

    return run


def exchange(x):
    sent = x.reshape(2 * LONG, -1, LONG)
    got = lax.all_to_all(sent, FLAT, 0, 0, axis_index_groups=chip_groups(), tiled=True)
    return lax.all_gather(got.reshape(x.shape), "c", axis=0, tiled=True)


def body(contrast, defocus, blurring):
    rows = NDIST * LONG
    (sent,) = call(first_kernel, ((rows, LONG),), "rows_forward", None)(contrast[0], ROW_FORWARD, ROW_TW)
    par = lax.all_gather(jnp.stack([defocus, blurring], axis=1), DIST, axis=0, tiled=True)
    got = exchange(sent)
    (middle,) = call(middle_kernel, ((2 * LONG, LONG),), "columns")(
        par, got, COL_FORWARD, COL_RIGHT, COL_LEFT, COL_BACK, COL_TW
    )
    whole = exchange(middle)
    return call(last_kernel, ((2, SHORT, SIZE),), "rows_back")(whole, ROW_BACK, ROW_TW)[0]


def solution(mesh):
    parts = Mesh(mesh.devices.reshape((2, 2) + PIX_SIZES), FLAT)
    return jax.shard_map(
        body,
        mesh=parts,
        in_specs=(P(DIST, None, PIX, None), P(DIST), P(DIST)),
        out_specs=P(None, PIX, None),
        check_vma=False,
    )
```

```python
import math

import jax
import jax.numpy as jnp
import numpy as np
from jax import lax
from jax.experimental import pallas as pl
from jax.experimental.pallas import tpu as pltpu
from jax.sharding import Mesh
from jax.sharding import PartitionSpec as P

ABSORB_RATIO = 0.1
REGULARIZER = 0.05
SIZE = 2048
LONG = 128
SHORT = 16
NDIST = 4
WIDE = 4
VMEM_LIMIT = 8 << 20
DIST = ("l", "c")
PIX = ("z", "x", "h")
PIX_SIZES = (8, 4, 4)
FLAT = DIST + PIX


FIRST = (7, 2, 2)


def far_first():
    place = np.unravel_index(np.arange(LONG), PIX_SIZES)
    z, x, h = [np.abs(p - f) for p, f in zip(place, FIRST)]
    hops = np.minimum(z, 8 - z) + np.minimum(x, 4 - x) + 2 * np.minimum(h, 4 - h)
    hops[np.ravel_multi_index(FIRST, PIX_SIZES)] = 99
    return np.argsort(-hops, kind="stable")


ORDER = far_first()


def chip_groups():
    return [[(2 * low + core) * LONG + int(k) for k in ORDER for low in range(2)] for core in range(2)]


def angle_tables(left, right, period):
    turns = np.outer(np.arange(left), np.arange(right)) % period
    angles = 2.0 * np.pi * turns / period
    return np.cos(angles), np.sin(angles)


def right_table():
    cosine, sine = angle_tables(SHORT, SHORT, SHORT)
    same = np.eye(WIDE)
    c, s = np.kron(same, cosine), np.kron(same, sine)
    return np.block([[c, -s], [s, c]])


def turn_lanes(table):
    half = table.shape[0] // 2
    return np.concatenate([-table[half:], table[:half]], axis=0)


def turn_after(table):
    half = table.shape[1] // 2
    return np.concatenate([table[:, half:], -table[:, :half]], axis=1)


COS, SIN = angle_tables(LONG, LONG, LONG)
RIGHT = right_table()
BACK = np.array(RIGHT.T)
ROW_TWIST = angle_tables(SHORT, LONG, SIZE)
COL_TWIST = tuple(np.tile(t, (1, 2 * WIDE)) for t in angle_tables(LONG, SHORT, SIZE))


def f32(x):
    return np.asarray(x, np.float32)


def split_table(x):
    high = np.asarray(x, jnp.bfloat16)
    return np.stack([high, np.asarray(x - high.astype(np.float64), jnp.bfloat16)])


ROW_FORWARD = split_table(np.concatenate([COS, SIN], axis=1)[ORDER])
COL_FORWARD = split_table(np.concatenate([COS[:, ORDER], SIN[:, ORDER]], axis=0))
COL_RIGHT = split_table(np.concatenate([RIGHT, turn_lanes(RIGHT)], axis=0))
COL_LEFT = split_table(np.concatenate([BACK, turn_after(BACK)], axis=1))
COL_BACK = split_table(np.concatenate([COS, -SIN], axis=1)[ORDER])
ROW_BACK = split_table(np.concatenate([COS[ORDER], -SIN[ORDER]], axis=0))
ROW_TW = f32(np.stack(ROW_TWIST))
COL_TW = f32(np.stack(COL_TWIST))


def halves(x):
    high = x.astype(jnp.bfloat16)
    return high, (x - high.astype(jnp.float32)).astype(jnp.bfloat16)


def joined(parts, axis):
    return tuple(jnp.concatenate([p[i] for p in parts], axis=axis) for i in range(2))


def product(a, b, a_dim=1, b_dim=0):
    def one(x, y):
        return lax.dot_general(
            x, y, (((a_dim,), (b_dim,)), ((), ())), preferred_element_type=jnp.float32
        )

    return one(a[0], b[0]) + (one(a[0], b[1]) + one(a[1], b[0]))


def four_point(z, sign):
    (r0, i0), (r1, i1), (r2, i2), (r3, i3) = z
    ar, ai, br, bi = r0 + r2, i0 + i2, r0 - r2, i0 - i2
    cr, ci, dr, di = r1 + r3, i1 + i3, r1 - r3, i1 - i3
    if sign > 0:
        plus, minus = (br + di, bi - dr), (br - di, bi + dr)
    else:
        plus, minus = (br - di, bi + dr), (br + di, bi - dr)
    return [(ar + cr, ai + ci), plus, (ar - cr, ai - ci), minus]


def times(z, turns, sign):
    r, i = z
    if turns == 0:
        return z
    c = float(np.float32(math.cos(2 * math.pi * turns / 16)))
    s = float(np.float32(sign * math.sin(2 * math.pi * turns / 16)))
    return r * c + i * s, i * c - r * s


def sixteen_point(z, sign):
    inner = [four_point([z[4 * a + b] for a in range(4)], sign) for b in range(4)]
    out = [None] * 16
    for c in range(4):
        mixed = four_point([times(inner[b][c], b * c, sign) for b in range(4)], sign)
        for e in range(4):
            out[c + 4 * e] = mixed[e]
    return out


def row_forward(images, table, twist):
    z = [(images[0][:, LONG * j : LONG * (j + 1)], images[1][:, LONG * j : LONG * (j + 1)]) for j in range(SHORT)]
    spread = sixteen_point(z, 1)
    turned = []
    for j, (r, i) in enumerate(spread):
        c, s = twist[0][j : j + 1, :], twist[1][j : j + 1, :]
        turned.append((r * c + i * s, i * c - r * s))
    out = []
    for d in range(NDIST):
        part = turned[WIDE * d : WIDE * (d + 1)]
        re, im = [r for r, _ in part], [i for _, i in part]
        re, im = halves(jnp.concatenate(re, axis=0)), halves(jnp.concatenate(im, axis=0))
        minus = tuple(-r for r in re)
        both = joined([joined([re, im], 0), joined([im, minus], 0)], 1)
        out.append(product(table, both, 1, 1))
    return out


def wave(turns):
    r = turns - jnp.floor(turns + 0.5)
    r = jnp.where(r > 0.25, 0.5 - r, jnp.where(r < -0.25, -0.5 - r, r))
    x = r * (2.0 * math.pi)
    y = x * x
    p = -1.0 / 39916800.0
    for term in (1.0 / 362880.0, -1.0 / 5040.0, 1.0 / 120.0, -1.0 / 6.0, 1.0):
        p = p * y + term
    return x * p


def signed_square(index):
    shifted = jnp.where(2 * index >= SIZE, index - SIZE, index)
    fraction = shifted.astype(jnp.float32) * (1.0 / SIZE)
    return fraction * fraction


def gains(defocus, blurring, first_col):
    shape = (LONG, LONG)
    lane = lax.broadcasted_iota(jnp.int32, shape, 1)
    row = lax.broadcasted_iota(jnp.int32, shape, 0)
    squared = signed_square(row + LONG * (lane & 15)) + signed_square(first_col + ((lane >> 4) & 3))
    low = lane < LONG // 2
    amplitude = math.sqrt(1.0 + ABSORB_RATIO * ABSORB_RATIO)
    shift = math.atan(ABSORB_RATIO) / (2.0 * math.pi)
    out = []
    for d in range(0, NDIST, 2):
        focus = jnp.where(low, defocus[d], defocus[d + 1]) * (1.0 / (2.0 * math.pi))
        blur = jnp.where(low, blurring[d], blurring[d + 1])
        g = (amplitude * jnp.exp(-blur * squared)) * wave(focus * squared + shift)
        other = jnp.concatenate([g[:, LONG // 2 :], g[:, : LONG // 2]], axis=1)
        out += [jnp.where(low, g, other), jnp.where(low, other, g)]
    return out


def column_middle(blocks, gain, forward, right, left, back, twist):
    c, s = twist[0], twist[1]
    parts = []
    for x in blocks:
        both = product(forward, halves(x))
        u, v = both[:LONG], both[LONG:]
        parts.append(joined([halves(u * c - v * s), halves(v * c + u * s)], 1))
    spectra = product(joined(parts, 0), right)
    quotient = gain[0] * spectra[:LONG]
    for d in range(1, NDIST):
        quotient = quotient + gain[d] * spectra[LONG * d : LONG * (d + 1)]
    both = product(halves(quotient), left)
    a, b = both[:, :LONG], both[:, LONG:]
    upright = joined([halves(a * c - b * s), halves(b * c + a * s)], 0)
    return product(back, upright)


def row_back(blocks, table, twist):
    z = []
    scale = 1.0 / (SIZE * SIZE)
    for d in range(NDIST):
        half = LONG // 2
        t = halves(blocks[d].T)
        turned = joined([tuple(p[half:] for p in t), tuple(-p[:half] for p in t)], 0)
        o = product(joined([t, turned], 1), table)
        for j in range(WIDE):
            r = o[SHORT * j : SHORT * (j + 1)]
            i = o[half + SHORT * j : half + SHORT * (j + 1)]
            v = WIDE * d + j
            c, s = twist[0][v : v + 1, :] * scale, twist[1][v : v + 1, :] * scale
            z.append((r * c - i * s, i * c + r * s))
    return sixteen_point(z, -1)


def first_kernel(images, table, twist, out):
    for d, band in enumerate(row_forward(images[...], table[...], twist[...])):
        out[pl.ds(d, LONG, stride=NDIST), :] = band


def gain_kernel(par, out):
    first_col = SHORT * lax.axis_index(PIX) + WIDE * lax.axis_index(DIST)
    defocus = [par[d : d + 1, :1] for d in range(NDIST)]
    blurring = [par[d : d + 1, 1:] for d in range(NDIST)]
    table = gains(defocus, blurring, first_col)
    weight = table[0] * table[0]
    for g in table[1:]:
        weight = weight + g * g
    share = 0.5 / (weight + REGULARIZER)
    for d, g in enumerate(table):
        out[d, :, :] = g * share


def middle_kernel(gain, x, forward, right, left, back, twist, out):
    core = lax.axis_index("c")
    blocks = []
    for d in range(NDIST):
        start = NDIST * LONG * (d % 2) + 2 * (d // 2) + core
        blocks.append(x[pl.ds(start, LONG, stride=NDIST), :])
    y = column_middle(blocks, gain[...], forward[...], right[...], left[...], back[...], twist[...])
    for low in range(2):
        out[pl.ds(low, LONG, stride=2), :] = y


def last_kernel(x, table, twist, out):
    blocks = [x[pl.ds(2 * LONG * (d % 2) + d // 2, LONG, stride=2), :] for d in range(NDIST)]
    for j, (r, i) in enumerate(row_back(blocks, table[...], twist[...])):
        out[0, :, LONG * j : LONG * (j + 1)] = r
        out[1, :, LONG * j : LONG * (j + 1)] = i


def call(kernel, shapes, name, limit=VMEM_LIMIT):
    def run(*args):
        return pl.pallas_call(
            kernel,
            out_shape=[jax.ShapeDtypeStruct(shape, jnp.float32) for shape in shapes],
            in_specs=[pl.BlockSpec(memory_space=pltpu.VMEM) for _ in args],
            out_specs=[pl.BlockSpec(memory_space=pltpu.VMEM) for _ in shapes],
            compiler_params=pltpu.CompilerParams(vmem_limit_bytes=limit),
            name=name,
        )(*args)

    return run


def exchange(x):
    sent = x.reshape(2 * LONG, -1, LONG)
    got = lax.all_to_all(sent, FLAT, 0, 0, axis_index_groups=chip_groups(), tiled=True)
    return lax.all_gather(got.reshape(x.shape), "c", axis=0, tiled=True)


def body(contrast, defocus, blurring):
    rows = NDIST * LONG
    (sent,) = call(first_kernel, ((rows, LONG),), "rows_forward", None)(contrast[0], ROW_FORWARD, ROW_TW)
    par = lax.all_gather(jnp.stack([defocus, blurring], axis=1), DIST, axis=0, tiled=True)
    got = exchange(sent)
    (gain,) = call(gain_kernel, ((NDIST, LONG, LONG),), "gains")(par)
    (middle,) = call(middle_kernel, ((2 * LONG, LONG),), "columns")(
        gain, got, COL_FORWARD, COL_RIGHT, COL_LEFT, COL_BACK, COL_TW
    )
    whole = exchange(middle)
    return call(last_kernel, ((2, SHORT, SIZE),), "rows_back")(whole, ROW_BACK, ROW_TW)[0]


def solution(mesh):
    parts = Mesh(mesh.devices.reshape((2, 2) + PIX_SIZES), FLAT)
    return jax.shard_map(
        body,
        mesh=parts,
        in_specs=(P(DIST, None, PIX, None), P(DIST), P(DIST)),
        out_specs=P(None, PIX, None),
        check_vma=False,
    )
```

```python
import math

import jax
import jax.numpy as jnp
import numpy as np
from jax import lax
from jax.experimental import pallas as pl
from jax.experimental.pallas import tpu as pltpu
from jax.sharding import Mesh
from jax.sharding import PartitionSpec as P

ABSORB_RATIO = 0.1
REGULARIZER = 0.05
SIZE = 2048
LONG = 128
SHORT = 16
NDIST = 4
WIDE = 4
VMEM_LIMIT = 8 << 20
DIST = ("l", "c")
PIX = ("z", "x", "h")
PIX_SIZES = (8, 4, 4)
FLAT = DIST + PIX


FIRST = (5, 2, 2)


def far_first():
    place = np.unravel_index(np.arange(LONG), PIX_SIZES)
    z, x, h = [np.abs(p - f) for p, f in zip(place, FIRST)]
    hops = np.minimum(z, 8 - z) + np.minimum(x, 4 - x) + 2 * np.minimum(h, 4 - h)
    hops[np.ravel_multi_index(FIRST, PIX_SIZES)] = 99
    return np.argsort(-hops, kind="stable")


ORDER = far_first()


def chip_groups():
    return [[(2 * low + core) * LONG + int(k) for k in ORDER for low in range(2)] for core in range(2)]


def angle_tables(left, right, period):
    turns = np.outer(np.arange(left), np.arange(right)) % period
    angles = 2.0 * np.pi * turns / period
    return np.cos(angles), np.sin(angles)


def right_table():
    cosine, sine = angle_tables(SHORT, SHORT, SHORT)
    same = np.eye(WIDE)
    c, s = np.kron(same, cosine), np.kron(same, sine)
    return np.block([[c, -s], [s, c]])


def turn_lanes(table):
    half = table.shape[0] // 2
    return np.concatenate([-table[half:], table[:half]], axis=0)


def turn_after(table):
    half = table.shape[1] // 2
    return np.concatenate([table[:, half:], -table[:, :half]], axis=1)


COS, SIN = angle_tables(LONG, LONG, LONG)
RIGHT = right_table()
BACK = np.array(RIGHT.T)
ROW_TWIST = angle_tables(SHORT, LONG, SIZE)
COL_TWIST = tuple(np.tile(t, (1, 2 * WIDE)) for t in angle_tables(LONG, SHORT, SIZE))


def f32(x):
    return np.asarray(x, np.float32)


def split_table(x):
    high = np.asarray(x, jnp.bfloat16)
    return np.stack([high, np.asarray(x - high.astype(np.float64), jnp.bfloat16)])


ROW_FORWARD = split_table(np.concatenate([COS, SIN], axis=1)[ORDER])
COL_FORWARD = split_table(np.concatenate([COS[:, ORDER], SIN[:, ORDER]], axis=0))
COL_RIGHT = split_table(np.concatenate([RIGHT, turn_lanes(RIGHT)], axis=0))
COL_LEFT = split_table(np.concatenate([BACK, turn_after(BACK)], axis=1))
COL_BACK = split_table(np.concatenate([COS, -SIN], axis=1)[ORDER])
ROW_BACK = split_table(np.concatenate([COS[ORDER], -SIN[ORDER]], axis=0))
ROW_TW = f32(np.stack(ROW_TWIST))
COL_TW = f32(np.stack(COL_TWIST))


def halves(x):
    high = x.astype(jnp.bfloat16)
    return high, (x - high.astype(jnp.float32)).astype(jnp.bfloat16)


def joined(parts, axis):
    return tuple(jnp.concatenate([p[i] for p in parts], axis=axis) for i in range(2))


def product(a, b, a_dim=1, b_dim=0):
    def one(x, y):
        return lax.dot_general(
            x, y, (((a_dim,), (b_dim,)), ((), ())), preferred_element_type=jnp.float32
        )

    return one(a[0], b[0]) + (one(a[0], b[1]) + one(a[1], b[0]))


def four_point(z, sign):
    (r0, i0), (r1, i1), (r2, i2), (r3, i3) = z
    ar, ai, br, bi = r0 + r2, i0 + i2, r0 - r2, i0 - i2
    cr, ci, dr, di = r1 + r3, i1 + i3, r1 - r3, i1 - i3
    if sign > 0:
        plus, minus = (br + di, bi - dr), (br - di, bi + dr)
    else:
        plus, minus = (br - di, bi + dr), (br + di, bi - dr)
    return [(ar + cr, ai + ci), plus, (ar - cr, ai - ci), minus]


def times(z, turns, sign):
    r, i = z
    if turns == 0:
        return z
    c = float(np.float32(math.cos(2 * math.pi * turns / 16)))
    s = float(np.float32(sign * math.sin(2 * math.pi * turns / 16)))
    return r * c + i * s, i * c - r * s


def sixteen_point(z, sign):
    inner = [four_point([z[4 * a + b] for a in range(4)], sign) for b in range(4)]
    out = [None] * 16
    for c in range(4):
        mixed = four_point([times(inner[b][c], b * c, sign) for b in range(4)], sign)
        for e in range(4):
            out[c + 4 * e] = mixed[e]
    return out


def row_forward(images, table, twist):
    z = [(images[0][:, LONG * j : LONG * (j + 1)], images[1][:, LONG * j : LONG * (j + 1)]) for j in range(SHORT)]
    spread = sixteen_point(z, 1)
    turned = []
    for j, (r, i) in enumerate(spread):
        c, s = twist[0][j : j + 1, :], twist[1][j : j + 1, :]
        turned.append((r * c + i * s, i * c - r * s))
    out = []
    for d in range(NDIST):
        part = turned[WIDE * d : WIDE * (d + 1)]
        re, im = [r for r, _ in part], [i for _, i in part]
        re, im = halves(jnp.concatenate(re, axis=0)), halves(jnp.concatenate(im, axis=0))
        minus = tuple(-r for r in re)
        both = joined([joined([re, im], 0), joined([im, minus], 0)], 1)
        out.append(product(table, both, 1, 1))
    return out


def wave(turns):
    r = turns - jnp.floor(turns + 0.5)
    r = jnp.where(r > 0.25, 0.5 - r, jnp.where(r < -0.25, -0.5 - r, r))
    x = r * (2.0 * math.pi)
    y = x * x
    p = -1.0 / 39916800.0
    for term in (1.0 / 362880.0, -1.0 / 5040.0, 1.0 / 120.0, -1.0 / 6.0, 1.0):
        p = p * y + term
    return x * p


def signed_square(index):
    shifted = jnp.where(2 * index >= SIZE, index - SIZE, index)
    fraction = shifted.astype(jnp.float32) * (1.0 / SIZE)
    return fraction * fraction


def gains(defocus, blurring, first_col):
    shape = (LONG, LONG)
    lane = lax.broadcasted_iota(jnp.int32, shape, 1)
    row = lax.broadcasted_iota(jnp.int32, shape, 0)
    squared = signed_square(row + LONG * (lane & 15)) + signed_square(first_col + ((lane >> 4) & 3))
    low = lane < LONG // 2
    amplitude = math.sqrt(1.0 + ABSORB_RATIO * ABSORB_RATIO)
    shift = math.atan(ABSORB_RATIO) / (2.0 * math.pi)
    out = []
    for d in range(0, NDIST, 2):
        focus = jnp.where(low, defocus[d], defocus[d + 1]) * (1.0 / (2.0 * math.pi))
        blur = jnp.where(low, blurring[d], blurring[d + 1])
        g = (amplitude * jnp.exp(-blur * squared)) * wave(focus * squared + shift)
        other = jnp.concatenate([g[:, LONG // 2 :], g[:, : LONG // 2]], axis=1)
        out += [jnp.where(low, g, other), jnp.where(low, other, g)]
    return out


def column_middle(blocks, gain, forward, right, left, back, twist):
    c, s = twist[0], twist[1]
    parts = []
    for x in blocks:
        both = product(forward, halves(x))
        u, v = both[:LONG], both[LONG:]
        parts.append(joined([halves(u * c - v * s), halves(v * c + u * s)], 1))
    spectra = product(joined(parts, 0), right)
    quotient = gain[0] * spectra[:LONG]
    for d in range(1, NDIST):
        quotient = quotient + gain[d] * spectra[LONG * d : LONG * (d + 1)]
    both = product(halves(quotient), left)
    a, b = both[:, :LONG], both[:, LONG:]
    upright = joined([halves(a * c - b * s), halves(b * c + a * s)], 0)
    return product(back, upright)


def row_back(blocks, table, twist):
    z = []
    scale = 1.0 / (SIZE * SIZE)
    for d in range(NDIST):
        half = LONG // 2
        t = halves(blocks[d].T)
        turned = joined([tuple(p[half:] for p in t), tuple(-p[:half] for p in t)], 0)
        o = product(joined([t, turned], 1), table)
        for j in range(WIDE):
            r = o[SHORT * j : SHORT * (j + 1)]
            i = o[half + SHORT * j : half + SHORT * (j + 1)]
            v = WIDE * d + j
            c, s = twist[0][v : v + 1, :] * scale, twist[1][v : v + 1, :] * scale
            z.append((r * c - i * s, i * c + r * s))
    return sixteen_point(z, -1)


def first_kernel(images, table, twist, out):
    for d, band in enumerate(row_forward(images[...], table[...], twist[...])):
        out[pl.ds(d, LONG, stride=NDIST), :] = band


def gain_kernel(par, out):
    first_col = SHORT * lax.axis_index(PIX) + WIDE * lax.axis_index(DIST)
    defocus = [par[d : d + 1, :1] for d in range(NDIST)]
    blurring = [par[d : d + 1, 1:] for d in range(NDIST)]
    table = gains(defocus, blurring, first_col)
    weight = table[0] * table[0]
    for g in table[1:]:
        weight = weight + g * g
    share = 0.5 / (weight + REGULARIZER)
    for d, g in enumerate(table):
        out[d, :, :] = g * share


def middle_kernel(gain, x, forward, right, left, back, twist, out):
    core = lax.axis_index("c")
    blocks = []
    for d in range(NDIST):
        start = NDIST * LONG * (d % 2) + 2 * (d // 2) + core
        blocks.append(x[pl.ds(start, LONG, stride=NDIST), :])
    y = column_middle(blocks, gain[...], forward[...], right[...], left[...], back[...], twist[...])
    for low in range(2):
        out[pl.ds(low, LONG, stride=2), :] = y


def last_kernel(x, table, twist, out):
    blocks = [x[pl.ds(2 * LONG * (d % 2) + d // 2, LONG, stride=2), :] for d in range(NDIST)]
    for j, (r, i) in enumerate(row_back(blocks, table[...], twist[...])):
        out[0, :, LONG * j : LONG * (j + 1)] = r
        out[1, :, LONG * j : LONG * (j + 1)] = i


def call(kernel, shapes, name, limit=VMEM_LIMIT):
    def run(*args):
        return pl.pallas_call(
            kernel,
            out_shape=[jax.ShapeDtypeStruct(shape, jnp.float32) for shape in shapes],
            in_specs=[pl.BlockSpec(memory_space=pltpu.VMEM) for _ in args],
            out_specs=[pl.BlockSpec(memory_space=pltpu.VMEM) for _ in shapes],
            compiler_params=pltpu.CompilerParams(vmem_limit_bytes=limit),
            name=name,
        )(*args)

    return run


def exchange(x):
    sent = x.reshape(2 * LONG, -1, LONG)
    got = lax.all_to_all(sent, FLAT, 0, 0, axis_index_groups=chip_groups(), tiled=True)
    return lax.all_gather(got.reshape(x.shape), "c", axis=0, tiled=True)


def body(contrast, defocus, blurring):
    rows = NDIST * LONG
    (sent,) = call(first_kernel, ((rows, LONG),), "rows_forward", None)(contrast[0], ROW_FORWARD, ROW_TW)
    par = lax.all_gather(jnp.stack([defocus, blurring], axis=1), DIST, axis=0, tiled=True)
    got = exchange(sent)
    (gain,) = call(gain_kernel, ((NDIST, LONG, LONG),), "gains")(par)
    (middle,) = call(middle_kernel, ((2 * LONG, LONG),), "columns")(
        gain, got, COL_FORWARD, COL_RIGHT, COL_LEFT, COL_BACK, COL_TW
    )
    whole = exchange(middle)
    return call(last_kernel, ((2, SHORT, SIZE),), "rows_back")(whole, ROW_BACK, ROW_TW)[0]


def solution(mesh):
    parts = Mesh(mesh.devices.reshape((2, 2) + PIX_SIZES), FLAT)
    return jax.shard_map(
        body,
        mesh=parts,
        in_specs=(P(DIST, None, PIX, None), P(DIST), P(DIST)),
        out_specs=P(None, PIX, None),
        check_vma=False,
    )
```

```python
import math

import jax
import jax.numpy as jnp
import numpy as np
from jax import lax
from jax.experimental import pallas as pl
from jax.experimental.pallas import tpu as pltpu
from jax.sharding import Mesh
from jax.sharding import PartitionSpec as P

ABSORB_RATIO = 0.1
REGULARIZER = 0.05
SIZE = 2048
LONG = 128
SHORT = 16
NDIST = 4
WIDE = 4
VMEM_LIMIT = 8 << 20
DIST = ("l", "c")
PIX = ("z", "x", "h")
PIX_SIZES = (8, 4, 4)
FLAT = DIST + PIX


FIRST = (4, 2, 2)


def far_first():
    place = np.unravel_index(np.arange(LONG), PIX_SIZES)
    z, x, h = [np.abs(p - f) for p, f in zip(place, FIRST)]
    hops = np.minimum(z, 8 - z) + np.minimum(x, 4 - x) + 2 * np.minimum(h, 4 - h)
    hops[np.ravel_multi_index(FIRST, PIX_SIZES)] = 99
    return np.argsort(-hops, kind="stable")


ORDER = far_first()


def chip_groups():
    return [[(2 * low + core) * LONG + int(k) for k in ORDER for low in range(2)] for core in range(2)]


def angle_tables(left, right, period):
    turns = np.outer(np.arange(left), np.arange(right)) % period
    angles = 2.0 * np.pi * turns / period
    return np.cos(angles), np.sin(angles)


def right_table():
    cosine, sine = angle_tables(SHORT, SHORT, SHORT)
    same = np.eye(WIDE)
    c, s = np.kron(same, cosine), np.kron(same, sine)
    return np.block([[c, -s], [s, c]])


def turn_lanes(table):
    half = table.shape[0] // 2
    return np.concatenate([-table[half:], table[:half]], axis=0)


def turn_after(table):
    half = table.shape[1] // 2
    return np.concatenate([table[:, half:], -table[:, :half]], axis=1)


COS, SIN = angle_tables(LONG, LONG, LONG)
RIGHT = right_table()
BACK = np.array(RIGHT.T)
ROW_TWIST = angle_tables(SHORT, LONG, SIZE)
COL_TWIST = tuple(np.tile(t, (1, 2 * WIDE)) for t in angle_tables(LONG, SHORT, SIZE))


def f32(x):
    return np.asarray(x, np.float32)


def split_table(x):
    high = np.asarray(x, jnp.bfloat16)
    return np.stack([high, np.asarray(x - high.astype(np.float64), jnp.bfloat16)])


ROW_FORWARD = split_table(np.concatenate([COS, SIN], axis=1)[ORDER])
COL_FORWARD = split_table(np.concatenate([COS[:, ORDER], SIN[:, ORDER]], axis=0))
COL_RIGHT = split_table(np.concatenate([RIGHT, turn_lanes(RIGHT)], axis=0))
COL_LEFT = split_table(np.concatenate([BACK, turn_after(BACK)], axis=1))
COL_BACK = split_table(np.concatenate([COS, -SIN], axis=1)[ORDER])
ROW_BACK = split_table(np.concatenate([COS[ORDER], -SIN[ORDER]], axis=0))
ROW_TW = f32(np.stack(ROW_TWIST))
COL_TW = f32(np.stack(COL_TWIST))


def halves(x):
    high = x.astype(jnp.bfloat16)
    return high, (x - high.astype(jnp.float32)).astype(jnp.bfloat16)


def joined(parts, axis):
    return tuple(jnp.concatenate([p[i] for p in parts], axis=axis) for i in range(2))


def product(a, b, a_dim=1, b_dim=0):
    def one(x, y):
        return lax.dot_general(
            x, y, (((a_dim,), (b_dim,)), ((), ())), preferred_element_type=jnp.float32
        )

    return one(a[0], b[0]) + (one(a[0], b[1]) + one(a[1], b[0]))


def four_point(z, sign):
    (r0, i0), (r1, i1), (r2, i2), (r3, i3) = z
    ar, ai, br, bi = r0 + r2, i0 + i2, r0 - r2, i0 - i2
    cr, ci, dr, di = r1 + r3, i1 + i3, r1 - r3, i1 - i3
    if sign > 0:
        plus, minus = (br + di, bi - dr), (br - di, bi + dr)
    else:
        plus, minus = (br - di, bi + dr), (br + di, bi - dr)
    return [(ar + cr, ai + ci), plus, (ar - cr, ai - ci), minus]


def times(z, turns, sign):
    r, i = z
    if turns == 0:
        return z
    c = float(np.float32(math.cos(2 * math.pi * turns / 16)))
    s = float(np.float32(sign * math.sin(2 * math.pi * turns / 16)))
    return r * c + i * s, i * c - r * s


def sixteen_point(z, sign):
    inner = [four_point([z[4 * a + b] for a in range(4)], sign) for b in range(4)]
    out = [None] * 16
    for c in range(4):
        mixed = four_point([times(inner[b][c], b * c, sign) for b in range(4)], sign)
        for e in range(4):
            out[c + 4 * e] = mixed[e]
    return out


def row_forward(images, table, twist):
    z = [(images[0][:, LONG * j : LONG * (j + 1)], images[1][:, LONG * j : LONG * (j + 1)]) for j in range(SHORT)]
    spread = sixteen_point(z, 1)
    turned = []
    for j, (r, i) in enumerate(spread):
        c, s = twist[0][j : j + 1, :], twist[1][j : j + 1, :]
        turned.append((r * c + i * s, i * c - r * s))
    out = []
    for d in range(NDIST):
        part = turned[WIDE * d : WIDE * (d + 1)]
        re, im = [r for r, _ in part], [i for _, i in part]
        re, im = halves(jnp.concatenate(re, axis=0)), halves(jnp.concatenate(im, axis=0))
        minus = tuple(-r for r in re)
        both = joined([joined([re, im], 0), joined([im, minus], 0)], 1)
        out.append(product(table, both, 1, 1))
    return out


def wave(turns):
    r = turns - jnp.floor(turns + 0.5)
    r = jnp.where(r > 0.25, 0.5 - r, jnp.where(r < -0.25, -0.5 - r, r))
    x = r * (2.0 * math.pi)
    y = x * x
    p = -1.0 / 39916800.0
    for term in (1.0 / 362880.0, -1.0 / 5040.0, 1.0 / 120.0, -1.0 / 6.0, 1.0):
        p = p * y + term
    return x * p


def signed_square(index):
    shifted = jnp.where(2 * index >= SIZE, index - SIZE, index)
    fraction = shifted.astype(jnp.float32) * (1.0 / SIZE)
    return fraction * fraction


def gains(defocus, blurring, first_col):
    shape = (LONG, LONG)
    lane = lax.broadcasted_iota(jnp.int32, shape, 1)
    row = lax.broadcasted_iota(jnp.int32, shape, 0)
    squared = signed_square(row + LONG * (lane & 15)) + signed_square(first_col + ((lane >> 4) & 3))
    low = lane < LONG // 2
    amplitude = math.sqrt(1.0 + ABSORB_RATIO * ABSORB_RATIO)
    shift = math.atan(ABSORB_RATIO) / (2.0 * math.pi)
    out = []
    for d in range(0, NDIST, 2):
        focus = jnp.where(low, defocus[d], defocus[d + 1]) * (1.0 / (2.0 * math.pi))
        blur = jnp.where(low, blurring[d], blurring[d + 1])
        g = (amplitude * jnp.exp(-blur * squared)) * wave(focus * squared + shift)
        other = jnp.concatenate([g[:, LONG // 2 :], g[:, : LONG // 2]], axis=1)
        out += [jnp.where(low, g, other), jnp.where(low, other, g)]
    return out


def column_middle(blocks, gain, forward, right, left, back, twist):
    c, s = twist[0], twist[1]
    parts = []
    for x in blocks:
        both = product(forward, halves(x))
        u, v = both[:LONG], both[LONG:]
        parts.append(joined([halves(u * c - v * s), halves(v * c + u * s)], 1))
    spectra = product(joined(parts, 0), right)
    quotient = gain[0] * spectra[:LONG]
    for d in range(1, NDIST):
        quotient = quotient + gain[d] * spectra[LONG * d : LONG * (d + 1)]
    both = product(halves(quotient), left)
    a, b = both[:, :LONG], both[:, LONG:]
    upright = joined([halves(a * c - b * s), halves(b * c + a * s)], 0)
    return product(back, upright)


def row_back(blocks, table, twist):
    z = []
    scale = 1.0 / (SIZE * SIZE)
    for d in range(NDIST):
        half = LONG // 2
        t = halves(blocks[d].T)
        turned = joined([tuple(p[half:] for p in t), tuple(-p[:half] for p in t)], 0)
        o = product(joined([t, turned], 1), table)
        for j in range(WIDE):
            r = o[SHORT * j : SHORT * (j + 1)]
            i = o[half + SHORT * j : half + SHORT * (j + 1)]
            v = WIDE * d + j
            c, s = twist[0][v : v + 1, :] * scale, twist[1][v : v + 1, :] * scale
            z.append((r * c - i * s, i * c + r * s))
    return sixteen_point(z, -1)


def first_kernel(images, table, twist, out):
    for d, band in enumerate(row_forward(images[...], table[...], twist[...])):
        out[pl.ds(d, LONG, stride=NDIST), :] = band


def gain_kernel(par, out):
    first_col = SHORT * lax.axis_index(PIX) + WIDE * lax.axis_index(DIST)
    defocus = [par[d : d + 1, :1] for d in range(NDIST)]
    blurring = [par[d : d + 1, 1:] for d in range(NDIST)]
    table = gains(defocus, blurring, first_col)
    weight = table[0] * table[0]
    for g in table[1:]:
        weight = weight + g * g
    share = 0.5 / (weight + REGULARIZER)
    for d, g in enumerate(table):
        out[d, :, :] = g * share


def middle_kernel(gain, x, forward, right, left, back, twist, out):
    core = lax.axis_index("c")
    blocks = []
    for d in range(NDIST):
        start = NDIST * LONG * (d % 2) + 2 * (d // 2) + core
        blocks.append(x[pl.ds(start, LONG, stride=NDIST), :])
    y = column_middle(blocks, gain[...], forward[...], right[...], left[...], back[...], twist[...])
    for low in range(2):
        out[pl.ds(low, LONG, stride=2), :] = y


def last_kernel(x, table, twist, out):
    blocks = [x[pl.ds(2 * LONG * (d % 2) + d // 2, LONG, stride=2), :] for d in range(NDIST)]
    for j, (r, i) in enumerate(row_back(blocks, table[...], twist[...])):
        out[0, :, LONG * j : LONG * (j + 1)] = r
        out[1, :, LONG * j : LONG * (j + 1)] = i


def call(kernel, shapes, name, limit=VMEM_LIMIT):
    def run(*args):
        return pl.pallas_call(
            kernel,
            out_shape=[jax.ShapeDtypeStruct(shape, jnp.float32) for shape in shapes],
            in_specs=[pl.BlockSpec(memory_space=pltpu.VMEM) for _ in args],
            out_specs=[pl.BlockSpec(memory_space=pltpu.VMEM) for _ in shapes],
            compiler_params=pltpu.CompilerParams(vmem_limit_bytes=limit),
            name=name,
        )(*args)

    return run


def exchange(x):
    sent = x.reshape(2 * LONG, -1, LONG)
    got = lax.all_to_all(sent, FLAT, 0, 0, axis_index_groups=chip_groups(), tiled=True)
    return lax.all_gather(got.reshape(x.shape), "c", axis=0, tiled=True)


def body(contrast, defocus, blurring):
    rows = NDIST * LONG
    (sent,) = call(first_kernel, ((rows, LONG),), "rows_forward", None)(contrast[0], ROW_FORWARD, ROW_TW)
    par = lax.all_gather(jnp.stack([defocus, blurring], axis=1), DIST, axis=0, tiled=True)
    got = exchange(sent)
    (gain,) = call(gain_kernel, ((NDIST, LONG, LONG),), "gains")(par)
    (middle,) = call(middle_kernel, ((2 * LONG, LONG),), "columns")(
        gain, got, COL_FORWARD, COL_RIGHT, COL_LEFT, COL_BACK, COL_TW
    )
    whole = exchange(middle)
    return call(last_kernel, ((2, SHORT, SIZE),), "rows_back")(whole, ROW_BACK, ROW_TW)[0]


def solution(mesh):
    parts = Mesh(mesh.devices.reshape((2, 2) + PIX_SIZES), FLAT)
    return jax.shard_map(
        body,
        mesh=parts,
        in_specs=(P(DIST, None, PIX, None), P(DIST), P(DIST)),
        out_specs=P(None, PIX, None),
        check_vma=False,
    )
```

```python
import math

import jax
import jax.numpy as jnp
import numpy as np
from jax import lax
from jax.experimental import pallas as pl
from jax.experimental.pallas import tpu as pltpu
from jax.sharding import Mesh
from jax.sharding import PartitionSpec as P

ABSORB_RATIO = 0.1
REGULARIZER = 0.05
SIZE = 2048
LONG = 128
SHORT = 16
NDIST = 4
WIDE = 4
VMEM_LIMIT = 8 << 20
DIST = ("l", "c")
PIX = ("z", "x", "h")
PIX_SIZES = (8, 4, 4)
FLAT = DIST + PIX


FIRST_OUT = (5, 2, 2)
FIRST_BACK = (4, 2, 2)


def far_first(first):
    place = np.unravel_index(np.arange(LONG), PIX_SIZES)
    z, x, h = [np.abs(p - f) for p, f in zip(place, first)]
    hops = np.minimum(z, 8 - z) + np.minimum(x, 4 - x) + 2 * np.minimum(h, 4 - h)
    hops[np.ravel_multi_index(first, PIX_SIZES)] = 99
    return np.argsort(-hops, kind="stable")


OUT_ORDER = far_first(FIRST_OUT)
BACK_ORDER = far_first(FIRST_BACK)


def chip_groups(order):
    return [[(2 * low + core) * LONG + int(k) for k in order for low in range(2)] for core in range(2)]


def angle_tables(left, right, period):
    turns = np.outer(np.arange(left), np.arange(right)) % period
    angles = 2.0 * np.pi * turns / period
    return np.cos(angles), np.sin(angles)


def right_table():
    cosine, sine = angle_tables(SHORT, SHORT, SHORT)
    same = np.eye(WIDE)
    c, s = np.kron(same, cosine), np.kron(same, sine)
    return np.block([[c, -s], [s, c]])


def turn_lanes(table):
    half = table.shape[0] // 2
    return np.concatenate([-table[half:], table[:half]], axis=0)


def turn_after(table):
    half = table.shape[1] // 2
    return np.concatenate([table[:, half:], -table[:, :half]], axis=1)


COS, SIN = angle_tables(LONG, LONG, LONG)
RIGHT = right_table()
BACK = np.array(RIGHT.T)
ROW_TWIST = angle_tables(SHORT, LONG, SIZE)
COL_TWIST = tuple(np.tile(t, (1, 2 * WIDE)) for t in angle_tables(LONG, SHORT, SIZE))


def f32(x):
    return np.asarray(x, np.float32)


def split_table(x):
    high = np.asarray(x, jnp.bfloat16)
    return np.stack([high, np.asarray(x - high.astype(np.float64), jnp.bfloat16)])


ROW_FORWARD = split_table(np.concatenate([COS, SIN], axis=1)[OUT_ORDER])
COL_FORWARD = split_table(np.concatenate([COS[:, OUT_ORDER], SIN[:, OUT_ORDER]], axis=0))
COL_RIGHT = split_table(np.concatenate([RIGHT, turn_lanes(RIGHT)], axis=0))
COL_LEFT = split_table(np.concatenate([BACK, turn_after(BACK)], axis=1))
COL_BACK = split_table(np.concatenate([COS, -SIN], axis=1)[BACK_ORDER])
ROW_BACK = split_table(np.concatenate([COS[BACK_ORDER], -SIN[BACK_ORDER]], axis=0))
ROW_TW = f32(np.stack(ROW_TWIST))
COL_TW = f32(np.stack(COL_TWIST))


def halves(x):
    high = x.astype(jnp.bfloat16)
    return high, (x - high.astype(jnp.float32)).astype(jnp.bfloat16)


def joined(parts, axis):
    return tuple(jnp.concatenate([p[i] for p in parts], axis=axis) for i in range(2))


def product(a, b, a_dim=1, b_dim=0):
    def one(x, y):
        return lax.dot_general(
            x, y, (((a_dim,), (b_dim,)), ((), ())), preferred_element_type=jnp.float32
        )

    return one(a[0], b[0]) + (one(a[0], b[1]) + one(a[1], b[0]))


def four_point(z, sign):
    (r0, i0), (r1, i1), (r2, i2), (r3, i3) = z
    ar, ai, br, bi = r0 + r2, i0 + i2, r0 - r2, i0 - i2
    cr, ci, dr, di = r1 + r3, i1 + i3, r1 - r3, i1 - i3
    if sign > 0:
        plus, minus = (br + di, bi - dr), (br - di, bi + dr)
    else:
        plus, minus = (br - di, bi + dr), (br + di, bi - dr)
    return [(ar + cr, ai + ci), plus, (ar - cr, ai - ci), minus]


def times(z, turns, sign):
    r, i = z
    if turns == 0:
        return z
    c = float(np.float32(math.cos(2 * math.pi * turns / 16)))
    s = float(np.float32(sign * math.sin(2 * math.pi * turns / 16)))
    return r * c + i * s, i * c - r * s


def sixteen_point(z, sign):
    inner = [four_point([z[4 * a + b] for a in range(4)], sign) for b in range(4)]
    out = [None] * 16
    for c in range(4):
        mixed = four_point([times(inner[b][c], b * c, sign) for b in range(4)], sign)
        for e in range(4):
            out[c + 4 * e] = mixed[e]
    return out


def row_forward(images, table, twist):
    z = [(images[0][:, LONG * j : LONG * (j + 1)], images[1][:, LONG * j : LONG * (j + 1)]) for j in range(SHORT)]
    spread = sixteen_point(z, 1)
    turned = []
    for j, (r, i) in enumerate(spread):
        c, s = twist[0][j : j + 1, :], twist[1][j : j + 1, :]
        turned.append((r * c + i * s, i * c - r * s))
    out = []
    for d in range(NDIST):
        part = turned[WIDE * d : WIDE * (d + 1)]
        re, im = [r for r, _ in part], [i for _, i in part]
        re, im = halves(jnp.concatenate(re, axis=0)), halves(jnp.concatenate(im, axis=0))
        minus = tuple(-r for r in re)
        both = joined([joined([re, im], 0), joined([im, minus], 0)], 1)
        out.append(product(table, both, 1, 1))
    return out


def wave(turns):
    r = turns - jnp.floor(turns + 0.5)
    r = jnp.where(r > 0.25, 0.5 - r, jnp.where(r < -0.25, -0.5 - r, r))
    x = r * (2.0 * math.pi)
    y = x * x
    p = -1.0 / 39916800.0
    for term in (1.0 / 362880.0, -1.0 / 5040.0, 1.0 / 120.0, -1.0 / 6.0, 1.0):
        p = p * y + term
    return x * p


def signed_square(index):
    shifted = jnp.where(2 * index >= SIZE, index - SIZE, index)
    fraction = shifted.astype(jnp.float32) * (1.0 / SIZE)
    return fraction * fraction


def gains(defocus, blurring, first_col):
    shape = (LONG, LONG)
    lane = lax.broadcasted_iota(jnp.int32, shape, 1)
    row = lax.broadcasted_iota(jnp.int32, shape, 0)
    squared = signed_square(row + LONG * (lane & 15)) + signed_square(first_col + ((lane >> 4) & 3))
    low = lane < LONG // 2
    amplitude = math.sqrt(1.0 + ABSORB_RATIO * ABSORB_RATIO)
    shift = math.atan(ABSORB_RATIO) / (2.0 * math.pi)
    out = []
    for d in range(0, NDIST, 2):
        focus = jnp.where(low, defocus[d], defocus[d + 1]) * (1.0 / (2.0 * math.pi))
        blur = jnp.where(low, blurring[d], blurring[d + 1])
        g = (amplitude * jnp.exp(-blur * squared)) * wave(focus * squared + shift)
        other = jnp.concatenate([g[:, LONG // 2 :], g[:, : LONG // 2]], axis=1)
        out += [jnp.where(low, g, other), jnp.where(low, other, g)]
    return out


def column_middle(blocks, gain, forward, right, left, back, twist):
    c, s = twist[0], twist[1]
    parts = []
    for x in blocks:
        both = product(forward, halves(x))
        u, v = both[:LONG], both[LONG:]
        parts.append(joined([halves(u * c - v * s), halves(v * c + u * s)], 1))
    spectra = product(joined(parts, 0), right)
    quotient = gain[0] * spectra[:LONG]
    for d in range(1, NDIST):
        quotient = quotient + gain[d] * spectra[LONG * d : LONG * (d + 1)]
    both = product(halves(quotient), left)
    a, b = both[:, :LONG], both[:, LONG:]
    upright = joined([halves(a * c - b * s), halves(b * c + a * s)], 0)
    return product(back, upright)


def row_back(blocks, table, twist):
    z = []
    scale = 1.0 / (SIZE * SIZE)
    for d in range(NDIST):
        half = LONG // 2
        t = halves(blocks[d].T)
        turned = joined([tuple(p[half:] for p in t), tuple(-p[:half] for p in t)], 0)
        o = product(joined([t, turned], 1), table)
        for j in range(WIDE):
            r = o[SHORT * j : SHORT * (j + 1)]
            i = o[half + SHORT * j : half + SHORT * (j + 1)]
            v = WIDE * d + j
            c, s = twist[0][v : v + 1, :] * scale, twist[1][v : v + 1, :] * scale
            z.append((r * c - i * s, i * c + r * s))
    return sixteen_point(z, -1)


def first_kernel(images, table, twist, out):
    for d, band in enumerate(row_forward(images[...], table[...], twist[...])):
        out[pl.ds(d, LONG, stride=NDIST), :] = band


def shares(par):
    first_col = SHORT * lax.axis_index(PIX) + WIDE * lax.axis_index(DIST)
    defocus = [par[d : d + 1, :1] for d in range(NDIST)]
    blurring = [par[d : d + 1, 1:] for d in range(NDIST)]
    table = gains(defocus, blurring, first_col)
    weight = table[0] * table[0]
    for g in table[1:]:
        weight = weight + g * g
    share = 0.5 / (weight + REGULARIZER)
    return [g * share for g in table]


def middle_kernel(par, x, forward, right, left, back, twist, out):
    core = lax.axis_index("c")
    blocks = []
    for d in range(NDIST):
        start = NDIST * LONG * (d % 2) + 2 * (d // 2) + core
        blocks.append(x[pl.ds(start, LONG, stride=NDIST), :])
    y = column_middle(blocks, shares(par), forward[...], right[...], left[...], back[...], twist[...])
    for low in range(2):
        out[pl.ds(low, LONG, stride=2), :] = y


def last_kernel(x, table, twist, out):
    blocks = [x[pl.ds(2 * LONG * (d % 2) + d // 2, LONG, stride=2), :] for d in range(NDIST)]
    for j, (r, i) in enumerate(row_back(blocks, table[...], twist[...])):
        out[0, :, LONG * j : LONG * (j + 1)] = r
        out[1, :, LONG * j : LONG * (j + 1)] = i


def call(kernel, shapes, name, limit=VMEM_LIMIT):
    def run(*args):
        return pl.pallas_call(
            kernel,
            out_shape=[jax.ShapeDtypeStruct(shape, jnp.float32) for shape in shapes],
            in_specs=[pl.BlockSpec(memory_space=pltpu.VMEM) for _ in args],
            out_specs=[pl.BlockSpec(memory_space=pltpu.VMEM) for _ in shapes],
            compiler_params=pltpu.CompilerParams(vmem_limit_bytes=limit),
            name=name,
        )(*args)

    return run


def exchange(x, order):
    sent = x.reshape(2 * LONG, -1, LONG)
    got = lax.all_to_all(sent, FLAT, 0, 0, axis_index_groups=chip_groups(order), tiled=True)
    return lax.all_gather(got.reshape(x.shape), "c", axis=0, tiled=True)


def body(contrast, defocus, blurring):
    rows = NDIST * LONG
    (sent,) = call(first_kernel, ((rows, LONG),), "rows_forward", None)(contrast[0], ROW_FORWARD, ROW_TW)
    par = lax.all_gather(jnp.stack([defocus, blurring], axis=1), DIST, axis=0, tiled=True)
    got = exchange(sent, OUT_ORDER)
    (middle,) = call(middle_kernel, ((2 * LONG, LONG),), "columns")(
        par, got, COL_FORWARD, COL_RIGHT, COL_LEFT, COL_BACK, COL_TW
    )
    whole = exchange(middle, BACK_ORDER)
    return call(last_kernel, ((2, SHORT, SIZE),), "rows_back")(whole, ROW_BACK, ROW_TW)[0]


def solution(mesh):
    parts = Mesh(mesh.devices.reshape((2, 2) + PIX_SIZES), FLAT)
    return jax.shard_map(
        body,
        mesh=parts,
        in_specs=(P(DIST, None, PIX, None), P(DIST), P(DIST)),
        out_specs=P(None, PIX, None),
        check_vma=False,
    )
```

```python
import math

import jax
import jax.numpy as jnp
import numpy as np
from jax import lax
from jax.experimental import pallas as pl
from jax.experimental.pallas import tpu as pltpu
from jax.sharding import Mesh
from jax.sharding import PartitionSpec as P

ABSORB_RATIO = 0.1
REGULARIZER = 0.05
SIZE = 2048
LONG = 128
SHORT = 16
NDIST = 4
WIDE = 4
VMEM_LIMIT = 8 << 20
DIST = ("l", "c")
PIX = ("z", "x", "h")
PIX_SIZES = (8, 4, 4)
FLAT = DIST + PIX


FIRST_OUT = (5, 2, 2)
FIRST_BACK = (4, 2, 2)


def by_hops(first, sign):
    place = np.unravel_index(np.arange(LONG), PIX_SIZES)
    z, x, h = [np.abs(p - f) for p, f in zip(place, first)]
    hops = np.minimum(z, 8 - z) + np.minimum(x, 4 - x) + 2 * np.minimum(h, 4 - h)
    hops[np.ravel_multi_index(first, PIX_SIZES)] = -99 * sign
    return np.argsort(sign * hops, kind="stable")


OUT_ORDER = by_hops(FIRST_OUT, 1)
BACK_ORDER = by_hops(FIRST_BACK, -1)


def chip_groups(order):
    return [[(2 * low + core) * LONG + int(k) for k in order for low in range(2)] for core in range(2)]


def angle_tables(left, right, period):
    turns = np.outer(np.arange(left), np.arange(right)) % period
    angles = 2.0 * np.pi * turns / period
    return np.cos(angles), np.sin(angles)


def right_table():
    cosine, sine = angle_tables(SHORT, SHORT, SHORT)
    same = np.eye(WIDE)
    c, s = np.kron(same, cosine), np.kron(same, sine)
    return np.block([[c, -s], [s, c]])


def turn_lanes(table):
    half = table.shape[0] // 2
    return np.concatenate([-table[half:], table[:half]], axis=0)


def turn_after(table):
    half = table.shape[1] // 2
    return np.concatenate([table[:, half:], -table[:, :half]], axis=1)


COS, SIN = angle_tables(LONG, LONG, LONG)
RIGHT = right_table()
BACK = np.array(RIGHT.T)
ROW_TWIST = angle_tables(SHORT, LONG, SIZE)
COL_TWIST = tuple(np.tile(t, (1, 2 * WIDE)) for t in angle_tables(LONG, SHORT, SIZE))


def f32(x):
    return np.asarray(x, np.float32)


def split_table(x):
    high = np.asarray(x, jnp.bfloat16)
    return np.stack([high, np.asarray(x - high.astype(np.float64), jnp.bfloat16)])


ROW_FORWARD = split_table(np.concatenate([COS, SIN], axis=1)[OUT_ORDER])
COL_FORWARD = split_table(np.concatenate([COS[:, OUT_ORDER], SIN[:, OUT_ORDER]], axis=0))
COL_RIGHT = split_table(np.concatenate([RIGHT, turn_lanes(RIGHT)], axis=0))
COL_LEFT = split_table(np.concatenate([BACK, turn_after(BACK)], axis=1))
COL_BACK = split_table(np.concatenate([COS, -SIN], axis=1)[BACK_ORDER])
ROW_BACK = split_table(np.concatenate([COS[BACK_ORDER], -SIN[BACK_ORDER]], axis=0))
ROW_TW = f32(np.stack(ROW_TWIST))
COL_TW = f32(np.stack(COL_TWIST))


def halves(x):
    high = x.astype(jnp.bfloat16)
    return high, (x - high.astype(jnp.float32)).astype(jnp.bfloat16)


def joined(parts, axis):
    return tuple(jnp.concatenate([p[i] for p in parts], axis=axis) for i in range(2))


def product(a, b, a_dim=1, b_dim=0):
    def one(x, y):
        return lax.dot_general(
            x, y, (((a_dim,), (b_dim,)), ((), ())), preferred_element_type=jnp.float32
        )

    return one(a[0], b[0]) + (one(a[0], b[1]) + one(a[1], b[0]))


def four_point(z, sign):
    (r0, i0), (r1, i1), (r2, i2), (r3, i3) = z
    ar, ai, br, bi = r0 + r2, i0 + i2, r0 - r2, i0 - i2
    cr, ci, dr, di = r1 + r3, i1 + i3, r1 - r3, i1 - i3
    if sign > 0:
        plus, minus = (br + di, bi - dr), (br - di, bi + dr)
    else:
        plus, minus = (br - di, bi + dr), (br + di, bi - dr)
    return [(ar + cr, ai + ci), plus, (ar - cr, ai - ci), minus]


def times(z, turns, sign):
    r, i = z
    if turns == 0:
        return z
    c = float(np.float32(math.cos(2 * math.pi * turns / 16)))
    s = float(np.float32(sign * math.sin(2 * math.pi * turns / 16)))
    return r * c + i * s, i * c - r * s


def sixteen_point(z, sign):
    inner = [four_point([z[4 * a + b] for a in range(4)], sign) for b in range(4)]
    out = [None] * 16
    for c in range(4):
        mixed = four_point([times(inner[b][c], b * c, sign) for b in range(4)], sign)
        for e in range(4):
            out[c + 4 * e] = mixed[e]
    return out


def row_forward(images, table, twist):
    z = [(images[0][:, LONG * j : LONG * (j + 1)], images[1][:, LONG * j : LONG * (j + 1)]) for j in range(SHORT)]
    spread = sixteen_point(z, 1)
    turned = []
    for j, (r, i) in enumerate(spread):
        c, s = twist[0][j : j + 1, :], twist[1][j : j + 1, :]
        turned.append((r * c + i * s, i * c - r * s))
    out = []
    for d in range(NDIST):
        part = turned[WIDE * d : WIDE * (d + 1)]
        re, im = [r for r, _ in part], [i for _, i in part]
        re, im = halves(jnp.concatenate(re, axis=0)), halves(jnp.concatenate(im, axis=0))
        minus = tuple(-r for r in re)
        both = joined([joined([re, im], 0), joined([im, minus], 0)], 1)
        out.append(product(table, both, 1, 1))
    return out


def wave(turns):
    r = turns - jnp.floor(turns + 0.5)
    r = jnp.where(r > 0.25, 0.5 - r, jnp.where(r < -0.25, -0.5 - r, r))
    x = r * (2.0 * math.pi)
    y = x * x
    p = -1.0 / 39916800.0
    for term in (1.0 / 362880.0, -1.0 / 5040.0, 1.0 / 120.0, -1.0 / 6.0, 1.0):
        p = p * y + term
    return x * p


def signed_square(index):
    shifted = jnp.where(2 * index >= SIZE, index - SIZE, index)
    fraction = shifted.astype(jnp.float32) * (1.0 / SIZE)
    return fraction * fraction


def gains(defocus, blurring, first_col):
    shape = (LONG, LONG)
    lane = lax.broadcasted_iota(jnp.int32, shape, 1)
    row = lax.broadcasted_iota(jnp.int32, shape, 0)
    squared = signed_square(row + LONG * (lane & 15)) + signed_square(first_col + ((lane >> 4) & 3))
    low = lane < LONG // 2
    amplitude = math.sqrt(1.0 + ABSORB_RATIO * ABSORB_RATIO)
    shift = math.atan(ABSORB_RATIO) / (2.0 * math.pi)
    out = []
    for d in range(0, NDIST, 2):
        focus = jnp.where(low, defocus[d], defocus[d + 1]) * (1.0 / (2.0 * math.pi))
        blur = jnp.where(low, blurring[d], blurring[d + 1])
        g = (amplitude * jnp.exp(-blur * squared)) * wave(focus * squared + shift)
        other = jnp.concatenate([g[:, LONG // 2 :], g[:, : LONG // 2]], axis=1)
        out += [jnp.where(low, g, other), jnp.where(low, other, g)]
    return out


def column_middle(blocks, gain, forward, right, left, back, twist):
    c, s = twist[0], twist[1]
    parts = []
    for x in blocks:
        both = product(forward, halves(x))
        u, v = both[:LONG], both[LONG:]
        parts.append(joined([halves(u * c - v * s), halves(v * c + u * s)], 1))
    spectra = product(joined(parts, 0), right)
    quotient = gain[0] * spectra[:LONG]
    for d in range(1, NDIST):
        quotient = quotient + gain[d] * spectra[LONG * d : LONG * (d + 1)]
    both = product(halves(quotient), left)
    a, b = both[:, :LONG], both[:, LONG:]
    upright = joined([halves(a * c - b * s), halves(b * c + a * s)], 0)
    return product(back, upright)


def row_back(blocks, table, twist):
    z = []
    scale = 1.0 / (SIZE * SIZE)
    for d in range(NDIST):
        half = LONG // 2
        t = halves(blocks[d].T)
        turned = joined([tuple(p[half:] for p in t), tuple(-p[:half] for p in t)], 0)
        o = product(joined([t, turned], 1), table)
        for j in range(WIDE):
            r = o[SHORT * j : SHORT * (j + 1)]
            i = o[half + SHORT * j : half + SHORT * (j + 1)]
            v = WIDE * d + j
            c, s = twist[0][v : v + 1, :] * scale, twist[1][v : v + 1, :] * scale
            z.append((r * c - i * s, i * c + r * s))
    return sixteen_point(z, -1)


def first_kernel(images, table, twist, out):
    for d, band in enumerate(row_forward(images[...], table[...], twist[...])):
        out[pl.ds(d, LONG, stride=NDIST), :] = band


def shares(par):
    first_col = SHORT * lax.axis_index(PIX) + WIDE * lax.axis_index(DIST)
    defocus = [par[d : d + 1, :1] for d in range(NDIST)]
    blurring = [par[d : d + 1, 1:] for d in range(NDIST)]
    table = gains(defocus, blurring, first_col)
    weight = table[0] * table[0]
    for g in table[1:]:
        weight = weight + g * g
    share = 0.5 / (weight + REGULARIZER)
    return [g * share for g in table]


def middle_kernel(par, x, forward, right, left, back, twist, out):
    core = lax.axis_index("c")
    blocks = []
    for d in range(NDIST):
        start = NDIST * LONG * (d % 2) + 2 * (d // 2) + core
        blocks.append(x[pl.ds(start, LONG, stride=NDIST), :])
    y = column_middle(blocks, shares(par), forward[...], right[...], left[...], back[...], twist[...])
    for low in range(2):
        out[pl.ds(low, LONG, stride=2), :] = y


def last_kernel(x, table, twist, out):
    blocks = [x[pl.ds(2 * LONG * (d % 2) + d // 2, LONG, stride=2), :] for d in range(NDIST)]
    for j, (r, i) in enumerate(row_back(blocks, table[...], twist[...])):
        out[0, :, LONG * j : LONG * (j + 1)] = r
        out[1, :, LONG * j : LONG * (j + 1)] = i


def call(kernel, shapes, name, limit=VMEM_LIMIT):
    def run(*args):
        return pl.pallas_call(
            kernel,
            out_shape=[jax.ShapeDtypeStruct(shape, jnp.float32) for shape in shapes],
            in_specs=[pl.BlockSpec(memory_space=pltpu.VMEM) for _ in args],
            out_specs=[pl.BlockSpec(memory_space=pltpu.VMEM) for _ in shapes],
            compiler_params=pltpu.CompilerParams(vmem_limit_bytes=limit),
            name=name,
        )(*args)

    return run


def exchange(x, order):
    sent = x.reshape(2 * LONG, -1, LONG)
    got = lax.all_to_all(sent, FLAT, 0, 0, axis_index_groups=chip_groups(order), tiled=True)
    return lax.all_gather(got.reshape(x.shape), "c", axis=0, tiled=True)


def body(contrast, defocus, blurring):
    rows = NDIST * LONG
    (sent,) = call(first_kernel, ((rows, LONG),), "rows_forward", None)(contrast[0], ROW_FORWARD, ROW_TW)
    par = lax.all_gather(jnp.stack([defocus, blurring], axis=1), DIST, axis=0, tiled=True)
    got = exchange(sent, OUT_ORDER)
    (middle,) = call(middle_kernel, ((2 * LONG, LONG),), "columns")(
        par, got, COL_FORWARD, COL_RIGHT, COL_LEFT, COL_BACK, COL_TW
    )
    whole = exchange(middle, BACK_ORDER)
    return call(last_kernel, ((2, SHORT, SIZE),), "rows_back")(whole, ROW_BACK, ROW_TW)[0]


def solution(mesh):
    parts = Mesh(mesh.devices.reshape((2, 2) + PIX_SIZES), FLAT)
    return jax.shard_map(
        body,
        mesh=parts,
        in_specs=(P(DIST, None, PIX, None), P(DIST), P(DIST)),
        out_specs=P(None, PIX, None),
        check_vma=False,
    )
```

```python
import math

import jax
import jax.numpy as jnp
import numpy as np
from jax import lax
from jax.experimental import pallas as pl
from jax.experimental.pallas import tpu as pltpu
from jax.sharding import Mesh
from jax.sharding import PartitionSpec as P

ABSORB_RATIO = 0.1
REGULARIZER = 0.05
SIZE = 2048
LONG = 128
SHORT = 16
NDIST = 4
WIDE = 4
VMEM_LIMIT = 8 << 20
DIST = ("l", "c")
PIX = ("z", "x", "h")
PIX_SIZES = (8, 4, 4)
FLAT = DIST + PIX


FIRST_OUT = (5, 2, 2)
FIRST_BACK = (4, 2, 2)


def far_first(first):
    place = np.unravel_index(np.arange(LONG), PIX_SIZES)
    z, x, h = [np.abs(p - f) for p, f in zip(place, first)]
    hops = np.minimum(z, 8 - z) + np.minimum(x, 4 - x) + 2 * np.minimum(h, 4 - h)
    hops[np.ravel_multi_index(first, PIX_SIZES)] = 99
    return np.argsort(-hops, kind="stable")


OUT_ORDER = far_first(FIRST_OUT)
BACK_ORDER = far_first(FIRST_BACK)


def chip_groups(order):
    return [[(2 * low + core) * LONG + int(k) for k in order for low in range(2)] for core in range(2)]


def angle_tables(left, right, period):
    turns = np.outer(np.arange(left), np.arange(right)) % period
    angles = 2.0 * np.pi * turns / period
    return np.cos(angles), np.sin(angles)


def right_table():
    cosine, sine = angle_tables(SHORT, SHORT, SHORT)
    same = np.eye(WIDE)
    c, s = np.kron(same, cosine), np.kron(same, sine)
    return np.block([[c, -s], [s, c]])


def turn_lanes(table):
    half = table.shape[0] // 2
    return np.concatenate([-table[half:], table[:half]], axis=0)


def turn_after(table):
    half = table.shape[1] // 2
    return np.concatenate([table[:, half:], -table[:, :half]], axis=1)


COS, SIN = angle_tables(LONG, LONG, LONG)
RIGHT = right_table()
BACK = np.array(RIGHT.T)
ROW_TWIST = angle_tables(SHORT, LONG, SIZE)
COL_TWIST = tuple(np.tile(t, (1, 2 * WIDE)) for t in angle_tables(LONG, SHORT, SIZE))


def f32(x):
    return np.asarray(x, np.float32)


def split_table(x):
    high = np.asarray(x, jnp.bfloat16)
    return np.stack([high, np.asarray(x - high.astype(np.float64), jnp.bfloat16)])


ROW_FORWARD = split_table(np.concatenate([COS, SIN], axis=1)[OUT_ORDER])
COL_FORWARD = split_table(np.concatenate([COS[:, OUT_ORDER], SIN[:, OUT_ORDER]], axis=0))
COL_RIGHT = split_table(np.concatenate([RIGHT, turn_lanes(RIGHT)], axis=0))
COL_LEFT = split_table(np.concatenate([BACK, turn_after(BACK)], axis=1))
COL_BACK = split_table(np.concatenate([COS, -SIN], axis=1)[BACK_ORDER])
ROW_BACK = split_table(np.concatenate([COS[BACK_ORDER], -SIN[BACK_ORDER]], axis=0))
ROW_TW = f32(np.stack(ROW_TWIST))
COL_TW = f32(np.stack(COL_TWIST))


def halves(x):
    high = x.astype(jnp.bfloat16)
    return high, (x - high.astype(jnp.float32)).astype(jnp.bfloat16)


def joined(parts, axis):
    return tuple(jnp.concatenate([p[i] for p in parts], axis=axis) for i in range(2))


def product(a, b, a_dim=1, b_dim=0):
    left = jnp.concatenate([a[0], a[0], a[1]], axis=a_dim)
    right = jnp.concatenate([b[0], b[1], b[0]], axis=b_dim)
    return lax.dot_general(
        left, right, (((a_dim,), (b_dim,)), ((), ())), preferred_element_type=jnp.float32
    )


def four_point(z, sign):
    (r0, i0), (r1, i1), (r2, i2), (r3, i3) = z
    ar, ai, br, bi = r0 + r2, i0 + i2, r0 - r2, i0 - i2
    cr, ci, dr, di = r1 + r3, i1 + i3, r1 - r3, i1 - i3
    if sign > 0:
        plus, minus = (br + di, bi - dr), (br - di, bi + dr)
    else:
        plus, minus = (br - di, bi + dr), (br + di, bi - dr)
    return [(ar + cr, ai + ci), plus, (ar - cr, ai - ci), minus]


def times(z, turns, sign):
    r, i = z
    if turns == 0:
        return z
    c = float(np.float32(math.cos(2 * math.pi * turns / 16)))
    s = float(np.float32(sign * math.sin(2 * math.pi * turns / 16)))
    return r * c + i * s, i * c - r * s


def sixteen_point(z, sign):
    inner = [four_point([z[4 * a + b] for a in range(4)], sign) for b in range(4)]
    out = [None] * 16
    for c in range(4):
        mixed = four_point([times(inner[b][c], b * c, sign) for b in range(4)], sign)
        for e in range(4):
            out[c + 4 * e] = mixed[e]
    return out


def row_forward(images, table, twist):
    z = [(images[0][:, LONG * j : LONG * (j + 1)], images[1][:, LONG * j : LONG * (j + 1)]) for j in range(SHORT)]
    spread = sixteen_point(z, 1)
    turned = []
    for j, (r, i) in enumerate(spread):
        c, s = twist[0][j : j + 1, :], twist[1][j : j + 1, :]
        turned.append((r * c + i * s, i * c - r * s))
    out = []
    for d in range(NDIST):
        part = turned[WIDE * d : WIDE * (d + 1)]
        re, im = [r for r, _ in part], [i for _, i in part]
        re, im = halves(jnp.concatenate(re, axis=0)), halves(jnp.concatenate(im, axis=0))
        minus = tuple(-r for r in re)
        both = joined([joined([re, im], 0), joined([im, minus], 0)], 1)
        out.append(product(table, both, 1, 1))
    return out


def wave(turns):
    r = turns - jnp.floor(turns + 0.5)
    r = jnp.where(r > 0.25, 0.5 - r, jnp.where(r < -0.25, -0.5 - r, r))
    x = r * (2.0 * math.pi)
    y = x * x
    p = -1.0 / 39916800.0
    for term in (1.0 / 362880.0, -1.0 / 5040.0, 1.0 / 120.0, -1.0 / 6.0, 1.0):
        p = p * y + term
    return x * p


def signed_square(index):
    shifted = jnp.where(2 * index >= SIZE, index - SIZE, index)
    fraction = shifted.astype(jnp.float32) * (1.0 / SIZE)
    return fraction * fraction


def gains(defocus, blurring, first_col):
    shape = (LONG, LONG)
    lane = lax.broadcasted_iota(jnp.int32, shape, 1)
    row = lax.broadcasted_iota(jnp.int32, shape, 0)
    squared = signed_square(row + LONG * (lane & 15)) + signed_square(first_col + ((lane >> 4) & 3))
    low = lane < LONG // 2
    amplitude = math.sqrt(1.0 + ABSORB_RATIO * ABSORB_RATIO)
    shift = math.atan(ABSORB_RATIO) / (2.0 * math.pi)
    out = []
    for d in range(0, NDIST, 2):
        focus = jnp.where(low, defocus[d], defocus[d + 1]) * (1.0 / (2.0 * math.pi))
        blur = jnp.where(low, blurring[d], blurring[d + 1])
        g = (amplitude * jnp.exp(-blur * squared)) * wave(focus * squared + shift)
        other = jnp.concatenate([g[:, LONG // 2 :], g[:, : LONG // 2]], axis=1)
        out += [jnp.where(low, g, other), jnp.where(low, other, g)]
    return out


def column_middle(blocks, gain, forward, right, left, back, twist):
    c, s = twist[0], twist[1]
    parts = []
    for x in blocks:
        both = product(forward, halves(x))
        u, v = both[:LONG], both[LONG:]
        parts.append(joined([halves(u * c - v * s), halves(v * c + u * s)], 1))
    spectra = product(joined(parts, 0), right)
    quotient = gain[0] * spectra[:LONG]
    for d in range(1, NDIST):
        quotient = quotient + gain[d] * spectra[LONG * d : LONG * (d + 1)]
    both = product(halves(quotient), left)
    a, b = both[:, :LONG], both[:, LONG:]
    upright = joined([halves(a * c - b * s), halves(b * c + a * s)], 0)
    return product(back, upright)


def row_back(blocks, table, twist):
    z = []
    scale = 1.0 / (SIZE * SIZE)
    for d in range(NDIST):
        half = LONG // 2
        t = halves(blocks[d].T)
        turned = joined([tuple(p[half:] for p in t), tuple(-p[:half] for p in t)], 0)
        o = product(joined([t, turned], 1), table)
        for j in range(WIDE):
            r = o[SHORT * j : SHORT * (j + 1)]
            i = o[half + SHORT * j : half + SHORT * (j + 1)]
            v = WIDE * d + j
            c, s = twist[0][v : v + 1, :] * scale, twist[1][v : v + 1, :] * scale
            z.append((r * c - i * s, i * c + r * s))
    return sixteen_point(z, -1)


def first_kernel(images, table, twist, out):
    for d, band in enumerate(row_forward(images[...], table[...], twist[...])):
        out[pl.ds(d, LONG, stride=NDIST), :] = band


def shares(par):
    first_col = SHORT * lax.axis_index(PIX) + WIDE * lax.axis_index(DIST)
    defocus = [par[d : d + 1, :1] for d in range(NDIST)]
    blurring = [par[d : d + 1, 1:] for d in range(NDIST)]
    table = gains(defocus, blurring, first_col)
    weight = table[0] * table[0]
    for g in table[1:]:
        weight = weight + g * g
    share = 0.5 / (weight + REGULARIZER)
    return [g * share for g in table]


def middle_kernel(par, x, forward, right, left, back, twist, out):
    core = lax.axis_index("c")
    blocks = []
    for d in range(NDIST):
        start = NDIST * LONG * (d % 2) + 2 * (d // 2) + core
        blocks.append(x[pl.ds(start, LONG, stride=NDIST), :])
    y = column_middle(blocks, shares(par), forward[...], right[...], left[...], back[...], twist[...])
    for low in range(2):
        out[pl.ds(low, LONG, stride=2), :] = y


def last_kernel(x, table, twist, out):
    blocks = [x[pl.ds(2 * LONG * (d % 2) + d // 2, LONG, stride=2), :] for d in range(NDIST)]
    for j, (r, i) in enumerate(row_back(blocks, table[...], twist[...])):
        out[0, :, LONG * j : LONG * (j + 1)] = r
        out[1, :, LONG * j : LONG * (j + 1)] = i


def call(kernel, shapes, name, limit=VMEM_LIMIT):
    def run(*args):
        return pl.pallas_call(
            kernel,
            out_shape=[jax.ShapeDtypeStruct(shape, jnp.float32) for shape in shapes],
            in_specs=[pl.BlockSpec(memory_space=pltpu.VMEM) for _ in args],
            out_specs=[pl.BlockSpec(memory_space=pltpu.VMEM) for _ in shapes],
            compiler_params=pltpu.CompilerParams(vmem_limit_bytes=limit),
            name=name,
        )(*args)

    return run


def exchange(x, order):
    sent = x.reshape(2 * LONG, -1, LONG)
    got = lax.all_to_all(sent, FLAT, 0, 0, axis_index_groups=chip_groups(order), tiled=True)
    return lax.all_gather(got.reshape(x.shape), "c", axis=0, tiled=True)


def body(contrast, defocus, blurring):
    rows = NDIST * LONG
    (sent,) = call(first_kernel, ((rows, LONG),), "rows_forward", None)(contrast[0], ROW_FORWARD, ROW_TW)
    par = lax.all_gather(jnp.stack([defocus, blurring], axis=1), DIST, axis=0, tiled=True)
    got = exchange(sent, OUT_ORDER)
    (middle,) = call(middle_kernel, ((2 * LONG, LONG),), "columns")(
        par, got, COL_FORWARD, COL_RIGHT, COL_LEFT, COL_BACK, COL_TW
    )
    whole = exchange(middle, BACK_ORDER)
    return call(last_kernel, ((2, SHORT, SIZE),), "rows_back")(whole, ROW_BACK, ROW_TW)[0]


def solution(mesh):
    parts = Mesh(mesh.devices.reshape((2, 2) + PIX_SIZES), FLAT)
    return jax.shard_map(
        body,
        mesh=parts,
        in_specs=(P(DIST, None, PIX, None), P(DIST), P(DIST)),
        out_specs=P(None, PIX, None),
        check_vma=False,
    )
```

```python
import math

import jax
import jax.numpy as jnp
import numpy as np
from jax import lax
from jax.experimental import pallas as pl
from jax.experimental.pallas import tpu as pltpu
from jax.sharding import Mesh
from jax.sharding import PartitionSpec as P

ABSORB_RATIO = 0.1
REGULARIZER = 0.05
SIZE = 2048
LONG = 128
SHORT = 16
NDIST = 4
WIDE = 4
VMEM_LIMIT = 8 << 20
DIST = ("l", "c")
PIX = ("z", "x", "h")
PIX_SIZES = (8, 4, 4)
FLAT = DIST + PIX


FIRST_OUT = (6, 2, 2)
FIRST_BACK = (4, 2, 2)


def far_first(first):
    place = np.unravel_index(np.arange(LONG), PIX_SIZES)
    z, x, h = [np.abs(p - f) for p, f in zip(place, first)]
    hops = np.minimum(z, 8 - z) + np.minimum(x, 4 - x) + 2 * np.minimum(h, 4 - h)
    hops[np.ravel_multi_index(first, PIX_SIZES)] = 99
    return np.argsort(-hops, kind="stable")


OUT_ORDER = far_first(FIRST_OUT)
BACK_ORDER = far_first(FIRST_BACK)


def chip_groups(order):
    return [[(2 * low + core) * LONG + int(k) for k in order for low in range(2)] for core in range(2)]


def angle_tables(left, right, period):
    turns = np.outer(np.arange(left), np.arange(right)) % period
    angles = 2.0 * np.pi * turns / period
    return np.cos(angles), np.sin(angles)


def right_table():
    cosine, sine = angle_tables(SHORT, SHORT, SHORT)
    same = np.eye(WIDE)
    c, s = np.kron(same, cosine), np.kron(same, sine)
    return np.block([[c, -s], [s, c]])


def turn_lanes(table):
    half = table.shape[0] // 2
    return np.concatenate([-table[half:], table[:half]], axis=0)


def turn_after(table):
    half = table.shape[1] // 2
    return np.concatenate([table[:, half:], -table[:, :half]], axis=1)


COS, SIN = angle_tables(LONG, LONG, LONG)
RIGHT = right_table()
BACK = np.array(RIGHT.T)
ROW_TWIST = angle_tables(SHORT, LONG, SIZE)
COL_TWIST = tuple(np.tile(t, (1, 2 * WIDE)) for t in angle_tables(LONG, SHORT, SIZE))


def f32(x):
    return np.asarray(x, np.float32)


def split_table(x):
    high = np.asarray(x, jnp.bfloat16)
    return np.stack([high, np.asarray(x - high.astype(np.float64), jnp.bfloat16)])


ROW_FORWARD = split_table(np.concatenate([COS, SIN], axis=1)[OUT_ORDER])
COL_FORWARD = split_table(np.concatenate([COS[:, OUT_ORDER], SIN[:, OUT_ORDER]], axis=0))
COL_RIGHT = split_table(np.concatenate([RIGHT, turn_lanes(RIGHT)], axis=0))
COL_LEFT = split_table(np.concatenate([BACK, turn_after(BACK)], axis=1))
COL_BACK = split_table(np.concatenate([COS, -SIN], axis=1)[BACK_ORDER])
ROW_BACK = split_table(np.concatenate([COS[BACK_ORDER], -SIN[BACK_ORDER]], axis=0))
ROW_TW = f32(np.stack(ROW_TWIST))
COL_TW = f32(np.stack(COL_TWIST))


def halves(x):
    high = x.astype(jnp.bfloat16)
    return high, (x - high.astype(jnp.float32)).astype(jnp.bfloat16)


def joined(parts, axis):
    return tuple(jnp.concatenate([p[i] for p in parts], axis=axis) for i in range(2))


def product(a, b, a_dim=1, b_dim=0):
    left = jnp.concatenate([a[0], a[0], a[1]], axis=a_dim)
    right = jnp.concatenate([b[0], b[1], b[0]], axis=b_dim)
    return lax.dot_general(
        left, right, (((a_dim,), (b_dim,)), ((), ())), preferred_element_type=jnp.float32
    )


def four_point(z, sign):
    (r0, i0), (r1, i1), (r2, i2), (r3, i3) = z
    ar, ai, br, bi = r0 + r2, i0 + i2, r0 - r2, i0 - i2
    cr, ci, dr, di = r1 + r3, i1 + i3, r1 - r3, i1 - i3
    if sign > 0:
        plus, minus = (br + di, bi - dr), (br - di, bi + dr)
    else:
        plus, minus = (br - di, bi + dr), (br + di, bi - dr)
    return [(ar + cr, ai + ci), plus, (ar - cr, ai - ci), minus]


def times(z, turns, sign):
    r, i = z
    if turns == 0:
        return z
    c = float(np.float32(math.cos(2 * math.pi * turns / 16)))
    s = float(np.float32(sign * math.sin(2 * math.pi * turns / 16)))
    return r * c + i * s, i * c - r * s


def sixteen_point(z, sign):
    inner = [four_point([z[4 * a + b] for a in range(4)], sign) for b in range(4)]
    out = [None] * 16
    for c in range(4):
        mixed = four_point([times(inner[b][c], b * c, sign) for b in range(4)], sign)
        for e in range(4):
            out[c + 4 * e] = mixed[e]
    return out


def row_forward(images, table, twist):
    z = [(images[0][:, LONG * j : LONG * (j + 1)], images[1][:, LONG * j : LONG * (j + 1)]) for j in range(SHORT)]
    spread = sixteen_point(z, 1)
    turned = []
    for j, (r, i) in enumerate(spread):
        c, s = twist[0][j : j + 1, :], twist[1][j : j + 1, :]
        turned.append((r * c + i * s, i * c - r * s))
    out = []
    for d in range(NDIST):
        part = turned[WIDE * d : WIDE * (d + 1)]
        re, im = [r for r, _ in part], [i for _, i in part]
        re, im = halves(jnp.concatenate(re, axis=0)), halves(jnp.concatenate(im, axis=0))
        minus = tuple(-r for r in re)
        both = joined([joined([re, im], 0), joined([im, minus], 0)], 1)
        out.append(product(table, both, 1, 1))
    return out


def wave(turns):
    r = turns - jnp.floor(turns + 0.5)
    r = jnp.where(r > 0.25, 0.5 - r, jnp.where(r < -0.25, -0.5 - r, r))
    x = r * (2.0 * math.pi)
    y = x * x
    p = -1.0 / 39916800.0
    for term in (1.0 / 362880.0, -1.0 / 5040.0, 1.0 / 120.0, -1.0 / 6.0, 1.0):
        p = p * y + term
    return x * p


def signed_square(index):
    shifted = jnp.where(2 * index >= SIZE, index - SIZE, index)
    fraction = shifted.astype(jnp.float32) * (1.0 / SIZE)
    return fraction * fraction


def gains(defocus, blurring, first_col):
    shape = (LONG, LONG)
    lane = lax.broadcasted_iota(jnp.int32, shape, 1)
    row = lax.broadcasted_iota(jnp.int32, shape, 0)
    squared = signed_square(row + LONG * (lane & 15)) + signed_square(first_col + ((lane >> 4) & 3))
    low = lane < LONG // 2
    amplitude = math.sqrt(1.0 + ABSORB_RATIO * ABSORB_RATIO)
    shift = math.atan(ABSORB_RATIO) / (2.0 * math.pi)
    out = []
    for d in range(0, NDIST, 2):
        focus = jnp.where(low, defocus[d], defocus[d + 1]) * (1.0 / (2.0 * math.pi))
        blur = jnp.where(low, blurring[d], blurring[d + 1])
        g = (amplitude * jnp.exp(-blur * squared)) * wave(focus * squared + shift)
        other = jnp.concatenate([g[:, LONG // 2 :], g[:, : LONG // 2]], axis=1)
        out += [jnp.where(low, g, other), jnp.where(low, other, g)]
    return out


def column_middle(blocks, gain, forward, right, left, back, twist):
    c, s = twist[0], twist[1]
    parts = []
    for x in blocks:
        both = product(forward, halves(x))
        u, v = both[:LONG], both[LONG:]
        parts.append(joined([halves(u * c - v * s), halves(v * c + u * s)], 1))
    spectra = product(joined(parts, 0), right)
    quotient = gain[0] * spectra[:LONG]
    for d in range(1, NDIST):
        quotient = quotient + gain[d] * spectra[LONG * d : LONG * (d + 1)]
    both = product(halves(quotient), left)
    a, b = both[:, :LONG], both[:, LONG:]
    upright = joined([halves(a * c - b * s), halves(b * c + a * s)], 0)
    return product(back, upright)


def row_back(blocks, table, twist):
    z = []
    scale = 1.0 / (SIZE * SIZE)
    for d in range(NDIST):
        half = LONG // 2
        t = halves(blocks[d].T)
        turned = joined([tuple(p[half:] for p in t), tuple(-p[:half] for p in t)], 0)
        o = product(joined([t, turned], 1), table)
        for j in range(WIDE):
            r = o[SHORT * j : SHORT * (j + 1)]
            i = o[half + SHORT * j : half + SHORT * (j + 1)]
            v = WIDE * d + j
            c, s = twist[0][v : v + 1, :] * scale, twist[1][v : v + 1, :] * scale
            z.append((r * c - i * s, i * c + r * s))
    return sixteen_point(z, -1)


def first_kernel(images, table, twist, out):
    for d, band in enumerate(row_forward(images[...], table[...], twist[...])):
        out[pl.ds(d, LONG, stride=NDIST), :] = band


def shares(par):
    first_col = SHORT * lax.axis_index(PIX) + WIDE * lax.axis_index(DIST)
    defocus = [par[d : d + 1, :1] for d in range(NDIST)]
    blurring = [par[d : d + 1, 1:] for d in range(NDIST)]
    table = gains(defocus, blurring, first_col)
    weight = table[0] * table[0]
    for g in table[1:]:
        weight = weight + g * g
    share = 0.5 / (weight + REGULARIZER)
    return [g * share for g in table]


def middle_kernel(par, x, forward, right, left, back, twist, out):
    core = lax.axis_index("c")
    blocks = []
    for d in range(NDIST):
        start = NDIST * LONG * (d % 2) + 2 * (d // 2) + core
        blocks.append(x[pl.ds(start, LONG, stride=NDIST), :])
    y = column_middle(blocks, shares(par), forward[...], right[...], left[...], back[...], twist[...])
    for low in range(2):
        out[pl.ds(low, LONG, stride=2), :] = y


def last_kernel(x, table, twist, out):
    blocks = [x[pl.ds(2 * LONG * (d % 2) + d // 2, LONG, stride=2), :] for d in range(NDIST)]
    for j, (r, i) in enumerate(row_back(blocks, table[...], twist[...])):
        out[0, :, LONG * j : LONG * (j + 1)] = r
        out[1, :, LONG * j : LONG * (j + 1)] = i


def call(kernel, shapes, name, limit=VMEM_LIMIT):
    def run(*args):
        return pl.pallas_call(
            kernel,
            out_shape=[jax.ShapeDtypeStruct(shape, jnp.float32) for shape in shapes],
            in_specs=[pl.BlockSpec(memory_space=pltpu.VMEM) for _ in args],
            out_specs=[pl.BlockSpec(memory_space=pltpu.VMEM) for _ in shapes],
            compiler_params=pltpu.CompilerParams(vmem_limit_bytes=limit),
            name=name,
        )(*args)

    return run


def exchange(x, order):
    sent = x.reshape(2 * LONG, -1, LONG)
    got = lax.all_to_all(sent, FLAT, 0, 0, axis_index_groups=chip_groups(order), tiled=True)
    return lax.all_gather(got.reshape(x.shape), "c", axis=0, tiled=True)


def body(contrast, defocus, blurring):
    rows = NDIST * LONG
    (sent,) = call(first_kernel, ((rows, LONG),), "rows_forward", None)(contrast[0], ROW_FORWARD, ROW_TW)
    par = lax.all_gather(jnp.stack([defocus, blurring], axis=1), DIST, axis=0, tiled=True)
    got = exchange(sent, OUT_ORDER)
    (middle,) = call(middle_kernel, ((2 * LONG, LONG),), "columns")(
        par, got, COL_FORWARD, COL_RIGHT, COL_LEFT, COL_BACK, COL_TW
    )
    whole = exchange(middle, BACK_ORDER)
    return call(last_kernel, ((2, SHORT, SIZE),), "rows_back")(whole, ROW_BACK, ROW_TW)[0]


def solution(mesh):
    parts = Mesh(mesh.devices.reshape((2, 2) + PIX_SIZES), FLAT)
    return jax.shard_map(
        body,
        mesh=parts,
        in_specs=(P(DIST, None, PIX, None), P(DIST), P(DIST)),
        out_specs=P(None, PIX, None),
        check_vma=False,
    )
```

```python
import math

import jax
import jax.numpy as jnp
import numpy as np
from jax import lax
from jax.experimental import pallas as pl
from jax.experimental.pallas import tpu as pltpu
from jax.sharding import Mesh
from jax.sharding import PartitionSpec as P

ABSORB_RATIO = 0.1
REGULARIZER = 0.05
SIZE = 2048
LONG = 128
SHORT = 16
NDIST = 4
WIDE = 4
VMEM_LIMIT = 8 << 20
DIST = ("l", "c")
PIX = ("z", "x", "h")
PIX_SIZES = (8, 4, 4)
FLAT = DIST + PIX


FIRST_OUT = (5, 2, 2)
FIRST_BACK = (4, 2, 2)


def far_first(first):
    place = np.unravel_index(np.arange(LONG), PIX_SIZES)
    z, x, h = [np.abs(p - f) for p, f in zip(place, first)]
    hops = np.minimum(z, 8 - z) + np.minimum(x, 4 - x) + 2 * np.minimum(h, 4 - h)
    hops[np.ravel_multi_index(first, PIX_SIZES)] = 99
    return np.argsort(-hops, kind="stable")


OUT_ORDER = far_first(FIRST_OUT)
BACK_ORDER = far_first(FIRST_BACK)


def out_groups():
    return [[(2 * low + core) * LONG + int(k) for k in OUT_ORDER for low in range(2)] for core in range(2)]


def back_groups():
    return [[(2 * low + core) * LONG + int(k) for low in range(2) for k in BACK_ORDER] for core in range(2)]


def angle_tables(left, right, period):
    turns = np.outer(np.arange(left), np.arange(right)) % period
    angles = 2.0 * np.pi * turns / period
    return np.cos(angles), np.sin(angles)


def right_table():
    cosine, sine = angle_tables(SHORT, SHORT, SHORT)
    same = np.eye(WIDE)
    c, s = np.kron(same, cosine), np.kron(same, sine)
    return np.block([[c, -s], [s, c]])


def turn_lanes(table):
    half = table.shape[0] // 2
    return np.concatenate([-table[half:], table[:half]], axis=0)


def turn_after(table):
    half = table.shape[1] // 2
    return np.concatenate([table[:, half:], -table[:, :half]], axis=1)


COS, SIN = angle_tables(LONG, LONG, LONG)
RIGHT = right_table()
BACK = np.array(RIGHT.T)
ROW_TWIST = angle_tables(SHORT, LONG, SIZE)
COL_TWIST = tuple(np.tile(t, (1, 2 * WIDE)) for t in angle_tables(LONG, SHORT, SIZE))


def f32(x):
    return np.asarray(x, np.float32)


def split_table(x):
    high = np.asarray(x, jnp.bfloat16)
    return np.stack([high, np.asarray(x - high.astype(np.float64), jnp.bfloat16)])


ROW_FORWARD = split_table(np.concatenate([COS, SIN], axis=1)[OUT_ORDER])
COL_FORWARD = split_table(np.concatenate([COS[:, OUT_ORDER], SIN[:, OUT_ORDER]], axis=0))
COL_RIGHT = split_table(np.concatenate([RIGHT, turn_lanes(RIGHT)], axis=0))
COL_LEFT = split_table(np.concatenate([BACK, turn_after(BACK)], axis=1))
COL_BACK = split_table(np.concatenate([COS, -SIN], axis=1)[BACK_ORDER])
ROW_BACK = split_table(np.concatenate([COS[BACK_ORDER], -SIN[BACK_ORDER]], axis=0))
ROW_TW = f32(np.stack(ROW_TWIST))
COL_TW = f32(np.stack(COL_TWIST))


def halves(x):
    high = x.astype(jnp.bfloat16)
    return high, (x - high.astype(jnp.float32)).astype(jnp.bfloat16)


def joined(parts, axis):
    return tuple(jnp.concatenate([p[i] for p in parts], axis=axis) for i in range(2))


def product(a, b, a_dim=1, b_dim=0):
    left = jnp.concatenate([a[0], a[0], a[1]], axis=a_dim)
    right = jnp.concatenate([b[0], b[1], b[0]], axis=b_dim)
    return lax.dot_general(
        left, right, (((a_dim,), (b_dim,)), ((), ())), preferred_element_type=jnp.float32
    )


def four_point(z, sign):
    (r0, i0), (r1, i1), (r2, i2), (r3, i3) = z
    ar, ai, br, bi = r0 + r2, i0 + i2, r0 - r2, i0 - i2
    cr, ci, dr, di = r1 + r3, i1 + i3, r1 - r3, i1 - i3
    if sign > 0:
        plus, minus = (br + di, bi - dr), (br - di, bi + dr)
    else:
        plus, minus = (br - di, bi + dr), (br + di, bi - dr)
    return [(ar + cr, ai + ci), plus, (ar - cr, ai - ci), minus]


def times(z, turns, sign):
    r, i = z
    if turns == 0:
        return z
    c = float(np.float32(math.cos(2 * math.pi * turns / 16)))
    s = float(np.float32(sign * math.sin(2 * math.pi * turns / 16)))
    return r * c + i * s, i * c - r * s


def sixteen_point(z, sign):
    inner = [four_point([z[4 * a + b] for a in range(4)], sign) for b in range(4)]
    out = [None] * 16
    for c in range(4):
        mixed = four_point([times(inner[b][c], b * c, sign) for b in range(4)], sign)
        for e in range(4):
            out[c + 4 * e] = mixed[e]
    return out


def row_forward(images, table, twist):
    z = [(images[0][:, LONG * j : LONG * (j + 1)], images[1][:, LONG * j : LONG * (j + 1)]) for j in range(SHORT)]
    spread = sixteen_point(z, 1)
    turned = []
    for j, (r, i) in enumerate(spread):
        c, s = twist[0][j : j + 1, :], twist[1][j : j + 1, :]
        turned.append((r * c + i * s, i * c - r * s))
    out = []
    for d in range(NDIST):
        part = turned[WIDE * d : WIDE * (d + 1)]
        re, im = [r for r, _ in part], [i for _, i in part]
        re, im = halves(jnp.concatenate(re, axis=0)), halves(jnp.concatenate(im, axis=0))
        minus = tuple(-r for r in re)
        both = joined([joined([re, im], 0), joined([im, minus], 0)], 1)
        out.append(product(table, both, 1, 1))
    return out


def wave(turns):
    r = turns - jnp.floor(turns + 0.5)
    r = jnp.where(r > 0.25, 0.5 - r, jnp.where(r < -0.25, -0.5 - r, r))
    x = r * (2.0 * math.pi)
    y = x * x
    p = -1.0 / 39916800.0
    for term in (1.0 / 362880.0, -1.0 / 5040.0, 1.0 / 120.0, -1.0 / 6.0, 1.0):
        p = p * y + term
    return x * p


def signed_square(index):
    shifted = jnp.where(2 * index >= SIZE, index - SIZE, index)
    fraction = shifted.astype(jnp.float32) * (1.0 / SIZE)
    return fraction * fraction


def gains(defocus, blurring, first_col):
    shape = (LONG, LONG)
    lane = lax.broadcasted_iota(jnp.int32, shape, 1)
    row = lax.broadcasted_iota(jnp.int32, shape, 0)
    squared = signed_square(row + LONG * (lane & 15)) + signed_square(first_col + ((lane >> 4) & 3))
    low = lane < LONG // 2
    amplitude = math.sqrt(1.0 + ABSORB_RATIO * ABSORB_RATIO)
    shift = math.atan(ABSORB_RATIO) / (2.0 * math.pi)
    out = []
    for d in range(0, NDIST, 2):
        focus = jnp.where(low, defocus[d], defocus[d + 1]) * (1.0 / (2.0 * math.pi))
        blur = jnp.where(low, blurring[d], blurring[d + 1])
        g = (amplitude * jnp.exp(-blur * squared)) * wave(focus * squared + shift)
        other = jnp.concatenate([g[:, LONG // 2 :], g[:, : LONG // 2]], axis=1)
        out += [jnp.where(low, g, other), jnp.where(low, other, g)]
    return out


def column_middle(blocks, gain, forward, right, left, back, twist):
    c, s = twist[0], twist[1]
    parts = []
    for x in blocks:
        both = product(forward, halves(x))
        u, v = both[:LONG], both[LONG:]
        parts.append(joined([halves(u * c - v * s), halves(v * c + u * s)], 1))
    spectra = product(joined(parts, 0), right)
    quotient = gain[0] * spectra[:LONG]
    for d in range(1, NDIST):
        quotient = quotient + gain[d] * spectra[LONG * d : LONG * (d + 1)]
    both = product(halves(quotient), left)
    a, b = both[:, :LONG], both[:, LONG:]
    upright = joined([halves(a * c - b * s), halves(b * c + a * s)], 0)
    return product(back, upright)


def row_back(blocks, table, twist):
    z = []
    scale = 1.0 / (SIZE * SIZE)
    for d in range(NDIST):
        half = LONG // 2
        t = halves(blocks[d].T)
        turned = joined([tuple(p[half:] for p in t), tuple(-p[:half] for p in t)], 0)
        o = product(joined([t, turned], 1), table)
        for j in range(WIDE):
            r = o[SHORT * j : SHORT * (j + 1)]
            i = o[half + SHORT * j : half + SHORT * (j + 1)]
            v = WIDE * d + j
            c, s = twist[0][v : v + 1, :] * scale, twist[1][v : v + 1, :] * scale
            z.append((r * c - i * s, i * c + r * s))
    return sixteen_point(z, -1)


def first_kernel(images, table, twist, out):
    for d, band in enumerate(row_forward(images[...], table[...], twist[...])):
        out[pl.ds(d, LONG, stride=NDIST), :] = band


def shares(par):
    first_col = SHORT * lax.axis_index(PIX) + WIDE * lax.axis_index(DIST)
    defocus = [par[d : d + 1, :1] for d in range(NDIST)]
    blurring = [par[d : d + 1, 1:] for d in range(NDIST)]
    table = gains(defocus, blurring, first_col)
    weight = table[0] * table[0]
    for g in table[1:]:
        weight = weight + g * g
    share = 0.5 / (weight + REGULARIZER)
    return [g * share for g in table]


def middle_kernel(par, x, forward, right, left, back, twist, out):
    core = lax.axis_index("c")
    blocks = []
    for d in range(NDIST):
        start = NDIST * LONG * (d % 2) + 2 * (d // 2) + core
        blocks.append(x[pl.ds(start, LONG, stride=NDIST), :])
    y = column_middle(blocks, shares(par), forward[...], right[...], left[...], back[...], twist[...])
    for low in range(2):
        out[LONG * low : LONG * (low + 1), :] = y


def last_kernel(x, table, twist, out):
    starts = [LONG * (2 * (d % 2) + d // 2) for d in range(NDIST)]
    blocks = [x[start : start + LONG, :] for start in starts]
    for j, (r, i) in enumerate(row_back(blocks, table[...], twist[...])):
        out[0, :, LONG * j : LONG * (j + 1)] = r
        out[1, :, LONG * j : LONG * (j + 1)] = i


def call(kernel, shapes, name, limit=VMEM_LIMIT):
    def run(*args):
        return pl.pallas_call(
            kernel,
            out_shape=[jax.ShapeDtypeStruct(shape, jnp.float32) for shape in shapes],
            in_specs=[pl.BlockSpec(memory_space=pltpu.VMEM) for _ in args],
            out_specs=[pl.BlockSpec(memory_space=pltpu.VMEM) for _ in shapes],
            compiler_params=pltpu.CompilerParams(vmem_limit_bytes=limit),
            name=name,
        )(*args)

    return run


def exchange(x, groups):
    sent = x.reshape(2 * LONG, -1, LONG)
    got = lax.all_to_all(sent, FLAT, 0, 0, axis_index_groups=groups, tiled=True)
    return lax.all_gather(got.reshape(x.shape), "c", axis=0, tiled=True)


def body(contrast, defocus, blurring):
    rows = NDIST * LONG
    (sent,) = call(first_kernel, ((rows, LONG),), "rows_forward", None)(contrast[0], ROW_FORWARD, ROW_TW)
    par = lax.all_gather(jnp.stack([defocus, blurring], axis=1), DIST, axis=0, tiled=True)
    got = exchange(sent, out_groups())
    (middle,) = call(middle_kernel, ((2 * LONG, LONG),), "columns")(
        par, got, COL_FORWARD, COL_RIGHT, COL_LEFT, COL_BACK, COL_TW
    )
    whole = exchange(middle, back_groups())
    return call(last_kernel, ((2, SHORT, SIZE),), "rows_back")(whole, ROW_BACK, ROW_TW)[0]


def solution(mesh):
    parts = Mesh(mesh.devices.reshape((2, 2) + PIX_SIZES), FLAT)
    return jax.shard_map(
        body,
        mesh=parts,
        in_specs=(P(DIST, None, PIX, None), P(DIST), P(DIST)),
        out_specs=P(None, PIX, None),
        check_vma=False,
    )
```

```python
import math

import jax
import jax.numpy as jnp
import numpy as np
from jax import lax
from jax.experimental import pallas as pl
from jax.experimental.pallas import tpu as pltpu
from jax.sharding import Mesh
from jax.sharding import PartitionSpec as P

ABSORB_RATIO = 0.1
REGULARIZER = 0.05
SIZE = 2048
LONG = 128
SHORT = 16
NDIST = 4
WIDE = 4
VMEM_LIMIT = 8 << 20
DIST = ("l", "c")
PIX = ("z", "x", "h")
PIX_SIZES = (8, 4, 4)
FLAT = DIST + PIX


FIRST_OUT = (5, 2, 2)
FIRST_BACK = (4, 2, 2)


def far_first(first):
    place = np.unravel_index(np.arange(LONG), PIX_SIZES)
    z, x, h = [np.abs(p - f) for p, f in zip(place, first)]
    hops = np.minimum(z, 8 - z) + np.minimum(x, 4 - x) + 2 * np.minimum(h, 4 - h)
    hops[np.ravel_multi_index(first, PIX_SIZES)] = 99
    return np.argsort(-hops, kind="stable")


OUT_ORDER = far_first(FIRST_OUT)
BACK_ORDER = far_first(FIRST_BACK)


def chip_groups(order):
    return [[(2 * low + core) * LONG + int(k) for low in range(2) for k in order] for core in range(2)]


def angle_tables(left, right, period):
    turns = np.outer(np.arange(left), np.arange(right)) % period
    angles = 2.0 * np.pi * turns / period
    return np.cos(angles), np.sin(angles)


def right_table():
    cosine, sine = angle_tables(SHORT, SHORT, SHORT)
    same = np.eye(WIDE)
    c, s = np.kron(same, cosine), np.kron(same, sine)
    return np.block([[c, -s], [s, c]])


def turn_lanes(table):
    half = table.shape[0] // 2
    return np.concatenate([-table[half:], table[:half]], axis=0)


def turn_after(table):
    half = table.shape[1] // 2
    return np.concatenate([table[:, half:], -table[:, :half]], axis=1)


COS, SIN = angle_tables(LONG, LONG, LONG)
RIGHT = right_table()
BACK = np.array(RIGHT.T)
ROW_TWIST = angle_tables(SHORT, LONG, SIZE)
COL_TWIST = tuple(np.tile(t, (1, 2 * WIDE)) for t in angle_tables(LONG, SHORT, SIZE))


def f32(x):
    return np.asarray(x, np.float32)


def split_table(x):
    high = np.asarray(x, jnp.bfloat16)
    return np.stack([high, np.asarray(x - high.astype(np.float64), jnp.bfloat16)])


ROW_FORWARD = split_table(np.concatenate([COS, SIN], axis=1)[OUT_ORDER])
COL_FORWARD = split_table(np.concatenate([COS[:, OUT_ORDER], SIN[:, OUT_ORDER]], axis=0))
COL_RIGHT = split_table(np.concatenate([RIGHT, turn_lanes(RIGHT)], axis=0))
COL_LEFT = split_table(np.concatenate([BACK, turn_after(BACK)], axis=1))
COL_BACK = split_table(np.concatenate([COS, -SIN], axis=1)[BACK_ORDER])
ROW_BACK = split_table(np.concatenate([COS[BACK_ORDER], -SIN[BACK_ORDER]], axis=0))
ROW_TW = f32(np.stack(ROW_TWIST))
COL_TW = f32(np.stack(COL_TWIST))


def halves(x):
    high = x.astype(jnp.bfloat16)
    return high, (x - high.astype(jnp.float32)).astype(jnp.bfloat16)


def joined(parts, axis):
    return tuple(jnp.concatenate([p[i] for p in parts], axis=axis) for i in range(2))


def product(a, b, a_dim=1, b_dim=0):
    left = jnp.concatenate([a[0], a[0], a[1]], axis=a_dim)
    right = jnp.concatenate([b[0], b[1], b[0]], axis=b_dim)
    return lax.dot_general(
        left, right, (((a_dim,), (b_dim,)), ((), ())), preferred_element_type=jnp.float32
    )


def four_point(z, sign):
    (r0, i0), (r1, i1), (r2, i2), (r3, i3) = z
    ar, ai, br, bi = r0 + r2, i0 + i2, r0 - r2, i0 - i2
    cr, ci, dr, di = r1 + r3, i1 + i3, r1 - r3, i1 - i3
    if sign > 0:
        plus, minus = (br + di, bi - dr), (br - di, bi + dr)
    else:
        plus, minus = (br - di, bi + dr), (br + di, bi - dr)
    return [(ar + cr, ai + ci), plus, (ar - cr, ai - ci), minus]


def times(z, turns, sign):
    r, i = z
    if turns == 0:
        return z
    c = float(np.float32(math.cos(2 * math.pi * turns / 16)))
    s = float(np.float32(sign * math.sin(2 * math.pi * turns / 16)))
    return r * c + i * s, i * c - r * s


def sixteen_point(z, sign):
    inner = [four_point([z[4 * a + b] for a in range(4)], sign) for b in range(4)]
    out = [None] * 16
    for c in range(4):
        mixed = four_point([times(inner[b][c], b * c, sign) for b in range(4)], sign)
        for e in range(4):
            out[c + 4 * e] = mixed[e]
    return out


def row_forward(images, table, twist):
    z = [(images[0][:, LONG * j : LONG * (j + 1)], images[1][:, LONG * j : LONG * (j + 1)]) for j in range(SHORT)]
    spread = sixteen_point(z, 1)
    turned = []
    for j, (r, i) in enumerate(spread):
        c, s = twist[0][j : j + 1, :], twist[1][j : j + 1, :]
        turned.append((r * c + i * s, i * c - r * s))
    out = []
    for d in range(NDIST):
        part = turned[WIDE * d : WIDE * (d + 1)]
        re, im = [r for r, _ in part], [i for _, i in part]
        re, im = halves(jnp.concatenate(re, axis=0)), halves(jnp.concatenate(im, axis=0))
        minus = tuple(-r for r in re)
        both = joined([joined([re, im], 0), joined([im, minus], 0)], 1)
        out.append(product(table, both, 1, 1))
    return out


def wave(turns):
    r = turns - jnp.floor(turns + 0.5)
    r = jnp.where(r > 0.25, 0.5 - r, jnp.where(r < -0.25, -0.5 - r, r))
    x = r * (2.0 * math.pi)
    y = x * x
    p = -1.0 / 39916800.0
    for term in (1.0 / 362880.0, -1.0 / 5040.0, 1.0 / 120.0, -1.0 / 6.0, 1.0):
        p = p * y + term
    return x * p


def signed_square(index):
    shifted = jnp.where(2 * index >= SIZE, index - SIZE, index)
    fraction = shifted.astype(jnp.float32) * (1.0 / SIZE)
    return fraction * fraction


def gains(defocus, blurring, first_col):
    shape = (LONG, LONG)
    lane = lax.broadcasted_iota(jnp.int32, shape, 1)
    row = lax.broadcasted_iota(jnp.int32, shape, 0)
    squared = signed_square(row + LONG * (lane & 15)) + signed_square(first_col + ((lane >> 4) & 3))
    low = lane < LONG // 2
    amplitude = math.sqrt(1.0 + ABSORB_RATIO * ABSORB_RATIO)
    shift = math.atan(ABSORB_RATIO) / (2.0 * math.pi)
    out = []
    for d in range(0, NDIST, 2):
        focus = jnp.where(low, defocus[d], defocus[d + 1]) * (1.0 / (2.0 * math.pi))
        blur = jnp.where(low, blurring[d], blurring[d + 1])
        g = (amplitude * jnp.exp(-blur * squared)) * wave(focus * squared + shift)
        other = jnp.concatenate([g[:, LONG // 2 :], g[:, : LONG // 2]], axis=1)
        out += [jnp.where(low, g, other), jnp.where(low, other, g)]
    return out


def column_middle(blocks, gain, forward, right, left, back, twist):
    c, s = twist[0], twist[1]
    parts = []
    for x in blocks:
        both = product(forward, halves(x))
        u, v = both[:LONG], both[LONG:]
        parts.append(joined([halves(u * c - v * s), halves(v * c + u * s)], 1))
    spectra = product(joined(parts, 0), right)
    quotient = gain[0] * spectra[:LONG]
    for d in range(1, NDIST):
        quotient = quotient + gain[d] * spectra[LONG * d : LONG * (d + 1)]
    both = product(halves(quotient), left)
    a, b = both[:, :LONG], both[:, LONG:]
    upright = joined([halves(a * c - b * s), halves(b * c + a * s)], 0)
    return product(back, upright)


def row_back(blocks, table, twist):
    z = []
    scale = 1.0 / (SIZE * SIZE)
    for d in range(NDIST):
        half = LONG // 2
        t = halves(blocks[d].T)
        turned = joined([tuple(p[half:] for p in t), tuple(-p[:half] for p in t)], 0)
        o = product(joined([t, turned], 1), table)
        for j in range(WIDE):
            r = o[SHORT * j : SHORT * (j + 1)]
            i = o[half + SHORT * j : half + SHORT * (j + 1)]
            v = WIDE * d + j
            c, s = twist[0][v : v + 1, :] * scale, twist[1][v : v + 1, :] * scale
            z.append((r * c - i * s, i * c + r * s))
    return sixteen_point(z, -1)


def first_kernel(images, table, twist, out):
    for d, band in enumerate(row_forward(images[...], table[...], twist[...])):
        out[pl.ds(2 * LONG * (d // 2) + d % 2, LONG, stride=2), :] = band


def shares(par):
    first_col = SHORT * lax.axis_index(PIX) + WIDE * lax.axis_index(DIST)
    defocus = [par[d : d + 1, :1] for d in range(NDIST)]
    blurring = [par[d : d + 1, 1:] for d in range(NDIST)]
    table = gains(defocus, blurring, first_col)
    weight = table[0] * table[0]
    for g in table[1:]:
        weight = weight + g * g
    share = 0.5 / (weight + REGULARIZER)
    return [g * share for g in table]


def middle_kernel(par, x, forward, right, left, back, twist, out):
    core = lax.axis_index("c")
    blocks = []
    for d in range(NDIST):
        start = NDIST * LONG * (d % 2) + 2 * LONG * (d // 2) + core
        blocks.append(x[pl.ds(start, LONG, stride=2), :])
    y = column_middle(blocks, shares(par), forward[...], right[...], left[...], back[...], twist[...])
    for low in range(2):
        out[LONG * low : LONG * (low + 1), :] = y


def last_kernel(x, table, twist, out):
    starts = [LONG * (2 * (d % 2) + d // 2) for d in range(NDIST)]
    blocks = [x[start : start + LONG, :] for start in starts]
    for j, (r, i) in enumerate(row_back(blocks, table[...], twist[...])):
        out[0, :, LONG * j : LONG * (j + 1)] = r
        out[1, :, LONG * j : LONG * (j + 1)] = i


def call(kernel, shapes, name, limit=VMEM_LIMIT):
    def run(*args):
        return pl.pallas_call(
            kernel,
            out_shape=[jax.ShapeDtypeStruct(shape, jnp.float32) for shape in shapes],
            in_specs=[pl.BlockSpec(memory_space=pltpu.VMEM) for _ in args],
            out_specs=[pl.BlockSpec(memory_space=pltpu.VMEM) for _ in shapes],
            compiler_params=pltpu.CompilerParams(vmem_limit_bytes=limit),
            name=name,
        )(*args)

    return run


def exchange(x, groups):
    sent = x.reshape(2 * LONG, -1, LONG)
    got = lax.all_to_all(sent, FLAT, 0, 0, axis_index_groups=groups, tiled=True)
    return lax.all_gather(got.reshape(x.shape), "c", axis=0, tiled=True)


def body(contrast, defocus, blurring):
    rows = NDIST * LONG
    (sent,) = call(first_kernel, ((rows, LONG),), "rows_forward", None)(contrast[0], ROW_FORWARD, ROW_TW)
    par = lax.all_gather(jnp.stack([defocus, blurring], axis=1), DIST, axis=0, tiled=True)
    got = exchange(sent, chip_groups(OUT_ORDER))
    (middle,) = call(middle_kernel, ((2 * LONG, LONG),), "columns")(
        par, got, COL_FORWARD, COL_RIGHT, COL_LEFT, COL_BACK, COL_TW
    )
    whole = exchange(middle, chip_groups(BACK_ORDER))
    return call(last_kernel, ((2, SHORT, SIZE),), "rows_back")(whole, ROW_BACK, ROW_TW)[0]


def solution(mesh):
    parts = Mesh(mesh.devices.reshape((2, 2) + PIX_SIZES), FLAT)
    return jax.shard_map(
        body,
        mesh=parts,
        in_specs=(P(DIST, None, PIX, None), P(DIST), P(DIST)),
        out_specs=P(None, PIX, None),
        check_vma=False,
    )
```

```python
import math

import jax
import jax.numpy as jnp
import numpy as np
from jax import lax
from jax.experimental import pallas as pl
from jax.experimental.pallas import tpu as pltpu
from jax.sharding import Mesh
from jax.sharding import PartitionSpec as P

ABSORB_RATIO = 0.1
REGULARIZER = 0.05
SIZE = 2048
LONG = 128
SHORT = 16
NDIST = 4
WIDE = 4
VMEM_LIMIT = 8 << 20
DIST = ("l", "c")
PIX = ("z", "x", "h")
PIX_SIZES = (8, 4, 4)
FLAT = DIST + PIX


FIRST_OUT = (5, 1, 2)
FIRST_BACK = (4, 2, 2)


def far_first(first):
    place = np.unravel_index(np.arange(LONG), PIX_SIZES)
    z, x, h = [np.abs(p - f) for p, f in zip(place, first)]
    hops = np.minimum(z, 8 - z) + np.minimum(x, 4 - x) + 2 * np.minimum(h, 4 - h)
    hops[np.ravel_multi_index(first, PIX_SIZES)] = 99
    return np.argsort(-hops, kind="stable")


OUT_ORDER = far_first(FIRST_OUT)
BACK_ORDER = far_first(FIRST_BACK)


def out_groups():
    return [[(2 * low + core) * LONG + int(k) for k in OUT_ORDER for low in range(2)] for core in range(2)]


def back_groups():
    return [[(2 * low + core) * LONG + int(k) for low in range(2) for k in BACK_ORDER] for core in range(2)]


def angle_tables(left, right, period):
    turns = np.outer(np.arange(left), np.arange(right)) % period
    angles = 2.0 * np.pi * turns / period
    return np.cos(angles), np.sin(angles)


def right_table():
    cosine, sine = angle_tables(SHORT, SHORT, SHORT)
    same = np.eye(WIDE)
    c, s = np.kron(same, cosine), np.kron(same, sine)
    return np.block([[c, -s], [s, c]])


def turn_lanes(table):
    half = table.shape[0] // 2
    return np.concatenate([-table[half:], table[:half]], axis=0)


def turn_after(table):
    half = table.shape[1] // 2
    return np.concatenate([table[:, half:], -table[:, :half]], axis=1)


COS, SIN = angle_tables(LONG, LONG, LONG)
RIGHT = right_table()
BACK = np.array(RIGHT.T)
ROW_TWIST = angle_tables(SHORT, LONG, SIZE)
COL_TWIST = tuple(np.tile(t, (1, 2 * WIDE)) for t in angle_tables(LONG, SHORT, SIZE))


def f32(x):
    return np.asarray(x, np.float32)


def split_table(x):
    high = np.asarray(x, jnp.bfloat16)
    return np.stack([high, np.asarray(x - high.astype(np.float64), jnp.bfloat16)])


ROW_FORWARD = split_table(np.concatenate([COS, SIN], axis=1)[OUT_ORDER])
COL_FORWARD = split_table(np.concatenate([COS[:, OUT_ORDER], SIN[:, OUT_ORDER]], axis=0))
COL_RIGHT = split_table(np.concatenate([RIGHT, turn_lanes(RIGHT)], axis=0))
COL_LEFT = split_table(np.concatenate([BACK, turn_after(BACK)], axis=1))
COL_BACK = split_table(np.concatenate([COS, -SIN], axis=1)[BACK_ORDER])
ROW_BACK = split_table(np.concatenate([COS[BACK_ORDER], -SIN[BACK_ORDER]], axis=0))
ROW_TW = f32(np.stack(ROW_TWIST))
COL_TW = f32(np.stack(COL_TWIST))


def halves(x):
    high = x.astype(jnp.bfloat16)
    return high, (x - high.astype(jnp.float32)).astype(jnp.bfloat16)


def joined(parts, axis):
    return tuple(jnp.concatenate([p[i] for p in parts], axis=axis) for i in range(2))


def product(a, b, a_dim=1, b_dim=0):
    left = jnp.concatenate([a[0], a[0], a[1]], axis=a_dim)
    right = jnp.concatenate([b[0], b[1], b[0]], axis=b_dim)
    return lax.dot_general(
        left, right, (((a_dim,), (b_dim,)), ((), ())), preferred_element_type=jnp.float32
    )


def four_point(z, sign):
    (r0, i0), (r1, i1), (r2, i2), (r3, i3) = z
    ar, ai, br, bi = r0 + r2, i0 + i2, r0 - r2, i0 - i2
    cr, ci, dr, di = r1 + r3, i1 + i3, r1 - r3, i1 - i3
    if sign > 0:
        plus, minus = (br + di, bi - dr), (br - di, bi + dr)
    else:
        plus, minus = (br - di, bi + dr), (br + di, bi - dr)
    return [(ar + cr, ai + ci), plus, (ar - cr, ai - ci), minus]


def times(z, turns, sign):
    r, i = z
    if turns == 0:
        return z
    c = float(np.float32(math.cos(2 * math.pi * turns / 16)))
    s = float(np.float32(sign * math.sin(2 * math.pi * turns / 16)))
    return r * c + i * s, i * c - r * s


def sixteen_point(z, sign):
    inner = [four_point([z[4 * a + b] for a in range(4)], sign) for b in range(4)]
    out = [None] * 16
    for c in range(4):
        mixed = four_point([times(inner[b][c], b * c, sign) for b in range(4)], sign)
        for e in range(4):
            out[c + 4 * e] = mixed[e]
    return out


def row_forward(images, table, twist):
    z = [(images[0][:, LONG * j : LONG * (j + 1)], images[1][:, LONG * j : LONG * (j + 1)]) for j in range(SHORT)]
    spread = sixteen_point(z, 1)
    turned = []
    for j, (r, i) in enumerate(spread):
        c, s = twist[0][j : j + 1, :], twist[1][j : j + 1, :]
        turned.append((r * c + i * s, i * c - r * s))
    out = []
    for d in range(NDIST):
        part = turned[WIDE * d : WIDE * (d + 1)]
        re, im = [r for r, _ in part], [i for _, i in part]
        re, im = halves(jnp.concatenate(re, axis=0)), halves(jnp.concatenate(im, axis=0))
        minus = tuple(-r for r in re)
        both = joined([joined([re, im], 0), joined([im, minus], 0)], 1)
        out.append(product(table, both, 1, 1))
    return out


def wave(turns):
    r = turns - jnp.floor(turns + 0.5)
    r = jnp.where(r > 0.25, 0.5 - r, jnp.where(r < -0.25, -0.5 - r, r))
    x = r * (2.0 * math.pi)
    y = x * x
    p = -1.0 / 39916800.0
    for term in (1.0 / 362880.0, -1.0 / 5040.0, 1.0 / 120.0, -1.0 / 6.0, 1.0):
        p = p * y + term
    return x * p


def signed_square(index):
    shifted = jnp.where(2 * index >= SIZE, index - SIZE, index)
    fraction = shifted.astype(jnp.float32) * (1.0 / SIZE)
    return fraction * fraction


def gains(defocus, blurring, first_col):
    shape = (LONG, LONG)
    lane = lax.broadcasted_iota(jnp.int32, shape, 1)
    row = lax.broadcasted_iota(jnp.int32, shape, 0)
    squared = signed_square(row + LONG * (lane & 15)) + signed_square(first_col + ((lane >> 4) & 3))
    low = lane < LONG // 2
    amplitude = math.sqrt(1.0 + ABSORB_RATIO * ABSORB_RATIO)
    shift = math.atan(ABSORB_RATIO) / (2.0 * math.pi)
    out = []
    for d in range(0, NDIST, 2):
        focus = jnp.where(low, defocus[d], defocus[d + 1]) * (1.0 / (2.0 * math.pi))
        blur = jnp.where(low, blurring[d], blurring[d + 1])
        g = (amplitude * jnp.exp(-blur * squared)) * wave(focus * squared + shift)
        other = jnp.concatenate([g[:, LONG // 2 :], g[:, : LONG // 2]], axis=1)
        out += [jnp.where(low, g, other), jnp.where(low, other, g)]
    return out


def column_middle(blocks, gain, forward, right, left, back, twist):
    c, s = twist[0], twist[1]
    parts = []
    for x in blocks:
        both = product(forward, halves(x))
        u, v = both[:LONG], both[LONG:]
        parts.append(joined([halves(u * c - v * s), halves(v * c + u * s)], 1))
    spectra = product(joined(parts, 0), right)
    quotient = gain[0] * spectra[:LONG]
    for d in range(1, NDIST):
        quotient = quotient + gain[d] * spectra[LONG * d : LONG * (d + 1)]
    both = product(halves(quotient), left)
    a, b = both[:, :LONG], both[:, LONG:]
    upright = joined([halves(a * c - b * s), halves(b * c + a * s)], 0)
    return product(back, upright)


def row_back(blocks, table, twist):
    z = []
    scale = 1.0 / (SIZE * SIZE)
    for d in range(NDIST):
        half = LONG // 2
        t = halves(blocks[d].T)
        turned = joined([tuple(p[half:] for p in t), tuple(-p[:half] for p in t)], 0)
        o = product(joined([t, turned], 1), table)
        for j in range(WIDE):
            r = o[SHORT * j : SHORT * (j + 1)]
            i = o[half + SHORT * j : half + SHORT * (j + 1)]
            v = WIDE * d + j
            c, s = twist[0][v : v + 1, :] * scale, twist[1][v : v + 1, :] * scale
            z.append((r * c - i * s, i * c + r * s))
    return sixteen_point(z, -1)


def first_kernel(images, table, twist, out):
    for d, band in enumerate(row_forward(images[...], table[...], twist[...])):
        out[pl.ds(d, LONG, stride=NDIST), :] = band


def shares(par):
    first_col = SHORT * lax.axis_index(PIX) + WIDE * lax.axis_index(DIST)
    defocus = [par[d : d + 1, :1] for d in range(NDIST)]
    blurring = [par[d : d + 1, 1:] for d in range(NDIST)]
    table = gains(defocus, blurring, first_col)
    weight = table[0] * table[0]
    for g in table[1:]:
        weight = weight + g * g
    share = 0.5 / (weight + REGULARIZER)
    return [g * share for g in table]


def middle_kernel(par, x, forward, right, left, back, twist, out):
    core = lax.axis_index("c")
    blocks = []
    for d in range(NDIST):
        start = NDIST * LONG * (d % 2) + 2 * (d // 2) + core
        blocks.append(x[pl.ds(start, LONG, stride=NDIST), :])
    y = column_middle(blocks, shares(par), forward[...], right[...], left[...], back[...], twist[...])
    for low in range(2):
        out[LONG * low : LONG * (low + 1), :] = y


def last_kernel(x, table, twist, out):
    starts = [LONG * (2 * (d % 2) + d // 2) for d in range(NDIST)]
    blocks = [x[start : start + LONG, :] for start in starts]
    for j, (r, i) in enumerate(row_back(blocks, table[...], twist[...])):
        out[0, :, LONG * j : LONG * (j + 1)] = r
        out[1, :, LONG * j : LONG * (j + 1)] = i


def call(kernel, shapes, name, limit=VMEM_LIMIT):
    def run(*args):
        return pl.pallas_call(
            kernel,
            out_shape=[jax.ShapeDtypeStruct(shape, jnp.float32) for shape in shapes],
            in_specs=[pl.BlockSpec(memory_space=pltpu.VMEM) for _ in args],
            out_specs=[pl.BlockSpec(memory_space=pltpu.VMEM) for _ in shapes],
            compiler_params=pltpu.CompilerParams(vmem_limit_bytes=limit),
            name=name,
        )(*args)

    return run


def exchange(x, groups):
    sent = x.reshape(2 * LONG, -1, LONG)
    got = lax.all_to_all(sent, FLAT, 0, 0, axis_index_groups=groups, tiled=True)
    return lax.all_gather(got.reshape(x.shape), "c", axis=0, tiled=True)


def body(contrast, defocus, blurring):
    rows = NDIST * LONG
    (sent,) = call(first_kernel, ((rows, LONG),), "rows_forward", None)(contrast[0], ROW_FORWARD, ROW_TW)
    par = lax.all_gather(jnp.stack([defocus, blurring], axis=1), DIST, axis=0, tiled=True)
    got = exchange(sent, out_groups())
    (middle,) = call(middle_kernel, ((2 * LONG, LONG),), "columns")(
        par, got, COL_FORWARD, COL_RIGHT, COL_LEFT, COL_BACK, COL_TW
    )
    whole = exchange(middle, back_groups())
    return call(last_kernel, ((2, SHORT, SIZE),), "rows_back")(whole, ROW_BACK, ROW_TW)[0]


def solution(mesh):
    parts = Mesh(mesh.devices.reshape((2, 2) + PIX_SIZES), FLAT)
    return jax.shard_map(
        body,
        mesh=parts,
        in_specs=(P(DIST, None, PIX, None), P(DIST), P(DIST)),
        out_specs=P(None, PIX, None),
        check_vma=False,
    )
```

```python
import math

import jax
import jax.numpy as jnp
import numpy as np
from jax import lax
from jax.experimental import pallas as pl
from jax.experimental.pallas import tpu as pltpu
from jax.sharding import Mesh
from jax.sharding import PartitionSpec as P

ABSORB_RATIO = 0.1
REGULARIZER = 0.05
SIZE = 2048
LONG = 128
SHORT = 16
NDIST = 4
WIDE = 4
VMEM_LIMIT = 8 << 20
DIST = ("l", "c")
PIX = ("z", "x", "h")
PIX_SIZES = (8, 4, 4)
FLAT = DIST + PIX


FIRST_OUT = (5, 2, 2)
FIRST_BACK = (5, 2, 2)


def far_first(first):
    place = np.unravel_index(np.arange(LONG), PIX_SIZES)
    z, x, h = [np.abs(p - f) for p, f in zip(place, first)]
    hops = np.minimum(z, 8 - z) + np.minimum(x, 4 - x) + 2 * np.minimum(h, 4 - h)
    hops[np.ravel_multi_index(first, PIX_SIZES)] = 99
    return np.argsort(-hops, kind="stable")


OUT_ORDER = far_first(FIRST_OUT)
BACK_ORDER = far_first(FIRST_BACK)


def out_groups():
    return [[(2 * low + core) * LONG + int(k) for k in OUT_ORDER for low in range(2)] for core in range(2)]


def back_groups():
    return [[(2 * low + core) * LONG + int(k) for low in range(2) for k in BACK_ORDER] for core in range(2)]


def angle_tables(left, right, period):
    turns = np.outer(np.arange(left), np.arange(right)) % period
    angles = 2.0 * np.pi * turns / period
    return np.cos(angles), np.sin(angles)


def right_table():
    cosine, sine = angle_tables(SHORT, SHORT, SHORT)
    same = np.eye(WIDE)
    c, s = np.kron(same, cosine), np.kron(same, sine)
    return np.block([[c, -s], [s, c]])


def turn_lanes(table):
    half = table.shape[0] // 2
    return np.concatenate([-table[half:], table[:half]], axis=0)


def turn_after(table):
    half = table.shape[1] // 2
    return np.concatenate([table[:, half:], -table[:, :half]], axis=1)


COS, SIN = angle_tables(LONG, LONG, LONG)
RIGHT = right_table()
BACK = np.array(RIGHT.T)
ROW_TWIST = angle_tables(SHORT, LONG, SIZE)
COL_TWIST = tuple(np.tile(t, (1, 2 * WIDE)) for t in angle_tables(LONG, SHORT, SIZE))


def f32(x):
    return np.asarray(x, np.float32)


def split_table(x):
    high = np.asarray(x, jnp.bfloat16)
    return np.stack([high, np.asarray(x - high.astype(np.float64), jnp.bfloat16)])


ROW_FORWARD = split_table(np.concatenate([COS, SIN], axis=1)[OUT_ORDER])
COL_FORWARD = split_table(np.concatenate([COS[:, OUT_ORDER], SIN[:, OUT_ORDER]], axis=0))
COL_RIGHT = split_table(np.concatenate([RIGHT, turn_lanes(RIGHT)], axis=0))
COL_LEFT = split_table(np.concatenate([BACK, turn_after(BACK)], axis=1))
COL_BACK = split_table(np.concatenate([COS, -SIN], axis=1)[BACK_ORDER])
ROW_BACK = split_table(np.concatenate([COS[BACK_ORDER], -SIN[BACK_ORDER]], axis=0))
ROW_TW = f32(np.stack(ROW_TWIST))
COL_TW = f32(np.stack(COL_TWIST))


def halves(x):
    high = x.astype(jnp.bfloat16)
    return high, (x - high.astype(jnp.float32)).astype(jnp.bfloat16)


def joined(parts, axis):
    return tuple(jnp.concatenate([p[i] for p in parts], axis=axis) for i in range(2))


def product(a, b, a_dim=1, b_dim=0):
    left = jnp.concatenate([a[0], a[0], a[1]], axis=a_dim)
    right = jnp.concatenate([b[0], b[1], b[0]], axis=b_dim)
    return lax.dot_general(
        left, right, (((a_dim,), (b_dim,)), ((), ())), preferred_element_type=jnp.float32
    )


def four_point(z, sign):
    (r0, i0), (r1, i1), (r2, i2), (r3, i3) = z
    ar, ai, br, bi = r0 + r2, i0 + i2, r0 - r2, i0 - i2
    cr, ci, dr, di = r1 + r3, i1 + i3, r1 - r3, i1 - i3
    if sign > 0:
        plus, minus = (br + di, bi - dr), (br - di, bi + dr)
    else:
        plus, minus = (br - di, bi + dr), (br + di, bi - dr)
    return [(ar + cr, ai + ci), plus, (ar - cr, ai - ci), minus]


def times(z, turns, sign):
    r, i = z
    if turns == 0:
        return z
    c = float(np.float32(math.cos(2 * math.pi * turns / 16)))
    s = float(np.float32(sign * math.sin(2 * math.pi * turns / 16)))
    return r * c + i * s, i * c - r * s


def sixteen_point(z, sign):
    inner = [four_point([z[4 * a + b] for a in range(4)], sign) for b in range(4)]
    out = [None] * 16
    for c in range(4):
        mixed = four_point([times(inner[b][c], b * c, sign) for b in range(4)], sign)
        for e in range(4):
            out[c + 4 * e] = mixed[e]
    return out


def row_forward(images, table, twist):
    z = [(images[0][:, LONG * j : LONG * (j + 1)], images[1][:, LONG * j : LONG * (j + 1)]) for j in range(SHORT)]
    spread = sixteen_point(z, 1)
    turned = []
    for j, (r, i) in enumerate(spread):
        c, s = twist[0][j : j + 1, :], twist[1][j : j + 1, :]
        turned.append((r * c + i * s, i * c - r * s))
    out = []
    for d in range(NDIST):
        part = turned[WIDE * d : WIDE * (d + 1)]
        re, im = [r for r, _ in part], [i for _, i in part]
        re, im = halves(jnp.concatenate(re, axis=0)), halves(jnp.concatenate(im, axis=0))
        minus = tuple(-r for r in re)
        both = joined([joined([re, im], 0), joined([im, minus], 0)], 1)
        out.append(product(table, both, 1, 1))
    return out


def wave(turns):
    r = turns - jnp.floor(turns + 0.5)
    r = jnp.where(r > 0.25, 0.5 - r, jnp.where(r < -0.25, -0.5 - r, r))
    x = r * (2.0 * math.pi)
    y = x * x
    p = -1.0 / 39916800.0
    for term in (1.0 / 362880.0, -1.0 / 5040.0, 1.0 / 120.0, -1.0 / 6.0, 1.0):
        p = p * y + term
    return x * p


def signed_square(index):
    shifted = jnp.where(2 * index >= SIZE, index - SIZE, index)
    fraction = shifted.astype(jnp.float32) * (1.0 / SIZE)
    return fraction * fraction


def gains(defocus, blurring, first_col):
    shape = (LONG, LONG)
    lane = lax.broadcasted_iota(jnp.int32, shape, 1)
    row = lax.broadcasted_iota(jnp.int32, shape, 0)
    squared = signed_square(row + LONG * (lane & 15)) + signed_square(first_col + ((lane >> 4) & 3))
    low = lane < LONG // 2
    amplitude = math.sqrt(1.0 + ABSORB_RATIO * ABSORB_RATIO)
    shift = math.atan(ABSORB_RATIO) / (2.0 * math.pi)
    out = []
    for d in range(0, NDIST, 2):
        focus = jnp.where(low, defocus[d], defocus[d + 1]) * (1.0 / (2.0 * math.pi))
        blur = jnp.where(low, blurring[d], blurring[d + 1])
        g = (amplitude * jnp.exp(-blur * squared)) * wave(focus * squared + shift)
        other = jnp.concatenate([g[:, LONG // 2 :], g[:, : LONG // 2]], axis=1)
        out += [jnp.where(low, g, other), jnp.where(low, other, g)]
    return out


def column_middle(blocks, gain, forward, right, left, back, twist):
    c, s = twist[0], twist[1]
    parts = []
    for x in blocks:
        both = product(forward, halves(x))
        u, v = both[:LONG], both[LONG:]
        parts.append(joined([halves(u * c - v * s), halves(v * c + u * s)], 1))
    spectra = product(joined(parts, 0), right)
    quotient = gain[0] * spectra[:LONG]
    for d in range(1, NDIST):
        quotient = quotient + gain[d] * spectra[LONG * d : LONG * (d + 1)]
    both = product(halves(quotient), left)
    a, b = both[:, :LONG], both[:, LONG:]
    upright = joined([halves(a * c - b * s), halves(b * c + a * s)], 0)
    return product(back, upright)


def row_back(blocks, table, twist):
    z = []
    scale = 1.0 / (SIZE * SIZE)
    for d in range(NDIST):
        half = LONG // 2
        t = halves(blocks[d].T)
        turned = joined([tuple(p[half:] for p in t), tuple(-p[:half] for p in t)], 0)
        o = product(joined([t, turned], 1), table)
        for j in range(WIDE):
            r = o[SHORT * j : SHORT * (j + 1)]
            i = o[half + SHORT * j : half + SHORT * (j + 1)]
            v = WIDE * d + j
            c, s = twist[0][v : v + 1, :] * scale, twist[1][v : v + 1, :] * scale
            z.append((r * c - i * s, i * c + r * s))
    return sixteen_point(z, -1)


def first_kernel(images, table, twist, out):
    for d, band in enumerate(row_forward(images[...], table[...], twist[...])):
        out[pl.ds(d, LONG, stride=NDIST), :] = band


def shares(par):
    first_col = SHORT * lax.axis_index(PIX) + WIDE * lax.axis_index(DIST)
    defocus = [par[d : d + 1, :1] for d in range(NDIST)]
    blurring = [par[d : d + 1, 1:] for d in range(NDIST)]
    table = gains(defocus, blurring, first_col)
    weight = table[0] * table[0]
    for g in table[1:]:
        weight = weight + g * g
    share = 0.5 / (weight + REGULARIZER)
    return [g * share for g in table]


def middle_kernel(par, x, forward, right, left, back, twist, out):
    core = lax.axis_index("c")
    blocks = []
    for d in range(NDIST):
        start = NDIST * LONG * (d % 2) + 2 * (d // 2) + core
        blocks.append(x[pl.ds(start, LONG, stride=NDIST), :])
    y = column_middle(blocks, shares(par), forward[...], right[...], left[...], back[...], twist[...])
    for low in range(2):
        out[LONG * low : LONG * (low + 1), :] = y


def last_kernel(x, table, twist, out):
    starts = [LONG * (2 * (d % 2) + d // 2) for d in range(NDIST)]
    blocks = [x[start : start + LONG, :] for start in starts]
    for j, (r, i) in enumerate(row_back(blocks, table[...], twist[...])):
        out[0, :, LONG * j : LONG * (j + 1)] = r
        out[1, :, LONG * j : LONG * (j + 1)] = i


def call(kernel, shapes, name, limit=VMEM_LIMIT):
    def run(*args):
        return pl.pallas_call(
            kernel,
            out_shape=[jax.ShapeDtypeStruct(shape, jnp.float32) for shape in shapes],
            in_specs=[pl.BlockSpec(memory_space=pltpu.VMEM) for _ in args],
            out_specs=[pl.BlockSpec(memory_space=pltpu.VMEM) for _ in shapes],
            compiler_params=pltpu.CompilerParams(vmem_limit_bytes=limit),
            name=name,
        )(*args)

    return run


def exchange(x, groups):
    sent = x.reshape(2 * LONG, -1, LONG)
    got = lax.all_to_all(sent, FLAT, 0, 0, axis_index_groups=groups, tiled=True)
    return lax.all_gather(got.reshape(x.shape), "c", axis=0, tiled=True)


def body(contrast, defocus, blurring):
    rows = NDIST * LONG
    (sent,) = call(first_kernel, ((rows, LONG),), "rows_forward", None)(contrast[0], ROW_FORWARD, ROW_TW)
    par = lax.all_gather(jnp.stack([defocus, blurring], axis=1), DIST, axis=0, tiled=True)
    got = exchange(sent, out_groups())
    (middle,) = call(middle_kernel, ((2 * LONG, LONG),), "columns")(
        par, got, COL_FORWARD, COL_RIGHT, COL_LEFT, COL_BACK, COL_TW
    )
    whole = exchange(middle, back_groups())
    return call(last_kernel, ((2, SHORT, SIZE),), "rows_back")(whole, ROW_BACK, ROW_TW)[0]


def solution(mesh):
    parts = Mesh(mesh.devices.reshape((2, 2) + PIX_SIZES), FLAT)
    return jax.shard_map(
        body,
        mesh=parts,
        in_specs=(P(DIST, None, PIX, None), P(DIST), P(DIST)),
        out_specs=P(None, PIX, None),
        check_vma=False,
    )
```
